128 devices in a mesh: gx: 8 (over y, core), gy: 4 (over z), gz: 4 (over x).
Axes of the slice: x: 4, y: 4, z: 4, core: 2. Of those that a mesh axis runs over, the one named last changes fastest.
Arguments:
- velocity: float32 [32768, 3, 128], P(('gx', 'gy', 'gz')), may hold values from -6 to 6
- cell_index: int32 [32768, 128], P(('gx', 'gy', 'gz')), may hold values from 0 to 5804
- block_target: int32 [32768, 1], P(('gx', 'gy', 'gz')), may hold values from 0 to 127; in each aligned block of 256 rows (0 to 255, 256 to 511, ...) at most 3 rows name the same one
- rotation_axis: int32 [32, 32, 32], replicated, may hold values from 0 to 63
- grid_shift: int32 [3], replicated, may hold values from 0 to 31
Outputs:
- brick_velocity: float32 [128, 128, 3, 3, 128], P(('gx', 'gy', 'gz'))
- cell_flow: float32 [3, 32, 32, 512], P(None, 'gx', 'gy', 'gz')
The draws below stay inside these ranges and needn't reach their ends.
Inputs may be any that keep to these rules, and one draw needn't show every extreme that they name: `block_target`: among the blocks that one device holds, no brick is named by more than 3 blocks, a bound that some block reaches.
All inputs are finite; a program needn't handle non-finite values.
Results may differ from the reference program's by a relative error of at most 0.0003.
Values sent between devices are 32-bit elements; how exact they have to be, the bound alone decides.
No kernel may reach another device: no remote copies, remote signals or barrier semaphores. Data moves between devices by JAX's collectives and lax.ppermute only.
A program may use at most 64 MiB of HBM per device.

```python
import math
import jax
import jax.numpy as jnp
import numpy as np
from jax import lax

CX = 4
CY = 8
CZ = 128
BLK_DEV = 256
BROWS = 128
NAX = 64
APER = 32
MOST = 3
NBLK = 32768
NCX = 32
NCY = 32
NCZ = 512
N_GY = 4
N_GZ = 4
DEVICES = 128


def with_ends(entries, rng, least, largest):
    spot = [jax.random.randint(jax.random.fold_in(rng, axis), (), 0, length) for axis, length in enumerate(entries.shape)]
    main_axis = entries.shape.index(max(entries.shape))
    neighbour = spot[:main_axis] + [(spot[main_axis] + 1) % entries.shape[main_axis]] + spot[main_axis + 1:]
    return entries.at[tuple(spot)].set(least).at[tuple(neighbour)].set(largest)


def shard_levels(stream_key, extent, cuts, least, high):
    factor_of = 1.0
    for axis_at, parts in cuts:
        draws = jax.random.uniform(jax.random.fold_in(jax.random.fold_in(stream_key, 6), axis_at), (parts,), jnp.float32, least / len(cuts), high / len(cuts))
        factor_of = factor_of * jnp.repeat(jnp.exp(draws), extent[axis_at] // parts).reshape((-1,) + (1,) * (len(extent) - 1 - axis_at))
    return factor_of


def routed_block(key, own, number, rows, amount, top, limit, slope):
    sequence = jax.random.permutation(key, amount)
    packed, common = load_shares(amount, rows * top, limit, slope, True), load_shares(amount, rows * top, limit, slope, False)
    places = jnp.arange(amount)

    def named(tallies, rotation):
        used = int((tallies > 0).sum())
        fixed = max(1, used // 4)
        moved = fixed + (places - fixed + rotation * (used - fixed)) % max(1, amount - fixed)
        return jnp.zeros((amount,), jnp.int32).at[sequence[jnp.where(places < fixed, places, moved)]].set(jnp.asarray(tallies, jnp.int32))

    tallies = jnp.where(number % 4 == 0, named(packed, number // 4), named(common, number - number // 4 - 1))
    mixed = jax.random.permutation(jax.random.fold_in(own, 3), amount)
    source_of, sink = mixed[0:amount // 2 * 2:2], mixed[1:amount // 2 * 2:2]
    room = jnp.minimum(tallies[source_of] - 1, limit - tallies[sink]) // 2
    room = jnp.where((source_of == sequence[0]) | (sink == sequence[0]) | (tallies[sink] == 0), 0, jnp.maximum(room, 0))
    moved = jax.random.randint(jax.random.fold_in(own, 4), (amount // 2,), 0, 1 << 20) % (room + 1)
    tallies = tallies.at[source_of].add(-moved).at[sink].add(moved)
    members = jnp.searchsorted(jnp.cumsum(tallies), jnp.arange(rows * top), side="right").astype(jnp.int32)
    table = members.reshape(top, rows).T
    table = table[jax.random.permutation(jax.random.fold_in(own, 1), rows)]
    rotation = jax.random.randint(jax.random.fold_in(own, 2), (rows, 1), 0, top)
    return jnp.take_along_axis(table, (jnp.arange(top)[None, :] + rotation) % top, axis=1)


def load_shares(amount, total, most, skew, full):
    portions = [(1 << 20) // math.isqrt(grade ** skew) + 1 for grade in range(1, amount + 1)]
    largest = most if full else min(most, max(-(-total // amount), total * portions[0] // sum(portions)))
    least = 1 if total - largest >= amount - 1 else 0
    given, surplus = [largest] + [least] * (amount - 1), total - largest - least * (amount - 1)
    while surplus > 0:
        movable = [i for i in range(1, amount) if given[i] < largest] or [i for i in range(1, amount) if given[i] < most]
        mass, left = sum([portions[i] for i in movable]), surplus
        for i in movable:
            addition = min(most - given[i], max(1, left * portions[i] // mass), surplus)
            given[i] = given[i] + addition
            surplus = surplus - addition
    return np.array(given)


def normal_values(key, dims, spread, limit, split=(), kind=jnp.bfloat16):
    values = spread * jax.random.normal(key, dims, jnp.float32)
    if split:
        values = values * shard_levels(key, dims, split, -0.22, 0.18)
    return jnp.clip(values, -limit, limit).astype(kind)


def setup_inputs(seed: int = 0) -> dict:
    splits = jax.random.split(jax.random.key(seed), 6)
    velocity = normal_values(splits[0], (NBLK, 3, BROWS), 1.0, 6.0, ((0, 128),), jnp.float32)
    cell_index = with_ends(jax.random.randint(splits[1], (NBLK, BROWS), 0, (CX + 1) * (CY + 1) * (CZ + 1)), jax.random.fold_in(splits[1], 1), 0, ((CX + 1) * (CY + 1) * (CZ + 1)) - 1).astype(jnp.int32)
    block_target_keys = jax.random.split(jax.random.fold_in(splits[2], 1), NBLK // BLK_DEV)
    block_target_turns = jax.random.permutation(jax.random.fold_in(splits[2], 3), NBLK // BLK_DEV)
    block_target = jax.vmap(lambda own, number: routed_block(jax.random.fold_in(splits[2], 2), own, number, BLK_DEV, DEVICES, 1, MOST, 1))(block_target_keys, block_target_turns).reshape((NBLK, 1))
    rotation_axis = with_ends(jax.random.randint(splits[3], (APER, APER, APER), 0, NAX), jax.random.fold_in(splits[3], 1), 0, NAX - 1).astype(jnp.int32)
    grid_shift = jax.random.randint(splits[4], (3,), 0, APER).astype(jnp.int32)
    return dict(velocity=velocity, cell_index=cell_index, block_target=block_target, rotation_axis=rotation_axis, grid_shift=grid_shift)


angle_cosine = -0.6427876096865393
angle_sine = 0.766044443118978

def axis_table():
    counter = jnp.arange(NAX, dtype=jnp.float32) + 0.5
    height = 1.0 - 2.0 * counter / NAX
    radius = jnp.sqrt(jnp.maximum(1.0 - height * height, 0.0))
    turning = counter * 2.399963229728653
    return jnp.stack([radius * jnp.cos(turning), radius * jnp.sin(turning), height])

def rotate_about(direction, relative):
    inner_product = direction[0] * relative[0] + direction[1] * relative[1] + direction[2] * relative[2]
    crossed = [direction[1] * relative[2] - direction[2] * relative[1], direction[2] * relative[0] - direction[0] * relative[2], direction[0] * relative[1] - direction[1] * relative[0]]
    return [relative[component] * angle_cosine + crossed[component] * angle_sine + direction[component] * inner_product * (1.0 - angle_cosine) for component in range(3)]

def reference(velocity, cell_index, block_target, rotation_axis, grid_shift):
    blocks = velocity.shape[0]
    devices = blocks // BLK_DEV
    target = block_target[:, 0]

    def ranks_of(targets):
        onehot = (targets[:, None] == jnp.arange(devices, dtype=jnp.int32)[None, :]).astype(jnp.int32)
        return lax.optimization_barrier(jnp.sum((jnp.cumsum(onehot, axis=0) - onehot) * onehot, axis=1))
    ranking = lax.map(ranks_of, target.reshape(devices, BLK_DEV)).reshape(blocks)
    sender = jnp.arange(blocks, dtype=jnp.int32) // BLK_DEV
    brick_x = target // (N_GY * N_GZ)
    brick_y = target // N_GZ % N_GY
    brick_z = target % N_GZ
    plane_cells = (CY + 1) * (CZ + 1)
    local_x = cell_index // plane_cells
    local_y = cell_index // (CZ + 1) % (CY + 1)
    local_z = cell_index % (CZ + 1)
    global_x = (brick_x[:, None] * CX + local_x) % NCX
    global_y = (brick_y[:, None] * CY + local_y) % NCY
    global_z = (brick_z[:, None] * CZ + local_z) % NCZ
    flat_cell = ((global_x * NCY + global_y) * NCZ + global_z).reshape(-1)
    moving = jnp.transpose(velocity, (1, 0, 2)).reshape(3, -1)
    cell_count = NCX * NCY * NCZ
    counts = jax.ops.segment_sum(jnp.ones(flat_cell.shape, jnp.float32), flat_cell, num_segments=cell_count)
    moments = jnp.stack([jax.ops.segment_sum(moving[component], flat_cell, num_segments=cell_count) for component in range(3)])
    cell_means = moments / jnp.maximum(counts, 1.0)
    cell_flow = cell_means.reshape(3, NCX, NCY, NCZ)
    picked = rotation_axis[(global_x + grid_shift[0]) % APER, (global_y + grid_shift[1]) % APER, (global_z + grid_shift[2]) % APER].reshape(-1)
    direction = axis_table()[:, picked]
    local_flow = cell_means[:, flat_cell]
    relative = [moving[component] - local_flow[component] for component in range(3)]
    turned = rotate_about(direction, relative)
    updated = jnp.stack([local_flow[component] + turned[component] for component in range(3)])
    updated = jnp.transpose(updated.reshape(3, blocks, BROWS), (1, 0, 2))
    places = (target * devices + sender) * MOST + ranking
    placed = jnp.zeros((devices * devices * MOST, 3, BROWS), jnp.float32).at[places].set(updated)
    brick_velocity = placed.reshape(devices, devices, MOST, 3, BROWS)
    return (brick_velocity, cell_flow)
```

```python
import functools

import jax
import jax.numpy as jnp
from jax import lax
from jax.experimental import pallas as pl
from jax.experimental.pallas import tpu as pltpu
from jax.sharding import PartitionSpec as P

CX = 4
CY = 8
CZ = 128
NAX = 64
APER = 32
MOST = 3
PX = CX + 1
PY = CY + 1
PLANES = PX * PY
ROWS = PLANES + 1
PADROWS = 48
EMPTY = 6400.0

angle_cosine = -0.6427876096865393
angle_sine = 0.766044443118978

f32 = jnp.float32
bf16 = jnp.bfloat16
i32 = jnp.int32


def iota(shape, dim):
    return lax.broadcasted_iota(i32, shape, dim)


def axis_table():
    counter = jnp.arange(NAX, dtype=f32) + 0.5
    height = 1.0 - 2.0 * counter / NAX
    radius = jnp.sqrt(jnp.maximum(1.0 - height * height, 0.0))
    turning = counter * 2.399963229728653
    return jnp.stack([radius * jnp.cos(turning), radius * jnp.sin(turning), height])


def split3(value):
    high = value.astype(bf16)
    rest = value - high.astype(f32)
    middle = rest.astype(bf16)
    return high, middle, (rest - middle.astype(f32)).astype(bf16)


def call(body, out_shape, **kw):
    return pl.pallas_call(
        body,
        out_shape=out_shape,
        compiler_params=pltpu.CompilerParams(vmem_limit_bytes=48 * 1024 * 1024),
        **kw,
    )


def pack_body(target_ref, velocity_ref, index_ref, out_ref):
    bricks = 128
    blocks = target_ref.shape[1]
    target = jnp.broadcast_to(target_ref[...], (bricks, blocks))
    onehot = target == iota((bricks, blocks), 0)
    onehot_bf = jnp.where(onehot, 1.0, 0.0).astype(bf16)
    earlier = jnp.where(iota((blocks, blocks), 0) < iota((blocks, blocks), 1), 1.0, 0.0)
    before = jnp.dot(onehot_bf, earlier.astype(bf16), preferred_element_type=f32)
    index = index_ref[...]
    plane = (index * 8129) >> 20
    depth = index - plane * (CZ + 1)
    top = depth == CZ
    label = jnp.where(top, PLANES * 128 + plane, plane * 128 + depth)
    parts = [velocity_ref[c] for c in range(3)] + [label.astype(f32) - EMPTY]
    splits = split3(jnp.concatenate(parts, axis=1))
    for rank in range(MOST):
        place = jnp.where(onehot & (before == float(rank)), 1.0, 0.0).astype(bf16)
        moved = sum(jnp.dot(place, s, preferred_element_type=f32) for s in reversed(splits))
        for c in range(4):
            value = moved[:, c * 128 : (c + 1) * 128]
            if c == 3:
                value = value + EMPTY
            out_ref[pl.ds(rank * 4 + c, bricks, stride=4 * MOST), :] = value


def axes_body(shift_ref, rotation_ref, out_ref, rows):
    base_x = lax.axis_index("gx") * CX + shift_ref[0]
    base_y = lax.axis_index("gy") * CY + shift_ref[1]
    rows[...] = jnp.zeros(rows.shape, i32)
    for ex in range(PX):
        for ey in range(PY):
            a = (base_x + ex) & (APER - 1)
            b = (base_y + ey) & (APER - 1)
            rows[pl.ds(ex * PY + ey, 1), :APER] = rotation_ref[a, pl.ds(b, 1), :]
    value = rows[...].astype(f32)
    value = value + pltpu.roll(value, 32, 1)
    value = value + pltpu.roll(value, 64, 1)
    value = pltpu.roll(value, (128 - shift_ref[2]) & 127, 1)
    first = column_as_row(value)
    out_ref[...] = jnp.where(iota(value.shape, 0) == PLANES, first, value)


def column_as_row(value):
    column = jnp.broadcast_to(value[:, 0:1], value.shape)
    same = iota(value.shape, 0) == iota(value.shape, 1)
    return jnp.sum(jnp.where(same, column, 0.0), axis=0, keepdims=True)


def gather_x_faces(total, c, head_ref, tail_ref):
    head_ref[c, 0:PY] = total[0:PY]
    head_ref[c, PY : PY + 1] = total[PLANES:ROWS]
    tail_ref[c, 0:PY] = total[PLANES - PY : PLANES]
    tail_ref[c, PY : PY + 1] = total[PLANES:ROWS]


SLOTS_STEP = 8


def deposit_body(slots_ref, total_ref, head_ref, tail_ref, acc, rows_q, rows_l):
    slots = slots_ref.shape[0] // 4
    label = slots_ref[pl.ds(3, slots, stride=4), :].astype(i32)
    rows_q[...] = (label >> 7).astype(f32)
    rows_l[...] = (label & 127).astype(f32)
    acc[...] = jnp.zeros(acc.shape, f32)
    sub8 = iota((8, 128), 0)
    sub16 = iota((16, 128), 0)
    half = jnp.where(sub16 >= 8, 1.0, 0.0).astype(bf16)
    step16 = sub16.astype(f32).astype(bf16)
    one = jnp.ones((16, 128), bf16)
    zero = jnp.zeros((16, 128), bf16)

    def step(i, carry):
        weighted, depths = [], []
        for k in range(SLOTS_STEP):
            slot = i * SLOTS_STEP + k
            own = slots_ref[pl.ds(pl.multiple_of(i * SLOTS_STEP * 4, 8) + 4 * k, 4), :]
            own = jnp.concatenate([own, own], axis=0)
            high = own.astype(bf16).astype(f32)
            value = jnp.where(sub8 < 4, high, own - high)
            value = jnp.where(sub8 == 3, 1.0, jnp.where(sub8 == 7, 0.0, value))
            value = jnp.concatenate([value, value], axis=0).astype(bf16)
            q = jnp.broadcast_to(rows_q[pl.ds(slot, 1), :], (16, 128)).astype(bf16) - half
            l = jnp.broadcast_to(rows_l[pl.ds(slot, 1), :], (16, 128)).astype(bf16) - step16
            weighted.append(
                jnp.concatenate(
                    [jnp.where(q == float(2 * j), value, zero) for j in range(ROWS // 2)], axis=0
                )
            )
            depths.append(
                jnp.concatenate(
                    [jnp.where(l == float(16 * j), one, zero) for j in range(8)], axis=0
                )
            )
        acc[...] += lax.dot_general(
            jnp.concatenate(weighted, axis=1),
            jnp.concatenate(depths, axis=1),
            (((1,), (1,)), ((), ())),
            preferred_element_type=f32,
        )
        return carry

    lax.fori_loop(0, slots // SLOTS_STEP, step, 0)
    for c in range(4):
        total = acc[pl.ds(c, ROWS, stride=8), :]
        if c < 3:
            total = total + acc[pl.ds(c + 4, ROWS, stride=8), :]
        total_ref[c, 0:ROWS] = total
        total_ref[c, ROWS:PADROWS] = jnp.zeros((PADROWS - ROWS, 128), f32)
        gather_x_faces(total, c, head_ref, tail_ref)


def moved_lanes(row, first, count, shift):
    lane = iota(row.shape, 1)
    rolled = pltpu.roll(row, shift % 128, 1)
    return jnp.where((lane >= first) & (lane < first + count), rolled, 0.0)


def fold_x_body(total_ref, up_ref, down_ref, out_ref, head_ref, tail_ref):
    last = PLANES - PY
    for c in range(4):
        out_ref[c] = total_ref[c]
        out_ref[c, 0:PY] = total_ref[c, 0:PY] + down_ref[c, 0:PY]
        out_ref[c, last:PLANES] = total_ref[c, last:PLANES] + up_ref[c, 0:PY]
        out_ref[c, PLANES:ROWS] = (
            total_ref[c, PLANES:ROWS]
            + moved_lanes(up_ref[c, PY : PY + 1], last, PY, last)
            + moved_lanes(down_ref[c, PY : PY + 1], 0, PY, -last)
        )
        head_ref[c, 0:PX] = out_ref[c, pl.ds(0, PX, stride=PY)]
        head_ref[c, PX : PX + 1] = out_ref[c, PLANES:ROWS]
        tail_ref[c, 0:PX] = out_ref[c, pl.ds(CY, PX, stride=PY)]
        tail_ref[c, PX : PX + 1] = out_ref[c, PLANES:ROWS]


def fold_y_body(total_ref, up_ref, down_ref, out_ref, head_ref, tail_ref):
    lane = iota((1, 128), 1)
    for c in range(4):
        out_ref[c] = total_ref[c]
        out_ref[c, pl.ds(CY, PX, stride=PY)] = (
            total_ref[c, pl.ds(CY, PX, stride=PY)] + up_ref[c, 0:PX]
        )
        out_ref[c, pl.ds(0, PX, stride=PY)] = (
            total_ref[c, pl.ds(0, PX, stride=PY)] + down_ref[c, 0:PX]
        )
        up = pltpu.roll(up_ref[c, PX : PX + 1], CY, 1)
        down = pltpu.roll(down_ref[c, PX : PX + 1], 128 - CY, 1)
        edge = lane % PY
        out_ref[c, PLANES:ROWS] = (
            total_ref[c, PLANES:ROWS]
            + jnp.where((edge == CY) & (lane < PLANES), up, 0.0)
            + jnp.where((edge == 0) & (lane < PLANES), down, 0.0)
        )
        total = out_ref[c]
        head_ref[c : c + 1] = column_as_row(total)
        tail_ref[c : c + 1] = total[PLANES:ROWS]
        head_ref[4 + c : 5 + c] = jnp.zeros((1, 128), f32)
        tail_ref[4 + c : 5 + c] = jnp.zeros((1, 128), f32)


GROUP = 4


def collide_body(
    total_ref, up_ref, down_ref, axes_ref, units_ref, slots_ref, out_ref, flow_ref, cells
):
    shape = (PADROWS, 128)
    row = iota(shape, 0)
    lane = iota(shape, 1)
    top = (row == PLANES) & (lane < PLANES)
    totals = []
    for c in range(4):
        own = total_ref[c]
        column = jnp.sum(
            jnp.where((row == lane) & (row < PLANES), down_ref[c : c + 1], 0.0),
            axis=1,
            keepdims=True,
        )
        own = own + jnp.where(lane == 0, column, 0.0)
        totals.append(own + jnp.where(top, up_ref[c : c + 1], 0.0))
    count = jnp.maximum(totals[3], 1.0)
    for c in range(3):
        mean = totals[c] / count
        cells[c] = mean
        for ex in range(CX):
            flow_ref[c, ex] = mean[ex * PY : ex * PY + CY]
    cells[3] = axes_ref[...]
    units = [jnp.broadcast_to(units_ref[c : c + 1], (8, 128)) for c in range(3)]

    def step(i, carry):
        places = []
        for k in range(GROUP):
            first = pl.multiple_of((i % (16 // GROUP)) * (8 * GROUP * 12), 8 * GROUP * 12)
            first = first + (i // (16 // GROUP)) * 4 + k * 8 * 12
            places.append(first)
        labels = [slots_ref[pl.ds(p + 3, 8, stride=12), :].astype(i32) for p in places]
        rows = [label >> 7 for label in labels]
        lanes = [label & 127 for label in labels]
        found = [[jnp.zeros((8, 128), f32) for c in range(4)] for k in range(GROUP)]
        for q in range(ROWS):
            for c in range(4):
                table = jnp.broadcast_to(cells[c, q : q + 1], (8, 128))
                for k in range(GROUP):
                    read = jnp.take_along_axis(table, lanes[k], axis=1)
                    found[k][c] = jnp.where(rows[k] == q, read, found[k][c])
        for k in range(GROUP):
            which = found[k][3].astype(i32)
            n = [jnp.take_along_axis(units[c], which, axis=1) for c in range(3)]
            u = found[k][:3]
            w = [slots_ref[pl.ds(places[k] + c, 8, stride=12), :] - u[c] for c in range(3)]
            inner = n[0] * w[0] + n[1] * w[1] + n[2] * w[2]
            crossed = [
                n[1] * w[2] - n[2] * w[1],
                n[2] * w[0] - n[0] * w[2],
                n[0] * w[1] - n[1] * w[0],
            ]
            rank = i // (16 // GROUP)
            source = pl.multiple_of((i % (16 // GROUP)) * (8 * GROUP) + 8 * k, 8)
            for c in range(3):
                out_ref[rank, c, pl.ds(source, 8), :] = (
                    u[c]
                    + w[c] * angle_cosine
                    + crossed[c] * angle_sine
                    + n[c] * inner * (1.0 - angle_cosine)
                )
        return carry

    lax.fori_loop(0, MOST * 16 // GROUP, step, 0)


def both_ways(head, tail, axis):
    count = lax.axis_size(axis)
    up = lax.ppermute(head, axis, [((i + 1) % count, i) for i in range(count)])
    down = lax.ppermute(tail, axis, [(i, (i + 1) % count) for i in range(count)])
    return up, down


def shards(velocity, cell_index, block_target, rotation_axis, grid_shift):
    devices = 128
    shape = jax.ShapeDtypeStruct
    vmem = pl.BlockSpec(memory_space=pltpu.VMEM)
    smem = pl.BlockSpec(memory_space=pltpu.SMEM)
    send = call(pack_body, shape((devices * MOST * 4, 128), f32), name="pack")(
        block_target.reshape(1, -1), jnp.transpose(velocity, (1, 0, 2)), cell_index
    )
    axes = call(
        axes_body,
        shape((PADROWS, 128), f32),
        in_specs=[smem, vmem],
        scratch_shapes=[pltpu.VMEM((PADROWS, 128), i32)],
        name="axes",
    )(grid_shift, rotation_axis)
    units = jnp.pad(axis_table(), ((0, 5), (0, 128 - NAX)))
    slots = lax.all_to_all(
        send.reshape(devices, MOST * 4, 128), ("gx", "gy", "gz"), split_axis=0, concat_axis=0, tiled=True
    ).reshape(devices * MOST * 4, 128)
    total_shape = shape((4, PADROWS, 128), f32)
    x_face = shape((4, 16, 128), f32)
    y_face = shape((4, 8, 128), f32)
    z_face = shape((8, 128), f32)
    total, head, tail = call(
        deposit_body,
        [total_shape, x_face, x_face],
        scratch_shapes=[
            pltpu.VMEM((ROWS * 8, 128), f32),
            pltpu.VMEM((devices * MOST, 128), f32),
            pltpu.VMEM((devices * MOST, 128), f32),
        ],
        name="deposit",
    )(slots)
    up, down = both_ways(head, tail, "gx")
    total, head, tail = call(fold_x_body, [total_shape, y_face, y_face], name="fold_x")(
        total, up, down
    )
    up, down = both_ways(head, tail, "gy")
    total, head, tail = call(fold_y_body, [total_shape, z_face, z_face], name="fold_y")(
        total, up, down
    )
    up, down = both_ways(head, tail, "gz")
    updated, cell_flow = call(
        collide_body,
        [shape((MOST, 3, devices, 128), f32), shape((3, CX, CY, CZ), f32)],
        scratch_shapes=[pltpu.VMEM((4, PADROWS, 128), f32)],
        name="collide",
    )(total, up, down, axes, units, slots)
    return jnp.transpose(updated, (2, 0, 1, 3))[None], cell_flow


def solution(mesh):
    return jax.shard_map(
        shards,
        mesh=mesh,
        in_specs=(
            P(("gx", "gy", "gz"), None, None),
            P(("gx", "gy", "gz"), None),
            P(("gx", "gy", "gz"), None),
            P(),
            P(),
        ),
        out_specs=(P(("gx", "gy", "gz"), None, None, None, None), P(None, "gx", "gy", "gz")),
        check_vma=False,
    )
```

```python
import functools

import jax
import jax.numpy as jnp
from jax import lax
from jax.experimental import pallas as pl
from jax.experimental.pallas import tpu as pltpu
from jax.sharding import PartitionSpec as P

CX = 4
CY = 8
CZ = 128
NAX = 64
APER = 32
MOST = 3
PX = CX + 1
PY = CY + 1
PLANES = PX * PY
ROWS = PLANES + 1
PADROWS = 48
EMPTY = 6400.0

angle_cosine = -0.6427876096865393
angle_sine = 0.766044443118978

f32 = jnp.float32
bf16 = jnp.bfloat16
i32 = jnp.int32


def iota(shape, dim):
    return lax.broadcasted_iota(i32, shape, dim)


def axis_table():
    counter = jnp.arange(NAX, dtype=f32) + 0.5
    height = 1.0 - 2.0 * counter / NAX
    radius = jnp.sqrt(jnp.maximum(1.0 - height * height, 0.0))
    turning = counter * 2.399963229728653
    return jnp.stack([radius * jnp.cos(turning), radius * jnp.sin(turning), height])


def split3(value):
    high = value.astype(bf16)
    rest = value - high.astype(f32)
    middle = rest.astype(bf16)
    return high, middle, (rest - middle.astype(f32)).astype(bf16)


def call(body, out_shape, **kw):
    return pl.pallas_call(
        body,
        out_shape=out_shape,
        compiler_params=pltpu.CompilerParams(vmem_limit_bytes=48 * 1024 * 1024),
        **kw,
    )


def pack_body(target_ref, velocity_ref, index_ref, out_ref):
    bricks = 128
    blocks = target_ref.shape[1]
    target = jnp.broadcast_to(target_ref[...], (bricks, blocks))
    onehot = target == iota((bricks, blocks), 0)
    onehot_bf = jnp.where(onehot, 1.0, 0.0).astype(bf16)
    earlier = jnp.where(iota((blocks, blocks), 0) < iota((blocks, blocks), 1), 1.0, 0.0)
    before = jnp.dot(onehot_bf, earlier.astype(bf16), preferred_element_type=f32)
    index = index_ref[...]
    plane = (index * 8129) >> 20
    depth = index - plane * (CZ + 1)
    top = depth == CZ
    label = jnp.where(top, PLANES * 128 + plane, plane * 128 + depth)
    parts = [velocity_ref[c] for c in range(3)] + [label.astype(f32) - EMPTY]
    splits = split3(jnp.concatenate(parts, axis=1))
    for rank in range(MOST):
        place = jnp.where(onehot & (before == float(rank)), 1.0, 0.0).astype(bf16)
        moved = sum(jnp.dot(place, s, preferred_element_type=f32) for s in reversed(splits))
        for c in range(4):
            value = moved[:, c * 128 : (c + 1) * 128]
            if c == 3:
                value = value + EMPTY
            out_ref[pl.ds(rank * 4 + c, bricks, stride=4 * MOST), :] = value


def axes_body(shift_ref, rotation_ref, out_ref, rows):
    base_x = lax.axis_index("gx") * CX + shift_ref[0]
    base_y = lax.axis_index("gy") * CY + shift_ref[1]
    rows[...] = jnp.zeros(rows.shape, i32)
    for ex in range(PX):
        for ey in range(PY):
            a = (base_x + ex) & (APER - 1)
            b = (base_y + ey) & (APER - 1)
            rows[pl.ds(ex * PY + ey, 1), :APER] = rotation_ref[a, pl.ds(b, 1), :]
    value = rows[...].astype(f32)
    value = value + pltpu.roll(value, 32, 1)
    value = value + pltpu.roll(value, 64, 1)
    value = pltpu.roll(value, (128 - shift_ref[2]) & 127, 1)
    first = column_as_row(value)
    out_ref[...] = jnp.where(iota(value.shape, 0) == PLANES, first, value)


def column_as_row(value):
    column = jnp.broadcast_to(value[:, 0:1], value.shape)
    same = iota(value.shape, 0) == iota(value.shape, 1)
    return jnp.sum(jnp.where(same, column, 0.0), axis=0, keepdims=True)


def gather_x_faces(total, c, head_ref, tail_ref):
    head_ref[c, 0:PY] = total[0:PY]
    head_ref[c, PY : PY + 1] = total[PLANES:ROWS]
    tail_ref[c, 0:PY] = total[PLANES - PY : PLANES]
    tail_ref[c, PY : PY + 1] = total[PLANES:ROWS]


STEP = 96
Q2 = ROWS // 2


def slot_places(slots_ref, rows_q, rows_l):
    slots = slots_ref.shape[0] // 4
    label = slots_ref[pl.ds(3, slots, stride=4), :].astype(i32)
    rows_q[...] = (label >> 8).astype(f32)
    rows_l[...] = (label & 255).astype(f32)


def lane_onehot(rows_l, slot):
    step = iota((16, 128), 0).astype(f32).astype(bf16)
    lane = jnp.broadcast_to(rows_l[pl.ds(slot, 1), :], (16, 128)).astype(bf16) - step
    one = jnp.ones((16, 128), bf16)
    zero = jnp.zeros((16, 128), bf16)
    return jnp.concatenate([jnp.where(lane == float(16 * j), one, zero) for j in range(16)], axis=0)


def deposit_body(slots_ref, total_ref, head_ref, tail_ref, acc, rows_q, rows_l):
    slots = slots_ref.shape[0] // 4
    slot_places(slots_ref, rows_q, rows_l)
    acc[...] = jnp.zeros(acc.shape, f32)
    sub8 = iota((8, 128), 0)
    half = jnp.where(iota((16, 128), 0) >= 8, 1.0, 0.0).astype(bf16)
    zero = jnp.zeros((16, 128), bf16)

    def step(i, carry):
        weighted, depths = [], []
        for k in range(STEP):
            slot = i * STEP + k
            own = slots_ref[pl.ds(pl.multiple_of(i * STEP * 4, 8) + 4 * k, 4), :]
            own = jnp.concatenate([own, own], axis=0)
            high = own.astype(bf16).astype(f32)
            value = jnp.where(sub8 < 4, high, own - high)
            value = jnp.where(sub8 == 3, 1.0, jnp.where(sub8 == 7, 0.0, value))
            value = jnp.concatenate([value, value], axis=0).astype(bf16)
            q = jnp.broadcast_to(rows_q[pl.ds(slot, 1), :], (16, 128)).astype(bf16) - half
            weighted.append(
                jnp.concatenate(
                    [jnp.where(q == float(2 * j), value, zero) for j in range(12)], axis=0
                )
            )
            depths.append(lane_onehot(rows_l, slot))
        got = lax.dot_general(
            jnp.concatenate(weighted, axis=1),
            jnp.concatenate(depths, axis=1),
            (((1,), (1,)), ((), ())),
            preferred_element_type=f32,
        )
        acc[0] += got[:, :128]
        acc[1] += got[:, 128:]
        return carry

    lax.fori_loop(0, slots // STEP, step, 0)
    for c in range(4):
        for odd in range(2):
            total = acc[odd, pl.ds(c, Q2, stride=8), :]
            if c < 3:
                total = total + acc[odd, pl.ds(c + 4, Q2, stride=8), :]
            total_ref[c, pl.ds(odd, Q2, stride=2)] = total
        total_ref[c, ROWS:PADROWS] = jnp.zeros((PADROWS - ROWS, 128), f32)
        gather_x_faces(total_ref[c], c, head_ref, tail_ref)


def moved_lanes(row, first, count, shift):
    lane = iota(row.shape, 1)
    rolled = pltpu.roll(row, shift % 128, 1)
    return jnp.where((lane >= first) & (lane < first + count), rolled, 0.0)


def fold_x_body(total_ref, up_ref, down_ref, out_ref, head_ref, tail_ref):
    last = PLANES - PY
    for c in range(4):
        out_ref[c] = total_ref[c]
        out_ref[c, 0:PY] = total_ref[c, 0:PY] + down_ref[c, 0:PY]
        out_ref[c, last:PLANES] = total_ref[c, last:PLANES] + up_ref[c, 0:PY]
        out_ref[c, PLANES:ROWS] = (
            total_ref[c, PLANES:ROWS]
            + moved_lanes(up_ref[c, PY : PY + 1], last, PY, last)
            + moved_lanes(down_ref[c, PY : PY + 1], 0, PY, -last)
        )
        head_ref[c, 0:PX] = out_ref[c, pl.ds(0, PX, stride=PY)]
        head_ref[c, PX : PX + 1] = out_ref[c, PLANES:ROWS]
        tail_ref[c, 0:PX] = out_ref[c, pl.ds(CY, PX, stride=PY)]
        tail_ref[c, PX : PX + 1] = out_ref[c, PLANES:ROWS]


def fold_y_body(total_ref, up_ref, down_ref, out_ref, head_ref, tail_ref):
    lane = iota((1, 128), 1)
    for c in range(4):
        out_ref[c] = total_ref[c]
        out_ref[c, pl.ds(CY, PX, stride=PY)] = (
            total_ref[c, pl.ds(CY, PX, stride=PY)] + up_ref[c, 0:PX]
        )
        out_ref[c, pl.ds(0, PX, stride=PY)] = (
            total_ref[c, pl.ds(0, PX, stride=PY)] + down_ref[c, 0:PX]
        )
        up = pltpu.roll(up_ref[c, PX : PX + 1], CY, 1)
        down = pltpu.roll(down_ref[c, PX : PX + 1], 128 - CY, 1)
        edge = lane % PY
        out_ref[c, PLANES:ROWS] = (
            total_ref[c, PLANES:ROWS]
            + jnp.where((edge == CY) & (lane < PLANES), up, 0.0)
            + jnp.where((edge == 0) & (lane < PLANES), down, 0.0)
        )
        total = out_ref[c]
        head_ref[c : c + 1] = column_as_row(total)
        tail_ref[c : c + 1] = total[PLANES:ROWS]
        head_ref[4 + c : 5 + c] = jnp.zeros((1, 128), f32)
        tail_ref[4 + c : 5 + c] = jnp.zeros((1, 128), f32)


GROUP = 4


def collide_body(
    total_ref, up_ref, down_ref, axes_ref, units_ref, slots_ref, out_ref, flow_ref,
    cells, wide, found, rows_q, rows_l,
):
    slots = slots_ref.shape[0] // 4
    shape = (PADROWS, 128)
    row = iota(shape, 0)
    lane = iota(shape, 1)
    top = (row == PLANES) & (lane < PLANES)
    totals = []
    for c in range(4):
        own = total_ref[c]
        column = jnp.sum(
            jnp.where((row == lane) & (row < PLANES), down_ref[c : c + 1], 0.0),
            axis=1,
            keepdims=True,
        )
        own = own + jnp.where(lane == 0, column, 0.0)
        totals.append(own + jnp.where(top, up_ref[c : c + 1], 0.0))
    count = jnp.maximum(totals[3], 1.0)
    wide[...] = jnp.zeros(wide.shape, f32)

    def tabulate(value, line):
        cells[...] = value
        for odd in range(2):
            wide[odd, pl.ds(line, Q2, stride=8), :] = cells[pl.ds(odd, Q2, stride=2)]

    for c in range(3):
        mean = totals[c] / count
        for ex in range(CX):
            flow_ref[c, ex] = mean[ex * PY : ex * PY + CY]
        high = mean.astype(bf16).astype(f32)
        tabulate(high, c)
        tabulate(mean - high, c + 4)
    tabulate(axes_ref[...], 3)
    table = jnp.concatenate([wide[0], wide[1]], axis=1).astype(bf16)
    slot_places(slots_ref, rows_q, rows_l)
    sub8 = iota((8, 128), 0)

    def look(i, carry):
        for k in range(STEP // 2):
            pair = [i * STEP + 2 * k, i * STEP + 2 * k + 1]
            hot = jnp.concatenate([lane_onehot(rows_l, slot) for slot in pair], axis=1)
            read = jnp.dot(table, hot, preferred_element_type=f32)
            got = []
            for h in range(2):
                q = jnp.broadcast_to(rows_q[pl.ds(pair[h], 1), :], (8, 128))
                value = jnp.zeros((8, 128), f32)
                for j in range(Q2):
                    own = read[8 * j : 8 * j + 8, 128 * h : 128 * h + 128]
                    value = jnp.where(q == float(j), own, value)
                got.append(value + pltpu.roll(value, 4, 0))
            place = pl.multiple_of((i * STEP + 2 * k) * 4, 8)
            found[pl.ds(place, 8), :] = jnp.where(sub8 < 4, got[0], got[1])
        return carry

    lax.fori_loop(0, slots // STEP, look, 0)
    units = [jnp.broadcast_to(units_ref[c : c + 1], (8, 128)) for c in range(3)]

    def turn(i, carry):
        rank = i // (16 // GROUP)
        for k in range(GROUP):
            source = pl.multiple_of((i % (16 // GROUP)) * (8 * GROUP) + 8 * k, 8)
            place = source * 12 + rank * 4
            which = found[pl.ds(place + 3, 8, stride=12), :].astype(i32)
            n = [jnp.take_along_axis(units[c], which, axis=1) for c in range(3)]
            u = [found[pl.ds(place + c, 8, stride=12), :] for c in range(3)]
            w = [slots_ref[pl.ds(place + c, 8, stride=12), :] - u[c] for c in range(3)]
            inner = n[0] * w[0] + n[1] * w[1] + n[2] * w[2]
            crossed = [
                n[1] * w[2] - n[2] * w[1],
                n[2] * w[0] - n[0] * w[2],
                n[0] * w[1] - n[1] * w[0],
            ]
            for c in range(3):
                out_ref[rank, c, pl.ds(source, 8), :] = (
                    u[c]
                    + w[c] * angle_cosine
                    + crossed[c] * angle_sine
                    + n[c] * inner * (1.0 - angle_cosine)
                )
        return carry

    lax.fori_loop(0, MOST * 16 // GROUP, turn, 0)


def both_ways(head, tail, axis):
    count = lax.axis_size(axis)
    up = lax.ppermute(head, axis, [((i + 1) % count, i) for i in range(count)])
    down = lax.ppermute(tail, axis, [(i, (i + 1) % count) for i in range(count)])
    return up, down


def shards(velocity, cell_index, block_target, rotation_axis, grid_shift):
    devices = 128
    shape = jax.ShapeDtypeStruct
    vmem = pl.BlockSpec(memory_space=pltpu.VMEM)
    smem = pl.BlockSpec(memory_space=pltpu.SMEM)
    send = call(pack_body, shape((devices * MOST * 4, 128), f32), name="pack")(
        block_target.reshape(1, -1), jnp.transpose(velocity, (1, 0, 2)), cell_index
    )
    axes = call(
        axes_body,
        shape((PADROWS, 128), f32),
        in_specs=[smem, vmem],
        scratch_shapes=[pltpu.VMEM((PADROWS, 128), i32)],
        name="axes",
    )(grid_shift, rotation_axis)
    units = jnp.pad(axis_table(), ((0, 5), (0, 128 - NAX)))
    slots = lax.all_to_all(
        send.reshape(devices, MOST, 4, 128), ("gx", "gy", "gz"), split_axis=0, concat_axis=0, tiled=True
    ).reshape(devices * MOST * 4, 128)
    total_shape = shape((4, PADROWS, 128), f32)
    x_face = shape((4, 16, 128), f32)
    y_face = shape((4, 8, 128), f32)
    z_face = shape((8, 128), f32)
    total, head, tail = call(
        deposit_body,
        [total_shape, x_face, x_face],
        scratch_shapes=[
            pltpu.VMEM((2, 192, 128), f32),
            pltpu.VMEM((devices * MOST, 128), f32),
            pltpu.VMEM((devices * MOST, 128), f32),
        ],
        name="deposit",
    )(slots)
    up, down = both_ways(head, tail, "gx")
    total, head, tail = call(fold_x_body, [total_shape, y_face, y_face], name="fold_x")(
        total, up, down
    )
    up, down = both_ways(head, tail, "gy")
    total, head, tail = call(fold_y_body, [total_shape, z_face, z_face], name="fold_y")(
        total, up, down
    )
    up, down = both_ways(head, tail, "gz")
    updated, cell_flow = call(
        collide_body,
        [shape((MOST, 3, devices, 128), f32), shape((3, CX, CY, CZ), f32)],
        scratch_shapes=[
            pltpu.VMEM((PADROWS, 128), f32),
            pltpu.VMEM((2, Q2 * 8, 128), f32),
            pltpu.VMEM((devices * MOST * 4, 128), f32),
            pltpu.VMEM((devices * MOST, 128), f32),
            pltpu.VMEM((devices * MOST, 128), f32),
        ],
        name="collide",
    )(total, up, down, axes, units, slots)
    return jnp.transpose(updated, (2, 0, 1, 3))[None], cell_flow


def solution(mesh):
    return jax.shard_map(
        shards,
        mesh=mesh,
        in_specs=(
            P(("gx", "gy", "gz"), None, None),
            P(("gx", "gy", "gz"), None),
            P(("gx", "gy", "gz"), None),
            P(),
            P(),
        ),
        out_specs=(P(("gx", "gy", "gz"), None, None, None, None), P(None, "gx", "gy", "gz")),
        check_vma=False,
    )
```

```python
import functools

import jax
import jax.numpy as jnp
from jax import lax
from jax.experimental import pallas as pl
from jax.experimental.pallas import tpu as pltpu
from jax.sharding import PartitionSpec as P

CX = 4
CY = 8
CZ = 128
NAX = 64
APER = 32
MOST = 3
PX = CX + 1
PY = CY + 1
PLANES = PX * PY
ROWS = PLANES + 1
PADROWS = 48
EMPTY = 6400.0

angle_cosine = -0.6427876096865393
angle_sine = 0.766044443118978

f32 = jnp.float32
bf16 = jnp.bfloat16
i32 = jnp.int32


def iota(shape, dim):
    return lax.broadcasted_iota(i32, shape, dim)


def axis_table():
    counter = jnp.arange(NAX, dtype=f32) + 0.5
    height = 1.0 - 2.0 * counter / NAX
    radius = jnp.sqrt(jnp.maximum(1.0 - height * height, 0.0))
    turning = counter * 2.399963229728653
    return jnp.stack([radius * jnp.cos(turning), radius * jnp.sin(turning), height])


def split3(value):
    high = value.astype(bf16)
    rest = value - high.astype(f32)
    middle = rest.astype(bf16)
    return high, middle, (rest - middle.astype(f32)).astype(bf16)


def call(body, out_shape, **kw):
    return pl.pallas_call(
        body,
        out_shape=out_shape,
        compiler_params=pltpu.CompilerParams(vmem_limit_bytes=48 * 1024 * 1024),
        **kw,
    )


def pack_body(target_hbm, velocity_hbm, index_hbm, out_ref, target_ref, velocity_ref, index_ref, sems):
    sources = (target_hbm, index_hbm, velocity_hbm)
    sinks = (target_ref, index_ref, velocity_ref)
    copies = [
        pltpu.make_async_copy(source, sink, sems.at[k])
        for k, (source, sink) in enumerate(zip(sources, sinks))
    ]
    for copy in copies:
        copy.start()
    bricks = 128
    blocks = target_ref.shape[1]
    copies[0].wait()
    target = jnp.broadcast_to(target_ref[...], (bricks, blocks))
    onehot = target == iota((bricks, blocks), 0)
    onehot_bf = jnp.where(onehot, 1.0, 0.0).astype(bf16)
    earlier = jnp.where(iota((blocks, blocks), 0) < iota((blocks, blocks), 1), 1.0, 0.0)
    before = jnp.dot(onehot_bf, earlier.astype(bf16), preferred_element_type=f32)
    places = [
        jnp.where(onehot & (before == float(rank)), 1.0, 0.0).astype(bf16) for rank in range(MOST)
    ]
    copies[1].wait()
    index = index_ref[...]
    plane = (index * 8129) >> 20
    depth = index - plane * (CZ + 1)
    top = depth == CZ
    label = jnp.where(top, PLANES * 128 + plane, plane * 128 + depth)
    label = label.astype(f32) - EMPTY
    copies[2].wait()
    splits = split3(jnp.concatenate([velocity_ref[c] for c in range(3)] + [label], axis=1))
    for rank in range(MOST):
        moved = sum(jnp.dot(places[rank], s, preferred_element_type=f32) for s in reversed(splits))
        for c in range(4):
            value = moved[:, c * 128 : (c + 1) * 128]
            if c == 3:
                value = value + EMPTY
            out_ref[pl.ds(rank * 4 + c, bricks, stride=4 * MOST), :] = value


def axes_body(shift_ref, rotation_ref, out_ref, rows):
    base_x = lax.axis_index("gx") * CX + shift_ref[0]
    base_y = lax.axis_index("gy") * CY + shift_ref[1]
    rows[...] = jnp.zeros(rows.shape, i32)
    for ex in range(PX):
        for ey in range(PY):
            a = (base_x + ex) & (APER - 1)
            b = (base_y + ey) & (APER - 1)
            rows[pl.ds(ex * PY + ey, 1), :APER] = rotation_ref[a, pl.ds(b, 1), :]
    value = rows[...].astype(f32)
    value = value + pltpu.roll(value, 32, 1)
    value = value + pltpu.roll(value, 64, 1)
    value = pltpu.roll(value, (128 - shift_ref[2]) & 127, 1)
    first = column_as_row(value)
    out_ref[...] = jnp.where(iota(value.shape, 0) == PLANES, first, value)


def column_as_row(value):
    column = jnp.broadcast_to(value[:, 0:1], value.shape)
    same = iota(value.shape, 0) == iota(value.shape, 1)
    return jnp.sum(jnp.where(same, column, 0.0), axis=0, keepdims=True)


def gather_x_faces(total, c, head_ref, tail_ref):
    head_ref[c, 0:PY] = total[0:PY]
    head_ref[c, PY : PY + 1] = total[PLANES:ROWS]
    tail_ref[c, 0:PY] = total[PLANES - PY : PLANES]
    tail_ref[c, PY : PY + 1] = total[PLANES:ROWS]


DEPOSIT_STEP = 128
STEP = 96
Q2 = ROWS // 2


def slot_places(slots_ref, rows_q, rows_l):
    slots = slots_ref.shape[0] // 4
    label = slots_ref[pl.ds(3, slots, stride=4), :].astype(i32)
    rows_q[...] = (label >> 8).astype(rows_q.dtype)
    rows_l[...] = jnp.where(label >= PADROWS * 128, 512, label & 255).astype(f32)


def lane_onehot(rows_l, slot):
    step = iota((16, 128), 0).astype(f32).astype(bf16)
    lane = jnp.broadcast_to(rows_l[pl.ds(slot, 1), :], (16, 128)).astype(bf16) - step
    one = jnp.ones((16, 128), bf16)
    zero = jnp.zeros((16, 128), bf16)
    return jnp.concatenate([jnp.where(lane == float(16 * j), one, zero) for j in range(16)], axis=0)


def deposit_body(slots_ref, total_ref, head_ref, tail_ref, acc, rows_q, rows_l):
    slots = slots_ref.shape[0] // 4
    slot_places(slots_ref, rows_q, rows_l)
    acc[...] = jnp.zeros(acc.shape, f32)
    sub8 = iota((8, 128), 0)
    half = jnp.where(iota((16, 128), 0) >= 8, 1.0, 0.0).astype(bf16)
    zero = jnp.zeros((16, 128), bf16)

    def step(i, carry):
        weighted, depths = [], []
        for k in range(DEPOSIT_STEP):
            slot = i * DEPOSIT_STEP + k
            own = slots_ref[pl.ds(pl.multiple_of(i * DEPOSIT_STEP * 4, 8) + 4 * k, 4), :]
            own = jnp.concatenate([own, own], axis=0)
            high = own.astype(bf16).astype(f32)
            value = jnp.where(sub8 < 4, high, own - high)
            value = jnp.where(sub8 == 3, 1.0, jnp.where(sub8 == 7, 0.0, value))
            value = jnp.concatenate([value, value], axis=0).astype(bf16)
            q = jnp.broadcast_to(rows_q[pl.ds(slot, 1), :], (16, 128)).astype(bf16) - half
            weighted.append(
                jnp.concatenate(
                    [jnp.where(q == float(2 * j), value, zero) for j in range(12)], axis=0
                )
            )
            depths.append(lane_onehot(rows_l, slot).astype(jnp.float8_e4m3fn))
        got = lax.dot_general(
            jnp.concatenate(weighted, axis=1),
            jnp.concatenate(depths, axis=1),
            (((1,), (1,)), ((), ())),
            preferred_element_type=f32,
        )
        acc[0] += got[:, :128]
        acc[1] += got[:, 128:]
        return carry

    lax.fori_loop(0, slots // DEPOSIT_STEP, step, 0)
    for c in range(4):
        for odd in range(2):
            total = acc[odd, pl.ds(c, Q2, stride=8), :]
            if c < 3:
                total = total + acc[odd, pl.ds(c + 4, Q2, stride=8), :]
            total_ref[c, pl.ds(odd, Q2, stride=2)] = total
        total_ref[c, ROWS:PADROWS] = jnp.zeros((PADROWS - ROWS, 128), f32)
        gather_x_faces(total_ref[c], c, head_ref, tail_ref)


def moved_lanes(row, first, count, shift):
    lane = iota(row.shape, 1)
    rolled = pltpu.roll(row, shift % 128, 1)
    return jnp.where((lane >= first) & (lane < first + count), rolled, 0.0)


def fold_x_body(total_ref, up_ref, down_ref, out_ref, head_ref, tail_ref):
    last = PLANES - PY
    for c in range(4):
        out_ref[c] = total_ref[c]
        out_ref[c, 0:PY] = total_ref[c, 0:PY] + down_ref[c, 0:PY]
        out_ref[c, last:PLANES] = total_ref[c, last:PLANES] + up_ref[c, 0:PY]
        out_ref[c, PLANES:ROWS] = (
            total_ref[c, PLANES:ROWS]
            + moved_lanes(up_ref[c, PY : PY + 1], last, PY, last)
            + moved_lanes(down_ref[c, PY : PY + 1], 0, PY, -last)
        )
        head_ref[c, 0:PX] = out_ref[c, pl.ds(0, PX, stride=PY)]
        head_ref[c, PX : PX + 1] = out_ref[c, PLANES:ROWS]
        tail_ref[c, 0:PX] = out_ref[c, pl.ds(CY, PX, stride=PY)]
        tail_ref[c, PX : PX + 1] = out_ref[c, PLANES:ROWS]


def fold_y_body(total_ref, up_ref, down_ref, out_ref, head_ref, tail_ref):
    lane = iota((1, 128), 1)
    for c in range(4):
        out_ref[c] = total_ref[c]
        out_ref[c, pl.ds(CY, PX, stride=PY)] = (
            total_ref[c, pl.ds(CY, PX, stride=PY)] + up_ref[c, 0:PX]
        )
        out_ref[c, pl.ds(0, PX, stride=PY)] = (
            total_ref[c, pl.ds(0, PX, stride=PY)] + down_ref[c, 0:PX]
        )
        up = pltpu.roll(up_ref[c, PX : PX + 1], CY, 1)
        down = pltpu.roll(down_ref[c, PX : PX + 1], 128 - CY, 1)
        edge = lane % PY
        out_ref[c, PLANES:ROWS] = (
            total_ref[c, PLANES:ROWS]
            + jnp.where((edge == CY) & (lane < PLANES), up, 0.0)
            + jnp.where((edge == 0) & (lane < PLANES), down, 0.0)
        )
        total = out_ref[c]
        head_ref[c : c + 1] = column_as_row(total)
        tail_ref[c : c + 1] = total[PLANES:ROWS]
        head_ref[4 + c : 5 + c] = jnp.zeros((1, 128), f32)
        tail_ref[4 + c : 5 + c] = jnp.zeros((1, 128), f32)


def select_row(rows, bits):
    for bit in bits:
        rows = [
            jnp.where(bit, rows[j + 1], rows[j]) if j + 1 < len(rows) else rows[j]
            for j in range(0, len(rows), 2)
        ]
    return rows[0]


def collide_body(
    total_ref, up_ref, down_ref, axes_ref, units_ref, slots_ref, out_hbm, flow_ref,
    cells, wide, found, rows_q, rows_l, out_ref, sems,
):
    slots = slots_ref.shape[0] // 4
    shape = (PADROWS, 128)
    row = iota(shape, 0)
    lane = iota(shape, 1)
    top = (row == PLANES) & (lane < PLANES)
    totals = []
    for c in range(4):
        own = total_ref[c]
        column = jnp.sum(
            jnp.where((row == lane) & (row < PLANES), down_ref[c : c + 1], 0.0),
            axis=1,
            keepdims=True,
        )
        own = own + jnp.where(lane == 0, column, 0.0)
        totals.append(own + jnp.where(top, up_ref[c : c + 1], 0.0))
    count = jnp.maximum(totals[3], 1.0)
    wide[...] = jnp.zeros(wide.shape, f32)

    def tabulate(value, line):
        cells[...] = value
        for odd in range(2):
            wide[odd, pl.ds(line, Q2, stride=8), :] = cells[pl.ds(odd, Q2, stride=2)]

    for c in range(3):
        mean = totals[c] / count
        for ex in range(CX):
            flow_ref[c, ex] = mean[ex * PY : ex * PY + CY]
        high = mean.astype(bf16).astype(f32)
        tabulate(high, c)
        tabulate(mean - high, c + 4)
    tabulate(axes_ref[...], 3)
    table = jnp.concatenate([wide[0], wide[1]], axis=1).astype(bf16)
    slot_places(slots_ref, rows_q, rows_l)
    sub8 = iota((8, 128), 0)

    units = [jnp.broadcast_to(units_ref[c : c + 1], (8, 128)) for c in range(3)]

    def look(i):
        for k in range(STEP // 2):
            pair = [i * STEP + 2 * k, i * STEP + 2 * k + 1]
            hot = jnp.concatenate([lane_onehot(rows_l, slot) for slot in pair], axis=1)
            read = jnp.dot(table, hot, preferred_element_type=f32)
            got = []
            for h in range(2):
                q = jnp.broadcast_to(rows_q[pl.ds(pair[h], 1), :], (8, 128))
                bits = [(q & (1 << b)) != 0 for b in range(5)]
                lines = [read[8 * j : 8 * j + 8, 128 * h : 128 * h + 128] for j in range(Q2)]
                value = select_row(lines, bits)
                got.append(value + pltpu.roll(value, 4, 0))
            found[pl.ds((i * STEP + 2 * k) * 4, 8), :] = jnp.where(sub8 < 4, got[0], got[1])

    senders = STEP // MOST

    def copy(i):
        part = pl.ds(i * senders, senders)
        return pltpu.make_async_copy(
            out_ref.at[:, :, part, :], out_hbm.at[:, :, part, :], sems.at[i]
        )

    def turn(i):
        for rank in range(MOST):
            for k in range(senders // 8):
                source = i * senders + 8 * k
                place = (source * MOST + rank) * 4
                which = found[pl.ds(place + 3, 8, stride=12), :].astype(i32)
                n = [jnp.take_along_axis(units[c], which, axis=1) for c in range(3)]
                u = [found[pl.ds(place + c, 8, stride=12), :] for c in range(3)]
                w = [slots_ref[pl.ds(place + c, 8, stride=12), :] - u[c] for c in range(3)]
                inner = n[0] * w[0] + n[1] * w[1] + n[2] * w[2]
                crossed = [
                    n[1] * w[2] - n[2] * w[1],
                    n[2] * w[0] - n[0] * w[2],
                    n[0] * w[1] - n[1] * w[0],
                ]
                for c in range(3):
                    out_ref[rank, c, pl.ds(source, 8), :] = (
                        u[c]
                        + w[c] * angle_cosine
                        + crossed[c] * angle_sine
                        + n[c] * inner * (1.0 - angle_cosine)
                    )
        copy(i).start()

    steps = slots // STEP
    for i in range(steps):
        if i > 0:
            turn(i - 1)
        look(i)
    turn(steps - 1)
    for i in range(steps):
        copy(i).wait()


def both_ways(head, tail, axis):
    count = lax.axis_size(axis)
    up = lax.ppermute(head, axis, [((i + 1) % count, i) for i in range(count)])
    down = lax.ppermute(tail, axis, [(i, (i + 1) % count) for i in range(count)])
    return up, down


def shards(velocity, cell_index, block_target, rotation_axis, grid_shift):
    devices = 128
    shape = jax.ShapeDtypeStruct
    vmem = pl.BlockSpec(memory_space=pltpu.VMEM)
    smem = pl.BlockSpec(memory_space=pltpu.SMEM)
    hbm = pl.BlockSpec(memory_space=pltpu.HBM)
    blocks = velocity.shape[0]
    send = call(
        pack_body,
        shape((devices * MOST * 4, 128), f32),
        in_specs=[hbm, hbm, hbm],
        scratch_shapes=[
            pltpu.VMEM((1, blocks), i32),
            pltpu.VMEM((3, blocks, 128), f32),
            pltpu.VMEM((blocks, 128), i32),
            pltpu.SemaphoreType.DMA((3,)),
        ],
        name="pack",
    )(
        *(
            pltpu.with_memory_space_constraint(x, pltpu.HBM)
            for x in (block_target.reshape(1, -1), jnp.transpose(velocity, (1, 0, 2)), cell_index)
        )
    )
    axes = call(
        axes_body,
        shape((PADROWS, 128), f32),
        in_specs=[smem, vmem],
        scratch_shapes=[pltpu.VMEM((PADROWS, 128), i32)],
        name="axes",
    )(grid_shift, rotation_axis)
    units = jnp.pad(axis_table(), ((0, 5), (0, 128 - NAX)))
    slots = lax.all_to_all(
        send.reshape(devices, MOST, 4, 128), ("gx", "gy", "gz"), split_axis=0, concat_axis=0, tiled=True
    ).reshape(devices * MOST * 4, 128)
    total_shape = shape((4, PADROWS, 128), f32)
    x_face = shape((4, 16, 128), f32)
    y_face = shape((4, 8, 128), f32)
    z_face = shape((8, 128), f32)
    total, head, tail = call(
        deposit_body,
        [total_shape, x_face, x_face],
        scratch_shapes=[
            pltpu.VMEM((2, 192, 128), f32),
            pltpu.VMEM((devices * MOST, 128), f32),
            pltpu.VMEM((devices * MOST, 128), f32),
        ],
        name="deposit",
    )(slots)
    up, down = both_ways(head, tail, "gx")
    total, head, tail = call(fold_x_body, [total_shape, y_face, y_face], name="fold_x")(
        total, up, down
    )
    up, down = both_ways(head, tail, "gy")
    total, head, tail = call(fold_y_body, [total_shape, z_face, z_face], name="fold_y")(
        total, up, down
    )
    up, down = both_ways(head, tail, "gz")
    updated, cell_flow = call(
        collide_body,
        [shape((MOST, 3, devices, 128), f32), shape((3, CX, CY, CZ), f32)],
        out_specs=[hbm, vmem],
        scratch_shapes=[
            pltpu.VMEM((PADROWS, 128), f32),
            pltpu.VMEM((2, Q2 * 8, 128), f32),
            pltpu.VMEM((devices * MOST * 4, 128), f32),
            pltpu.VMEM((devices * MOST, 128), i32),
            pltpu.VMEM((devices * MOST, 128), f32),
            pltpu.VMEM((MOST, 3, devices, 128), f32),
            pltpu.SemaphoreType.DMA((devices * MOST // STEP,)),
        ],
        name="collide",
    )(total, up, down, axes, units, slots)
    return jnp.transpose(updated, (2, 0, 1, 3))[None], cell_flow


def solution(mesh):
    return jax.shard_map(
        shards,
        mesh=mesh,
        in_specs=(
            P(("gx", "gy", "gz"), None, None),
            P(("gx", "gy", "gz"), None),
            P(("gx", "gy", "gz"), None),
            P(),
            P(),
        ),
        out_specs=(P(("gx", "gy", "gz"), None, None, None, None), P(None, "gx", "gy", "gz")),
        check_vma=False,
    )
```

```python
import functools

import jax
import jax.numpy as jnp
from jax import lax
from jax.experimental import pallas as pl
from jax.experimental.pallas import tpu as pltpu
from jax.sharding import PartitionSpec as P

CX = 4
CY = 8
CZ = 128
NAX = 64
APER = 32
MOST = 3
PX = CX + 1
PY = CY + 1
PLANES = PX * PY
ROWS = PLANES + 1
PADROWS = 48
EMPTY = 6400.0

angle_cosine = -0.6427876096865393
angle_sine = 0.766044443118978

f32 = jnp.float32
bf16 = jnp.bfloat16
i32 = jnp.int32


def iota(shape, dim):
    return lax.broadcasted_iota(i32, shape, dim)


def axis_table():
    counter = jnp.arange(NAX, dtype=f32) + 0.5
    height = 1.0 - 2.0 * counter / NAX
    radius = jnp.sqrt(jnp.maximum(1.0 - height * height, 0.0))
    turning = counter * 2.399963229728653
    return jnp.stack([radius * jnp.cos(turning), radius * jnp.sin(turning), height])


def split3(value):
    high = value.astype(bf16)
    rest = value - high.astype(f32)
    middle = rest.astype(bf16)
    return high, middle, (rest - middle.astype(f32)).astype(bf16)


def call(body, out_shape, **kw):
    return pl.pallas_call(
        body,
        out_shape=out_shape,
        compiler_params=pltpu.CompilerParams(vmem_limit_bytes=48 * 1024 * 1024),
        **kw,
    )


def pack_body(target_hbm, velocity_hbm, index_hbm, out_ref, target_ref, velocity_ref, index_ref, sems):
    sources = (target_hbm, index_hbm, velocity_hbm)
    sinks = (target_ref, index_ref, velocity_ref)
    copies = [
        pltpu.make_async_copy(source, sink, sems.at[k])
        for k, (source, sink) in enumerate(zip(sources, sinks))
    ]
    for copy in copies:
        copy.start()
    bricks = 128
    blocks = target_ref.shape[1]
    copies[0].wait()
    target = jnp.broadcast_to(target_ref[...], (bricks, blocks))
    onehot = target == iota((bricks, blocks), 0)
    onehot_bf = jnp.where(onehot, 1.0, 0.0).astype(bf16)
    earlier = jnp.where(iota((blocks, blocks), 0) < iota((blocks, blocks), 1), 1.0, 0.0)
    before = jnp.dot(onehot_bf, earlier.astype(bf16), preferred_element_type=f32)
    places = [
        jnp.where(onehot & (before == float(rank)), 1.0, 0.0).astype(bf16) for rank in range(MOST)
    ]
    copies[1].wait()
    index = index_ref[...]
    plane = (index * 8129) >> 20
    depth = index - plane * (CZ + 1)
    top = depth == CZ
    label = jnp.where(top, PLANES * 128 + plane, plane * 128 + depth)
    label = label.astype(f32) - EMPTY
    copies[2].wait()
    splits = split3(jnp.concatenate([velocity_ref[c] for c in range(3)] + [label], axis=1))
    for rank in range(MOST):
        moved = sum(jnp.dot(places[rank], s, preferred_element_type=f32) for s in reversed(splits))
        for c in range(4):
            value = moved[:, c * 128 : (c + 1) * 128]
            if c == 3:
                value = value + EMPTY
            out_ref[pl.ds(rank * 4 + c, bricks, stride=4 * MOST), :] = value


def axes_body(shift_ref, rotation_ref, out_ref, rows):
    base_x = lax.axis_index("gx") * CX + shift_ref[0]
    base_y = lax.axis_index("gy") * CY + shift_ref[1]
    rows[...] = jnp.zeros(rows.shape, i32)
    for ex in range(PX):
        for ey in range(PY):
            a = (base_x + ex) & (APER - 1)
            b = (base_y + ey) & (APER - 1)
            rows[pl.ds(ex * PY + ey, 1), :APER] = rotation_ref[a, pl.ds(b, 1), :]
    value = rows[...].astype(f32)
    value = value + pltpu.roll(value, 32, 1)
    value = value + pltpu.roll(value, 64, 1)
    value = pltpu.roll(value, (128 - shift_ref[2]) & 127, 1)
    first = column_as_row(value)
    out_ref[...] = jnp.where(iota(value.shape, 0) == PLANES, first, value)


def column_as_row(value):
    column = jnp.broadcast_to(value[:, 0:1], value.shape)
    same = iota(value.shape, 0) == iota(value.shape, 1)
    return jnp.sum(jnp.where(same, column, 0.0), axis=0, keepdims=True)


def gather_x_faces(total, c, head_ref, tail_ref):
    head_ref[c, 0:PY] = total[0:PY]
    head_ref[c, PY : PY + 1] = total[PLANES:ROWS]
    tail_ref[c, 0:PY] = total[PLANES - PY : PLANES]
    tail_ref[c, PY : PY + 1] = total[PLANES:ROWS]


DEPOSIT_STEP = 128
Q2 = ROWS // 2


def slot_places(slots_ref, rows_q, rows_l):
    slots = slots_ref.shape[0] // 4
    label = slots_ref[pl.ds(3, slots, stride=4), :].astype(i32)
    rows_q[...] = (label >> 8).astype(rows_q.dtype)
    rows_l[...] = jnp.where(label >= PADROWS * 128, 512, label & 255).astype(f32)


def lane_onehot(rows_l, slot):
    step = iota((16, 128), 0).astype(f32).astype(bf16)
    lane = jnp.broadcast_to(rows_l[pl.ds(slot, 1), :], (16, 128)).astype(bf16) - step
    one = jnp.ones((16, 128), bf16)
    zero = jnp.zeros((16, 128), bf16)
    return jnp.concatenate([jnp.where(lane == float(16 * j), one, zero) for j in range(16)], axis=0)


def deposit_body(slots_ref, total_ref, head_ref, tail_ref, acc, rows_q, rows_l):
    slots = slots_ref.shape[0] // 4
    slot_places(slots_ref, rows_q, rows_l)
    acc[...] = jnp.zeros(acc.shape, f32)
    sub8 = iota((8, 128), 0)
    half = jnp.where(iota((16, 128), 0) >= 8, 1.0, 0.0).astype(bf16)
    zero = jnp.zeros((16, 128), bf16)

    def step(i, carry):
        weighted, depths = [], []
        for k in range(DEPOSIT_STEP):
            slot = i * DEPOSIT_STEP + k
            own = slots_ref[pl.ds(pl.multiple_of(i * DEPOSIT_STEP * 4, 8) + 4 * k, 4), :]
            own = jnp.concatenate([own, own], axis=0)
            high = own.astype(bf16).astype(f32)
            value = jnp.where(sub8 < 4, high, own - high)
            value = jnp.where(sub8 == 3, 1.0, jnp.where(sub8 == 7, 0.0, value))
            value = jnp.concatenate([value, value], axis=0).astype(bf16)
            q = jnp.broadcast_to(rows_q[pl.ds(slot, 1), :], (16, 128)).astype(bf16) - half
            weighted.append(
                jnp.concatenate(
                    [jnp.where(q == float(2 * j), value, zero) for j in range(12)], axis=0
                )
            )
            depths.append(lane_onehot(rows_l, slot).astype(jnp.float8_e4m3fn))
        got = lax.dot_general(
            jnp.concatenate(weighted, axis=1),
            jnp.concatenate(depths, axis=1),
            (((1,), (1,)), ((), ())),
            preferred_element_type=f32,
        )
        acc[0] += got[:, :128]
        acc[1] += got[:, 128:]
        return carry

    lax.fori_loop(0, slots // DEPOSIT_STEP, step, 0)
    for c in range(4):
        for odd in range(2):
            total = acc[odd, pl.ds(c, Q2, stride=8), :]
            if c < 3:
                total = total + acc[odd, pl.ds(c + 4, Q2, stride=8), :]
            total_ref[c, pl.ds(odd, Q2, stride=2)] = total
        total_ref[c, ROWS:PADROWS] = jnp.zeros((PADROWS - ROWS, 128), f32)
        gather_x_faces(total_ref[c], c, head_ref, tail_ref)


def moved_lanes(row, first, count, shift):
    lane = iota(row.shape, 1)
    rolled = pltpu.roll(row, shift % 128, 1)
    return jnp.where((lane >= first) & (lane < first + count), rolled, 0.0)


def fold_x_body(total_ref, up_ref, down_ref, out_ref, head_ref, tail_ref):
    last = PLANES - PY
    for c in range(4):
        out_ref[c] = total_ref[c]
        out_ref[c, 0:PY] = total_ref[c, 0:PY] + down_ref[c, 0:PY]
        out_ref[c, last:PLANES] = total_ref[c, last:PLANES] + up_ref[c, 0:PY]
        out_ref[c, PLANES:ROWS] = (
            total_ref[c, PLANES:ROWS]
            + moved_lanes(up_ref[c, PY : PY + 1], last, PY, last)
            + moved_lanes(down_ref[c, PY : PY + 1], 0, PY, -last)
        )
        head_ref[c, 0:PX] = out_ref[c, pl.ds(0, PX, stride=PY)]
        head_ref[c, PX : PX + 1] = out_ref[c, PLANES:ROWS]
        tail_ref[c, 0:PX] = out_ref[c, pl.ds(CY, PX, stride=PY)]
        tail_ref[c, PX : PX + 1] = out_ref[c, PLANES:ROWS]


def fold_y_body(total_ref, up_ref, down_ref, out_ref, head_ref, tail_ref):
    lane = iota((1, 128), 1)
    for c in range(4):
        out_ref[c] = total_ref[c]
        out_ref[c, pl.ds(CY, PX, stride=PY)] = (
            total_ref[c, pl.ds(CY, PX, stride=PY)] + up_ref[c, 0:PX]
        )
        out_ref[c, pl.ds(0, PX, stride=PY)] = (
            total_ref[c, pl.ds(0, PX, stride=PY)] + down_ref[c, 0:PX]
        )
        up = pltpu.roll(up_ref[c, PX : PX + 1], CY, 1)
        down = pltpu.roll(down_ref[c, PX : PX + 1], 128 - CY, 1)
        edge = lane % PY
        out_ref[c, PLANES:ROWS] = (
            total_ref[c, PLANES:ROWS]
            + jnp.where((edge == CY) & (lane < PLANES), up, 0.0)
            + jnp.where((edge == 0) & (lane < PLANES), down, 0.0)
        )
        total = out_ref[c]
        head_ref[c : c + 1] = column_as_row(total)
        tail_ref[c : c + 1] = total[PLANES:ROWS]
        head_ref[4 + c : 5 + c] = jnp.zeros((1, 128), f32)
        tail_ref[4 + c : 5 + c] = jnp.zeros((1, 128), f32)


def select_row(rows, bits):
    for bit in bits:
        rows = [
            jnp.where(bit, rows[j + 1], rows[j]) if j + 1 < len(rows) else rows[j]
            for j in range(0, len(rows), 2)
        ]
    return rows[0]


def look_body(total_ref, axes_ref, slots_ref, found, cells, wide, rows_q, rows_l):
    slots = slots_ref.shape[0] // 4
    count = jnp.maximum(total_ref[3], 1.0)
    wide[...] = jnp.zeros(wide.shape, f32)

    def tabulate(value, line):
        cells[...] = value
        for odd in range(2):
            wide[odd, pl.ds(line, Q2, stride=8), :] = cells[pl.ds(odd, Q2, stride=2)]

    for c in range(3):
        mean = total_ref[c] / count
        high = mean.astype(bf16).astype(f32)
        tabulate(high, c)
        tabulate(mean - high, c + 4)
    tabulate(axes_ref[...], 3)
    table = jnp.concatenate([wide[0], wide[1]], axis=1).astype(bf16)
    slot_places(slots_ref, rows_q, rows_l)
    sub8 = iota((8, 128), 0)
    for k in range(slots // 2):
        pair = [2 * k, 2 * k + 1]
        hot = jnp.concatenate([lane_onehot(rows_l, slot) for slot in pair], axis=1)
        read = jnp.dot(table, hot, preferred_element_type=f32)
        got = []
        for h in range(2):
            q = jnp.broadcast_to(rows_q[pl.ds(pair[h], 1), :], (8, 128))
            bits = [(q & (1 << b)) != 0 for b in range(5)]
            lines = [read[8 * j : 8 * j + 8, 128 * h : 128 * h + 128] for j in range(Q2)]
            value = select_row(lines, bits)
            got.append(value + pltpu.roll(value, 4, 0))
        found[pl.ds(8 * k, 8), :] = jnp.where(sub8 < 4, got[0], got[1])


SENDERS = 32


def turn_body(
    total_ref, up_ref, down_ref, units_ref, slots_ref, found, out_hbm, flow_ref, out_ref, sems
):
    devices = out_ref.shape[2]
    shape = (PADROWS, 128)
    row = iota(shape, 0)
    lane = iota(shape, 1)
    top = (row == PLANES) & (lane < PLANES)
    totals = []
    for c in range(4):
        own = total_ref[c]
        column = jnp.sum(
            jnp.where((row == lane) & (row < PLANES), down_ref[c : c + 1], 0.0),
            axis=1,
            keepdims=True,
        )
        own = own + jnp.where(lane == 0, column, 0.0)
        totals.append(own + jnp.where(top, up_ref[c : c + 1], 0.0))
    count = jnp.maximum(totals[3], 1.0)
    rims = []
    for c in range(3):
        mean = totals[c] / count
        for ex in range(CX):
            flow_ref[c, ex] = mean[ex * PY : ex * PY + CY]
        low = pltpu.roll(column_as_row(mean), 64, 1)
        rim = jnp.where(iota((1, 128), 1) < 64, mean[PLANES:ROWS], low)
        rims.append(jnp.broadcast_to(rim, (8, 128)))
    units = [jnp.broadcast_to(units_ref[c : c + 1], (8, 128)) for c in range(3)]

    def copy(i):
        part = pl.ds(i * SENDERS, SENDERS)
        return pltpu.make_async_copy(
            out_ref.at[:, :, part, :], out_hbm.at[:, :, part, :], sems.at[i]
        )

    for i in range(devices // SENDERS):
        for rank in range(MOST):
            for k in range(SENDERS // 8):
                source = i * SENDERS + 8 * k
                place = (source * MOST + rank) * 4
                label = slots_ref[pl.ds(place + 3, 8, stride=12), :].astype(i32)
                q = label >> 7
                l = label & 127
                above = q == PLANES
                below = (l == 0) & (q < PLANES)
                rim_lane = jnp.where(above, l, (q + 64) & 127)
                which = found[pl.ds(place + 3, 8, stride=12), :].astype(i32)
                n = [jnp.take_along_axis(units[c], which, axis=1) for c in range(3)]
                u = [
                    jnp.where(
                        above | below,
                        jnp.take_along_axis(rims[c], rim_lane, axis=1),
                        found[pl.ds(place + c, 8, stride=12), :],
                    )
                    for c in range(3)
                ]
                w = [slots_ref[pl.ds(place + c, 8, stride=12), :] - u[c] for c in range(3)]
                inner = n[0] * w[0] + n[1] * w[1] + n[2] * w[2]
                crossed = [
                    n[1] * w[2] - n[2] * w[1],
                    n[2] * w[0] - n[0] * w[2],
                    n[0] * w[1] - n[1] * w[0],
                ]
                for c in range(3):
                    out_ref[rank, c, pl.ds(source, 8), :] = (
                        u[c]
                        + w[c] * angle_cosine
                        + crossed[c] * angle_sine
                        + n[c] * inner * (1.0 - angle_cosine)
                    )
        copy(i).start()
    for i in range(devices // SENDERS):
        copy(i).wait()


def both_ways(head, tail, axis):
    count = lax.axis_size(axis)
    up = lax.ppermute(head, axis, [((i + 1) % count, i) for i in range(count)])
    down = lax.ppermute(tail, axis, [(i, (i + 1) % count) for i in range(count)])
    return up, down


def shards(velocity, cell_index, block_target, rotation_axis, grid_shift):
    devices = 128
    shape = jax.ShapeDtypeStruct
    vmem = pl.BlockSpec(memory_space=pltpu.VMEM)
    smem = pl.BlockSpec(memory_space=pltpu.SMEM)
    hbm = pl.BlockSpec(memory_space=pltpu.HBM)
    blocks = velocity.shape[0]
    send = call(
        pack_body,
        shape((devices * MOST * 4, 128), f32),
        in_specs=[hbm, hbm, hbm],
        scratch_shapes=[
            pltpu.VMEM((1, blocks), i32),
            pltpu.VMEM((3, blocks, 128), f32),
            pltpu.VMEM((blocks, 128), i32),
            pltpu.SemaphoreType.DMA((3,)),
        ],
        name="pack",
    )(
        *(
            pltpu.with_memory_space_constraint(x, pltpu.HBM)
            for x in (block_target.reshape(1, -1), jnp.transpose(velocity, (1, 0, 2)), cell_index)
        )
    )
    axes = call(
        axes_body,
        shape((PADROWS, 128), f32),
        in_specs=[smem, vmem],
        scratch_shapes=[pltpu.VMEM((PADROWS, 128), i32)],
        name="axes",
    )(grid_shift, rotation_axis)
    units = jnp.pad(axis_table(), ((0, 5), (0, 128 - NAX)))
    slots = lax.all_to_all(
        send.reshape(devices, MOST, 4, 128), ("gx", "gy", "gz"), split_axis=0, concat_axis=0, tiled=True
    ).reshape(devices * MOST * 4, 128)
    total_shape = shape((4, PADROWS, 128), f32)
    x_face = shape((4, 16, 128), f32)
    y_face = shape((4, 8, 128), f32)
    z_face = shape((8, 128), f32)
    total, head, tail = call(
        deposit_body,
        [total_shape, x_face, x_face],
        scratch_shapes=[
            pltpu.VMEM((2, 192, 128), f32),
            pltpu.VMEM((devices * MOST, 128), f32),
            pltpu.VMEM((devices * MOST, 128), f32),
        ],
        name="deposit",
    )(slots)
    up, down = both_ways(head, tail, "gx")
    total, head, tail = call(fold_x_body, [total_shape, y_face, y_face], name="fold_x")(
        total, up, down
    )
    up, down = both_ways(head, tail, "gy")
    up, down, axes, units = lax.optimization_barrier((up, down, axes, units))
    total, head, tail = call(fold_y_body, [total_shape, z_face, z_face], name="fold_y")(
        total, up, down
    )
    up, down = both_ways(head, tail, "gz")
    found = call(
        look_body,
        shape((devices * MOST * 4, 128), f32),
        scratch_shapes=[
            pltpu.VMEM((PADROWS, 128), f32),
            pltpu.VMEM((2, Q2 * 8, 128), f32),
            pltpu.VMEM((devices * MOST, 128), i32),
            pltpu.VMEM((devices * MOST, 128), f32),
        ],
        name="look",
    )(total, axes, slots)
    updated, cell_flow = call(
        turn_body,
        [shape((MOST, 3, devices, 128), f32), shape((3, CX, CY, CZ), f32)],
        out_specs=[hbm, vmem],
        scratch_shapes=[
            pltpu.VMEM((MOST, 3, devices, 128), f32),
            pltpu.SemaphoreType.DMA((devices // SENDERS,)),
        ],
        name="turn",
    )(total, up, down, units, slots, found)
    return jnp.transpose(updated, (2, 0, 1, 3))[None], cell_flow


def solution(mesh):
    return jax.shard_map(
        shards,
        mesh=mesh,
        in_specs=(
            P(("gx", "gy", "gz"), None, None),
            P(("gx", "gy", "gz"), None),
            P(("gx", "gy", "gz"), None),
            P(),
            P(),
        ),
        out_specs=(P(("gx", "gy", "gz"), None, None, None, None), P(None, "gx", "gy", "gz")),
        check_vma=False,
    )
```

```python
import functools

import jax
import jax.numpy as jnp
from jax import lax
from jax.experimental import pallas as pl
from jax.experimental.pallas import tpu as pltpu
from jax.sharding import PartitionSpec as P

CX = 4
CY = 8
CZ = 128
NAX = 64
APER = 32
MOST = 3
PX = CX + 1
PY = CY + 1
PLANES = PX * PY
ROWS = PLANES + 1
PADROWS = 48
EMPTY = 6400.0

angle_cosine = -0.6427876096865393
angle_sine = 0.766044443118978

f32 = jnp.float32
bf16 = jnp.bfloat16
i32 = jnp.int32


def iota(shape, dim):
    return lax.broadcasted_iota(i32, shape, dim)


def axis_table(shape):
    counter = iota(shape, 1).astype(f32) + 0.5
    height = 1.0 - 2.0 * counter / NAX
    radius = jnp.sqrt(jnp.maximum(1.0 - height * height, 0.0))
    turning = counter * 2.399963229728653
    return radius * jnp.cos(turning), radius * jnp.sin(turning), height


def split3(value):
    high = value.astype(bf16)
    rest = value - high.astype(f32)
    middle = rest.astype(bf16)
    return high, middle, (rest - middle.astype(f32)).astype(bf16)


def call(body, out_shape, **kw):
    return pl.pallas_call(
        body,
        out_shape=out_shape,
        compiler_params=pltpu.CompilerParams(vmem_limit_bytes=48 * 1024 * 1024),
        **kw,
    )


def pack_body(target_hbm, velocity_hbm, index_hbm, out_ref, target_ref, velocity_ref, index_ref, sems):
    sources = (target_hbm, index_hbm, velocity_hbm)
    sinks = (target_ref, index_ref, velocity_ref)
    copies = [
        pltpu.make_async_copy(source, sink, sems.at[k])
        for k, (source, sink) in enumerate(zip(sources, sinks))
    ]
    for copy in copies:
        copy.start()
    bricks = 128
    blocks = target_ref.shape[1]
    copies[0].wait()
    target = jnp.broadcast_to(target_ref[...], (bricks, blocks))
    onehot = target == iota((bricks, blocks), 0)
    onehot_bf = jnp.where(onehot, 1.0, 0.0).astype(bf16)
    earlier = jnp.where(iota((blocks, blocks), 0) < iota((blocks, blocks), 1), 1.0, 0.0)
    before = jnp.dot(onehot_bf, earlier.astype(bf16), preferred_element_type=f32)
    places = [
        jnp.where(onehot & (before == float(rank)), 1.0, 0.0).astype(bf16) for rank in range(MOST)
    ]
    copies[1].wait()
    index = index_ref[...]
    plane = (index * 8129) >> 20
    depth = index - plane * (CZ + 1)
    top = depth == CZ
    label = jnp.where(top, PLANES * 128 + plane, plane * 128 + depth)
    label = label.astype(f32) - EMPTY
    copies[2].wait()
    splits = split3(jnp.concatenate([velocity_ref[c] for c in range(3)] + [label], axis=1))
    for rank in range(MOST):
        moved = sum(jnp.dot(places[rank], s, preferred_element_type=f32) for s in reversed(splits))
        for c in range(4):
            value = moved[:, c * 128 : (c + 1) * 128]
            if c == 3:
                value = value + EMPTY
            out_ref[pl.ds(rank * 4 + c, bricks, stride=4 * MOST), :] = value


def axes_body(shift_ref, rotation_ref, out_ref, units_ref, rows):
    base_x = lax.axis_index("gx") * CX + shift_ref[0]
    base_y = lax.axis_index("gy") * CY + shift_ref[1]
    rows[...] = jnp.zeros(rows.shape, i32)
    for ex in range(PX):
        for ey in range(PY):
            a = (base_x + ex) & (APER - 1)
            b = (base_y + ey) & (APER - 1)
            rows[pl.ds(ex * PY + ey, 1), :APER] = rotation_ref[a, pl.ds(b, 1), :]
    value = rows[...].astype(f32)
    value = value + pltpu.roll(value, 32, 1)
    value = value + pltpu.roll(value, 64, 1)
    value = pltpu.roll(value, (128 - shift_ref[2]) & 127, 1)
    first = column_as_row(value)
    out_ref[...] = jnp.where(iota(value.shape, 0) == PLANES, first, value)
    for c, line in enumerate(axis_table((8, 128))):
        units_ref[c] = line


def column_as_row(value):
    column = jnp.broadcast_to(value[:, 0:1], value.shape)
    same = iota(value.shape, 0) == iota(value.shape, 1)
    return jnp.sum(jnp.where(same, column, 0.0), axis=0, keepdims=True)


DEPOSIT_STEP = 128
Q2 = ROWS // 2


def slot_places(slots_ref, rows_q, rows_l):
    slots = slots_ref.shape[0] // 4
    label = slots_ref[pl.ds(3, slots, stride=4), :].astype(i32)
    rows_q[...] = (label >> 8).astype(rows_q.dtype)
    rows_l[...] = jnp.where(label >= PADROWS * 128, 512, label & 255).astype(f32)


def lane_onehot(rows_l, slot, tiles=16):
    step = iota((16, 128), 0).astype(f32).astype(bf16)
    lane = jnp.broadcast_to(rows_l[pl.ds(slot, 1), :], (16, 128)).astype(bf16) - step
    one = jnp.ones((16, 128), bf16)
    zero = jnp.zeros((16, 128), bf16)
    return jnp.concatenate(
        [jnp.where(lane == float(16 * j), one, zero) for j in range(tiles)], axis=0
    )


def sum_rows(slots_ref, rows_q, rows_l, firsts, apart, tiles, store):
    slots = slots_ref.shape[0] // 4
    sub8 = iota((8, 128), 0)
    half = jnp.where(iota((16, 128), 0) >= 8, float(apart), 0.0).astype(bf16)
    zero = jnp.zeros((16, 128), bf16)

    def step(i, carry):
        weighted, depths = [], []
        for k in range(DEPOSIT_STEP):
            slot = i * DEPOSIT_STEP + k
            own = slots_ref[pl.ds(pl.multiple_of(i * DEPOSIT_STEP * 4, 8) + 4 * k, 4), :]
            own = jnp.concatenate([own, own], axis=0)
            high = own.astype(bf16).astype(f32)
            value = jnp.where(sub8 < 4, high, own - high)
            value = jnp.where(sub8 == 3, 1.0, jnp.where(sub8 == 7, 0.0, value))
            value = jnp.concatenate([value, value], axis=0).astype(bf16)
            q = jnp.broadcast_to(rows_q[pl.ds(slot, 1), :], (16, 128)).astype(bf16) - half
            weighted.append(
                jnp.concatenate([jnp.where(q == float(j), value, zero) for j in firsts], axis=0)
            )
            depths.append(lane_onehot(rows_l, slot, tiles).astype(jnp.float8_e4m3fn))
        store(
            lax.dot_general(
                jnp.concatenate(weighted, axis=1),
                jnp.concatenate(depths, axis=1),
                (((1,), (1,)), ((), ())),
                preferred_element_type=f32,
            )
        )
        return carry

    lax.fori_loop(0, slots // DEPOSIT_STEP, step, 0)


def deposit_faces_body(slots_ref, head_ref, tail_ref, acc, rows_q, rows_l):
    slots = slots_ref.shape[0] // 4
    label = slots_ref[pl.ds(3, slots, stride=4), :].astype(i32)
    rows_q[...] = (label >> 7).astype(f32)
    rows_l[...] = (label & 127).astype(f32)
    acc[...] = jnp.zeros(acc.shape, f32)

    def store(got):
        acc[...] += got

    firsts = [ex * PY for ex in range(PX)] + [PLANES]
    sum_rows(slots_ref, rows_q, rows_l, firsts, CY, 8, store)
    for c in range(4):
        for ref, first in ((head_ref, 0), (tail_ref, 8)):
            total = acc[pl.ds(first + c, PX, stride=16), :]
            above = acc[pl.ds(16 * PX + c, 1), :]
            if c < 3:
                total = total + acc[pl.ds(first + c + 4, PX, stride=16), :]
                above = above + acc[pl.ds(16 * PX + c + 4, 1), :]
            ref[c, 0:PX] = total
            ref[c, PX : PX + 1] = above


def deposit_body(slots_ref, total_ref, acc, rows_q, rows_l):
    slot_places(slots_ref, rows_q, rows_l)
    acc[...] = jnp.zeros(acc.shape, f32)

    def store(got):
        acc[0] += got[:, :128]
        acc[1] += got[:, 128:]

    sum_rows(slots_ref, rows_q, rows_l, [2 * j for j in range(12)], 1, 16, store)
    for c in range(4):
        for odd in range(2):
            total = acc[odd, pl.ds(c, Q2, stride=8), :]
            if c < 3:
                total = total + acc[odd, pl.ds(c + 4, Q2, stride=8), :]
            total_ref[c, pl.ds(odd, Q2, stride=2)] = total
        total_ref[c, ROWS:PADROWS] = jnp.zeros((PADROWS - ROWS, 128), f32)


def moved_lanes(row, first, count, shift):
    lane = iota(row.shape, 1)
    rolled = pltpu.roll(row, shift % 128, 1)
    return jnp.where((lane >= first) & (lane < first + count), rolled, 0.0)


def fold_y_body(total_ref, up_ref, down_ref, out_ref, head_ref, tail_ref):
    lane = iota((1, 128), 1)
    edge = lane % PY
    for c in range(4):
        out_ref[c] = total_ref[c]
        out_ref[c, pl.ds(CY, PX, stride=PY)] = (
            total_ref[c, pl.ds(CY, PX, stride=PY)] + up_ref[c, 0:PX]
        )
        out_ref[c, pl.ds(0, PX, stride=PY)] = (
            total_ref[c, pl.ds(0, PX, stride=PY)] + down_ref[c, 0:PX]
        )
        up = pltpu.roll(up_ref[c, PX : PX + 1], CY, 1)
        down = pltpu.roll(down_ref[c, PX : PX + 1], 128 - CY, 1)
        above = (
            total_ref[c, PLANES:ROWS]
            + jnp.where((edge == CY) & (lane < PLANES), up, 0.0)
            + jnp.where((edge == 0) & (lane < PLANES), down, 0.0)
        )
        out_ref[c, PLANES:ROWS] = above
        head_ref[c, 0:PY] = out_ref[c, 0:PY]
        head_ref[c, PY : PY + 1] = above
        tail_ref[c, 0:PY] = out_ref[c, PLANES - PY : PLANES]
        tail_ref[c, PY : PY + 1] = above


def fold_x_body(total_ref, up_ref, down_ref, out_ref, head_ref, tail_ref):
    last = PLANES - PY
    for c in range(4):
        out_ref[c] = total_ref[c]
        out_ref[c, 0:PY] = total_ref[c, 0:PY] + down_ref[c, 0:PY]
        out_ref[c, last:PLANES] = total_ref[c, last:PLANES] + up_ref[c, 0:PY]
        out_ref[c, PLANES:ROWS] = (
            total_ref[c, PLANES:ROWS]
            + moved_lanes(up_ref[c, PY : PY + 1], last, PY, last)
            + moved_lanes(down_ref[c, PY : PY + 1], 0, PY, -last)
        )
        total = out_ref[c]
        head_ref[c : c + 1] = column_as_row(total)
        tail_ref[c : c + 1] = total[PLANES:ROWS]
        head_ref[4 + c : 5 + c] = jnp.zeros((1, 128), f32)
        tail_ref[4 + c : 5 + c] = jnp.zeros((1, 128), f32)


def select_row(rows, bits):
    for bit in bits:
        rows = [
            jnp.where(bit, rows[j + 1], rows[j]) if j + 1 < len(rows) else rows[j]
            for j in range(0, len(rows), 2)
        ]
    return rows[0]


def look_body(total_ref, axes_ref, slots_ref, found, cells, wide, rows_q, rows_l):
    slots = slots_ref.shape[0] // 4
    count = jnp.maximum(total_ref[3], 1.0)
    wide[...] = jnp.zeros(wide.shape, f32)

    def tabulate(value, line):
        cells[...] = value
        for odd in range(2):
            wide[odd, pl.ds(line, Q2, stride=8), :] = cells[pl.ds(odd, Q2, stride=2)]

    for c in range(3):
        mean = total_ref[c] / count
        high = mean.astype(bf16).astype(f32)
        tabulate(high, c)
        tabulate(mean - high, c + 4)
    tabulate(axes_ref[...], 3)
    table = jnp.concatenate([wide[0], wide[1]], axis=1).astype(bf16)
    slot_places(slots_ref, rows_q, rows_l)
    sub8 = iota((8, 128), 0)
    for k in range(slots // 2):
        pair = [2 * k, 2 * k + 1]
        hot = jnp.concatenate([lane_onehot(rows_l, slot) for slot in pair], axis=1)
        read = jnp.dot(table, hot, preferred_element_type=f32)
        got = []
        for h in range(2):
            q = jnp.broadcast_to(rows_q[pl.ds(pair[h], 1), :], (8, 128))
            bits = [(q & (1 << b)) != 0 for b in range(5)]
            lines = [read[8 * j : 8 * j + 8, 128 * h : 128 * h + 128] for j in range(Q2)]
            value = select_row(lines, bits)
            got.append(value + pltpu.roll(value, 4, 0))
        found[pl.ds(8 * k, 8), :] = jnp.where(sub8 < 4, got[0], got[1])


SENDERS = 32


def turn_body(
    total_ref, up_ref, down_ref, units_ref, slots_ref, found, out_hbm, flow_ref, out_ref, sems
):
    devices = out_ref.shape[2]
    shape = (PADROWS, 128)
    row = iota(shape, 0)
    lane = iota(shape, 1)
    top = (row == PLANES) & (lane < PLANES)
    totals = []
    for c in range(4):
        own = total_ref[c]
        column = jnp.sum(
            jnp.where((row == lane) & (row < PLANES), down_ref[c : c + 1], 0.0),
            axis=1,
            keepdims=True,
        )
        own = own + jnp.where(lane == 0, column, 0.0)
        totals.append(own + jnp.where(top, up_ref[c : c + 1], 0.0))
    count = jnp.maximum(totals[3], 1.0)
    rims = []
    for c in range(3):
        mean = totals[c] / count
        for ex in range(CX):
            flow_ref[c, ex] = mean[ex * PY : ex * PY + CY]
        low = pltpu.roll(column_as_row(mean), 64, 1)
        rim = jnp.where(iota((1, 128), 1) < 64, mean[PLANES:ROWS], low)
        rims.append(jnp.broadcast_to(rim, (8, 128)))
    units = [units_ref[c] for c in range(3)]

    def copy(i):
        part = pl.ds(i * SENDERS, SENDERS)
        return pltpu.make_async_copy(
            out_ref.at[:, :, part, :], out_hbm.at[:, :, part, :], sems.at[i]
        )

    for i in range(devices // SENDERS):
        for rank in range(MOST):
            for k in range(SENDERS // 8):
                source = i * SENDERS + 8 * k
                place = (source * MOST + rank) * 4
                label = slots_ref[pl.ds(place + 3, 8, stride=12), :].astype(i32)
                q = label >> 7
                l = label & 127
                above = q == PLANES
                below = (l == 0) & (q < PLANES)
                rim_lane = jnp.where(above, l, (q + 64) & 127)
                which = found[pl.ds(place + 3, 8, stride=12), :].astype(i32)
                n = [jnp.take_along_axis(units[c], which, axis=1) for c in range(3)]
                u = [
                    jnp.where(
                        above | below,
                        jnp.take_along_axis(rims[c], rim_lane, axis=1),
                        found[pl.ds(place + c, 8, stride=12), :],
                    )
                    for c in range(3)
                ]
                w = [slots_ref[pl.ds(place + c, 8, stride=12), :] - u[c] for c in range(3)]
                inner = n[0] * w[0] + n[1] * w[1] + n[2] * w[2]
                crossed = [
                    n[1] * w[2] - n[2] * w[1],
                    n[2] * w[0] - n[0] * w[2],
                    n[0] * w[1] - n[1] * w[0],
                ]
                for c in range(3):
                    out_ref[rank, c, pl.ds(source, 8), :] = (
                        u[c]
                        + w[c] * angle_cosine
                        + crossed[c] * angle_sine
                        + n[c] * inner * (1.0 - angle_cosine)
                    )
        copy(i).start()
    for i in range(devices // SENDERS):
        copy(i).wait()


def both_ways(head, tail, axis):
    count = lax.axis_size(axis)
    up = lax.ppermute(head, axis, [((i + 1) % count, i) for i in range(count)])
    down = lax.ppermute(tail, axis, [(i, (i + 1) % count) for i in range(count)])
    return up, down


def shards(velocity, cell_index, block_target, rotation_axis, grid_shift):
    devices = 128
    shape = jax.ShapeDtypeStruct
    vmem = pl.BlockSpec(memory_space=pltpu.VMEM)
    smem = pl.BlockSpec(memory_space=pltpu.SMEM)
    hbm = pl.BlockSpec(memory_space=pltpu.HBM)
    blocks = velocity.shape[0]
    send = call(
        pack_body,
        shape((devices * MOST * 4, 128), f32),
        in_specs=[hbm, hbm, hbm],
        scratch_shapes=[
            pltpu.VMEM((1, blocks), i32),
            pltpu.VMEM((3, blocks, 128), f32),
            pltpu.VMEM((blocks, 128), i32),
            pltpu.SemaphoreType.DMA((3,)),
        ],
        name="pack",
    )(
        *(
            pltpu.with_memory_space_constraint(x, pltpu.HBM)
            for x in (block_target.reshape(1, -1), jnp.transpose(velocity, (1, 0, 2)), cell_index)
        )
    )
    axes, units = call(
        axes_body,
        [shape((PADROWS, 128), f32), shape((3, 8, 128), f32)],
        in_specs=[smem, vmem],
        scratch_shapes=[pltpu.VMEM((PADROWS, 128), i32)],
        name="axes",
    )(grid_shift, rotation_axis)
    slots = lax.all_to_all(
        send.reshape(devices, MOST, 4, 128), ("gx", "gy", "gz"), split_axis=0, concat_axis=0, tiled=True
    ).reshape(devices * MOST * 4, 128)
    total_shape = shape((4, PADROWS, 128), f32)
    x_face = shape((4, 16, 128), f32)
    y_face = shape((4, 8, 128), f32)
    z_face = shape((8, 128), f32)
    by_slot = pltpu.VMEM((devices * MOST, 128), f32)
    head, tail = call(
        deposit_faces_body,
        [y_face, y_face],
        scratch_shapes=[pltpu.VMEM((16 * (PX + 1), 128), f32), by_slot, by_slot],
        name="deposit_faces",
    )(slots)
    slots, head, tail = lax.optimization_barrier((slots, head, tail))
    up, down = both_ways(head, tail, "gy")
    total = call(
        deposit_body,
        total_shape,
        scratch_shapes=[pltpu.VMEM((2, 192, 128), f32), by_slot, by_slot],
        name="deposit",
    )(slots)
    total, head, tail = call(fold_y_body, [total_shape, x_face, x_face], name="fold_y")(
        total, up, down
    )
    up, down = both_ways(head, tail, "gx")
    up, down, axes, units = lax.optimization_barrier((up, down, axes, units))
    total, head, tail = call(fold_x_body, [total_shape, z_face, z_face], name="fold_x")(
        total, up, down
    )
    up, down = both_ways(head, tail, "gz")
    found = call(
        look_body,
        shape((devices * MOST * 4, 128), f32),
        scratch_shapes=[
            pltpu.VMEM((PADROWS, 128), f32),
            pltpu.VMEM((2, Q2 * 8, 128), f32),
            pltpu.VMEM((devices * MOST, 128), i32),
            pltpu.VMEM((devices * MOST, 128), f32),
        ],
        name="look",
    )(total, axes, slots)
    updated, cell_flow = call(
        turn_body,
        [shape((MOST, 3, devices, 128), f32), shape((3, CX, CY, CZ), f32)],
        out_specs=[hbm, vmem],
        scratch_shapes=[
            pltpu.VMEM((MOST, 3, devices, 128), f32),
            pltpu.SemaphoreType.DMA((devices // SENDERS,)),
        ],
        name="turn",
    )(total, up, down, units, slots, found)
    return jnp.transpose(updated, (2, 0, 1, 3))[None], cell_flow


def solution(mesh):
    return jax.shard_map(
        shards,
        mesh=mesh,
        in_specs=(
            P(("gx", "gy", "gz"), None, None),
            P(("gx", "gy", "gz"), None),
            P(("gx", "gy", "gz"), None),
            P(),
            P(),
        ),
        out_specs=(P(("gx", "gy", "gz"), None, None, None, None), P(None, "gx", "gy", "gz")),
        check_vma=False,
    )
```

```python
import functools

import jax
import jax.numpy as jnp
from jax import lax
from jax.experimental import pallas as pl
from jax.experimental.pallas import tpu as pltpu
from jax.sharding import PartitionSpec as P

CX = 4
CY = 8
CZ = 128
NAX = 64
APER = 32
MOST = 3
PX = CX + 1
PY = CY + 1
PLANES = PX * PY
ROWS = PLANES + 1
PADROWS = 48
EMPTY = 6400.0

angle_cosine = -0.6427876096865393
angle_sine = 0.766044443118978

f32 = jnp.float32
bf16 = jnp.bfloat16
i32 = jnp.int32


def iota(shape, dim):
    return lax.broadcasted_iota(i32, shape, dim)


def axis_table(shape):
    counter = iota(shape, 1).astype(f32) + 0.5
    height = 1.0 - 2.0 * counter / NAX
    radius = jnp.sqrt(jnp.maximum(1.0 - height * height, 0.0))
    turning = counter * 2.399963229728653
    return radius * jnp.cos(turning), radius * jnp.sin(turning), height


def split3(value):
    high = value.astype(bf16)
    rest = value - high.astype(f32)
    middle = rest.astype(bf16)
    return high, middle, (rest - middle.astype(f32)).astype(bf16)


def call(body, out_shape, **kw):
    return pl.pallas_call(
        body,
        out_shape=out_shape,
        compiler_params=pltpu.CompilerParams(vmem_limit_bytes=48 * 1024 * 1024),
        **kw,
    )


def pack_body(target_hbm, velocity_hbm, index_hbm, out_ref, target_ref, velocity_ref, index_ref, sems):
    sources = (target_hbm, index_hbm, velocity_hbm)
    sinks = (target_ref, index_ref, velocity_ref)
    copies = [
        pltpu.make_async_copy(source, sink, sems.at[k])
        for k, (source, sink) in enumerate(zip(sources, sinks))
    ]
    for copy in copies:
        copy.start()
    bricks = 128
    blocks = target_ref.shape[1]
    copies[0].wait()
    target = jnp.broadcast_to(target_ref[...], (bricks, blocks))
    onehot = target == iota((bricks, blocks), 0)
    onehot_bf = jnp.where(onehot, 1.0, 0.0).astype(bf16)
    earlier = jnp.where(iota((blocks, blocks), 0) < iota((blocks, blocks), 1), 1.0, 0.0)
    before = jnp.dot(onehot_bf, earlier.astype(bf16), preferred_element_type=f32)
    places = [
        jnp.where(onehot & (before == float(rank)), 1.0, 0.0).astype(bf16) for rank in range(MOST)
    ]
    copies[1].wait()
    index = index_ref[...]
    plane = (index * 8129) >> 20
    depth = index - plane * (CZ + 1)
    top = depth == CZ
    label = jnp.where(top, PLANES * 128 + plane, plane * 128 + depth)
    label = label.astype(f32) - EMPTY
    copies[2].wait()
    splits = split3(jnp.concatenate([velocity_ref[c] for c in range(3)] + [label], axis=1))
    for rank in range(MOST):
        moved = sum(jnp.dot(places[rank], s, preferred_element_type=f32) for s in reversed(splits))
        for c in range(4):
            value = moved[:, c * 128 : (c + 1) * 128]
            if c == 3:
                value = value + EMPTY
            out_ref[pl.ds(rank * 4 + c, bricks, stride=4 * MOST), :] = value


def axes_body(shift_ref, rotation_ref, out_ref, units_ref, rows):
    base_x = lax.axis_index("gx") * CX + shift_ref[0]
    base_y = lax.axis_index("gy") * CY + shift_ref[1]
    rows[...] = jnp.zeros(rows.shape, i32)
    for ex in range(PX):
        for ey in range(PY):
            a = (base_x + ex) & (APER - 1)
            b = (base_y + ey) & (APER - 1)
            rows[pl.ds(ex * PY + ey, 1), :APER] = rotation_ref[a, pl.ds(b, 1), :]
    value = rows[...].astype(f32)
    value = value + pltpu.roll(value, 32, 1)
    value = value + pltpu.roll(value, 64, 1)
    value = pltpu.roll(value, (128 - shift_ref[2]) & 127, 1)
    first = column_as_row(value)
    out_ref[...] = jnp.where(iota(value.shape, 0) == PLANES, first, value)
    for c, line in enumerate(axis_table((8, 128))):
        units_ref[c] = line


def column_as_row(value):
    column = jnp.broadcast_to(value[:, 0:1], value.shape)
    same = iota(value.shape, 0) == iota(value.shape, 1)
    return jnp.sum(jnp.where(same, column, 0.0), axis=0, keepdims=True)


DEPOSIT_STEP = 128
Q2 = ROWS // 2


def slot_places(slots_ref, rows_q, rows_l):
    slots = slots_ref.shape[0] // 4
    label = slots_ref[pl.ds(3, slots, stride=4), :].astype(i32)
    rows_q[...] = (label >> 8).astype(rows_q.dtype)
    rows_l[...] = jnp.where(label >= PADROWS * 128, 512, label & 255).astype(f32)


def lane_onehot(rows_l, slot, tiles=16):
    step = iota((16, 128), 0).astype(f32).astype(bf16)
    lane = jnp.broadcast_to(rows_l[pl.ds(slot, 1), :], (16, 128)).astype(bf16) - step
    one = jnp.ones((16, 128), bf16)
    zero = jnp.zeros((16, 128), bf16)
    return jnp.concatenate(
        [jnp.where(lane == float(16 * j), one, zero) for j in range(tiles)], axis=0
    )


def sum_rows(slots_ref, rows_q, rows_l, firsts, apart, tiles, store):
    slots = slots_ref.shape[0] // 4
    sub8 = iota((8, 128), 0)
    half = jnp.where(iota((16, 128), 0) >= 8, float(apart), 0.0).astype(bf16)
    zero = jnp.zeros((16, 128), bf16)

    def step(i, carry):
        weighted, depths = [], []
        for k in range(DEPOSIT_STEP):
            slot = i * DEPOSIT_STEP + k
            own = slots_ref[pl.ds(pl.multiple_of(i * DEPOSIT_STEP * 4, 8) + 4 * k, 4), :]
            own = jnp.concatenate([own, own], axis=0)
            high = own.astype(bf16).astype(f32)
            value = jnp.where(sub8 < 4, high, own - high)
            value = jnp.where(sub8 == 3, 1.0, jnp.where(sub8 == 7, 0.0, value))
            value = jnp.concatenate([value, value], axis=0).astype(bf16)
            q = jnp.broadcast_to(rows_q[pl.ds(slot, 1), :], (16, 128)).astype(bf16) - half
            weighted.append(
                jnp.concatenate([jnp.where(q == float(j), value, zero) for j in firsts], axis=0)
            )
            depths.append(lane_onehot(rows_l, slot, tiles).astype(jnp.float8_e4m3fn))
        store(
            lax.dot_general(
                jnp.concatenate(weighted, axis=1),
                jnp.concatenate(depths, axis=1),
                (((1,), (1,)), ((), ())),
                preferred_element_type=f32,
            )
        )
        return carry

    lax.fori_loop(0, slots // DEPOSIT_STEP, step, 0)


def deposit_faces_body(slots_ref, head_ref, tail_ref, acc, rows_q, rows_l):
    slots = slots_ref.shape[0] // 4
    label = slots_ref[pl.ds(3, slots, stride=4), :].astype(i32)
    rows_q[...] = (label >> 7).astype(f32)
    rows_l[...] = (label & 127).astype(f32)
    acc[...] = jnp.zeros(acc.shape, f32)

    def store(got):
        acc[...] += got

    firsts = [ex * PY for ex in range(PX)] + [PLANES]
    sum_rows(slots_ref, rows_q, rows_l, firsts, CY, 8, store)
    for c in range(4):
        for ref, first in ((head_ref, 0), (tail_ref, 8)):
            total = acc[pl.ds(first + c, PX, stride=16), :]
            above = acc[pl.ds(16 * PX + c, 1), :]
            if c < 3:
                total = total + acc[pl.ds(first + c + 4, PX, stride=16), :]
                above = above + acc[pl.ds(16 * PX + c + 4, 1), :]
            ref[c, 0:PX] = total
            ref[c, PX : PX + 1] = above


def deposit_body(slots_ref, total_ref, acc, rows_q, rows_l):
    slot_places(slots_ref, rows_q, rows_l)
    acc[...] = jnp.zeros(acc.shape, f32)

    def store(got):
        acc[0] += got[:, :128]
        acc[1] += got[:, 128:]

    sum_rows(slots_ref, rows_q, rows_l, [2 * j for j in range(12)], 1, 16, store)
    for c in range(4):
        for odd in range(2):
            total = acc[odd, pl.ds(c, Q2, stride=8), :]
            if c < 3:
                total = total + acc[odd, pl.ds(c + 4, Q2, stride=8), :]
            total_ref[c, pl.ds(odd, Q2, stride=2)] = total
        total_ref[c, ROWS:PADROWS] = jnp.zeros((PADROWS - ROWS, 128), f32)


def moved_lanes(row, first, count, shift):
    lane = iota(row.shape, 1)
    rolled = pltpu.roll(row, shift % 128, 1)
    return jnp.where((lane >= first) & (lane < first + count), rolled, 0.0)


def fold_y_body(total_ref, up_ref, down_ref, out_ref, head_ref, tail_ref):
    lane = iota((1, 128), 1)
    edge = lane % PY
    for c in range(4):
        out_ref[c] = total_ref[c]
        out_ref[c, pl.ds(CY, PX, stride=PY)] = (
            total_ref[c, pl.ds(CY, PX, stride=PY)] + up_ref[c, 0:PX]
        )
        out_ref[c, pl.ds(0, PX, stride=PY)] = (
            total_ref[c, pl.ds(0, PX, stride=PY)] + down_ref[c, 0:PX]
        )
        up = pltpu.roll(up_ref[c, PX : PX + 1], CY, 1)
        down = pltpu.roll(down_ref[c, PX : PX + 1], 128 - CY, 1)
        above = (
            total_ref[c, PLANES:ROWS]
            + jnp.where((edge == CY) & (lane < PLANES), up, 0.0)
            + jnp.where((edge == 0) & (lane < PLANES), down, 0.0)
        )
        out_ref[c, PLANES:ROWS] = above
        head_ref[c, 0:PY] = out_ref[c, 0:PY]
        head_ref[c, PY : PY + 1] = above
        tail_ref[c, 0:PY] = out_ref[c, PLANES - PY : PLANES]
        tail_ref[c, PY : PY + 1] = above


def fold_x_body(total_ref, up_ref, down_ref, out_ref, head_ref, tail_ref):
    last = PLANES - PY
    for c in range(4):
        out_ref[c] = total_ref[c]
        out_ref[c, 0:PY] = total_ref[c, 0:PY] + down_ref[c, 0:PY]
        out_ref[c, last:PLANES] = total_ref[c, last:PLANES] + up_ref[c, 0:PY]
        out_ref[c, PLANES:ROWS] = (
            total_ref[c, PLANES:ROWS]
            + moved_lanes(up_ref[c, PY : PY + 1], last, PY, last)
            + moved_lanes(down_ref[c, PY : PY + 1], 0, PY, -last)
        )
        total = out_ref[c]
        head_ref[c : c + 1] = column_as_row(total)
        tail_ref[c : c + 1] = total[PLANES:ROWS]
        head_ref[4 + c : 5 + c] = jnp.zeros((1, 128), f32)
        tail_ref[4 + c : 5 + c] = jnp.zeros((1, 128), f32)


def select_row(rows, bits):
    for bit in bits:
        rows = [
            jnp.where(bit, rows[j + 1], rows[j]) if j + 1 < len(rows) else rows[j]
            for j in range(0, len(rows), 2)
        ]
    return rows[0]


INNER = [ex * PY + ey for ex in range(1, CX) for ey in range(1, CY)]
OUTER = (
    list(range(PY))
    + list(range(PLANES - PY, PLANES))
    + [ex * PY + ey for ex in range(1, CX) for ey in (0, CY)]
    + [PLANES]
)


def position(row, inner):
    ex = (row * 57) >> 9
    ey = row - ex * PY
    is_inner = (ex >= 1) & (ex < CX) & (ey >= 1) & (ey < CY)
    if inner:
        return (ex - 1) * (CY - 1) + ey - 1, is_inner
    side = 2 * PY + 2 * (ex - 1) + jnp.where(ey == CY, 1, 0)
    place = jnp.where(ex == 0, ey, jnp.where(ex == CX, PY + ey, side))
    place = jnp.where(row == PLANES, len(OUTER) - 1, place)
    return place, jnp.logical_not(is_inner) & (row <= PLANES)


def look(total_ref, axes_ref, slots_ref, found, cells, wide, rows_q, rows_l, inner, earlier, after):
    slots = slots_ref.shape[0] // 4
    listed = INNER if inner else OUTER
    folded = (len(listed) + 1) // 2
    count = jnp.maximum(total_ref[3], 1.0)
    wide[...] = jnp.zeros(wide.shape, f32)

    def tabulate(value, line):
        cells[...] = value
        for p, row in enumerate(listed):
            wide[p & 1, pl.ds(8 * (p >> 1) + line, 1), :] = cells[pl.ds(row, 1), :]

    for c in range(3):
        mean = total_ref[c] / count
        high = mean.astype(bf16).astype(f32)
        tabulate(high, c)
        tabulate(mean - high, c + 4)
    tabulate(axes_ref[...], 3)
    table = jnp.concatenate([wide[0], wide[1]], axis=1).astype(bf16)
    label = slots_ref[pl.ds(3, slots, stride=4), :].astype(i32)
    place, here = position(label >> 7, inner)
    rows_q[...] = place >> 1
    rows_l[...] = jnp.where(here, (place & 1) * 128 + (label & 127), 512).astype(f32)
    sub8 = iota((8, 128), 0)
    for k in range(slots // 2):
        pair = [2 * k, 2 * k + 1]
        hot = jnp.concatenate([lane_onehot(rows_l, slot) for slot in pair], axis=1)
        read = jnp.dot(table, hot, preferred_element_type=f32)
        got = []
        for h in range(2):
            q = jnp.broadcast_to(rows_q[pl.ds(pair[h], 1), :], (8, 128))
            bits = [(q & (1 << b)) != 0 for b in range(4)]
            lines = [read[8 * j : 8 * j + 8, 128 * h : 128 * h + 128] for j in range(folded)]
            value = select_row(lines, bits)
            got.append(value + pltpu.roll(value, 4, 0))
        value = jnp.where(sub8 < 4, got[0], got[1])
        if earlier is not None:
            value = value + earlier[pl.ds(8 * k, 8), :]
        found[pl.ds(8 * k, 8), :] = value
        if after is not None:
            after(k)


def look_inner_body(total_ref, axes_ref, slots_ref, found, cells, wide, rows_q, rows_l):
    look(
        total_ref, axes_ref, slots_ref, found, cells, wide, rows_q, rows_l, True, None, None
    )


def look_outer_body(
    total_ref, axes_ref, units_ref, slots_ref, earlier, found, normal_ref, cells, wide, rows_q, rows_l
):
    units = [units_ref[c] for c in range(3)]
    pairs = 4 * MOST

    def normals(g):
        for rank in range(MOST):
            place = (g * 8 * MOST + rank) * 4 + 3
            which = found[pl.ds(place, 8, stride=4 * MOST), :].astype(i32)
            for c in range(3):
                normal_ref[rank, c, pl.ds(8 * g, 8), :] = jnp.take_along_axis(
                    units[c], which, axis=1
                )

    def after(k):
        if k % pairs == pairs - 1:
            normals(k // pairs)

    look(
        total_ref, axes_ref, slots_ref, found, cells, wide, rows_q, rows_l, False, earlier, after
    )


SENDERS = 32


def turn_body(
    total_ref, up_ref, down_ref, normal_ref, slots_ref, found, out_hbm, flow_ref, out_ref, sems
):
    devices = out_ref.shape[2]
    shape = (PADROWS, 128)
    row = iota(shape, 0)
    lane = iota(shape, 1)
    top = (row == PLANES) & (lane < PLANES)
    totals = []
    for c in range(4):
        own = total_ref[c]
        column = jnp.sum(
            jnp.where((row == lane) & (row < PLANES), down_ref[c : c + 1], 0.0),
            axis=1,
            keepdims=True,
        )
        own = own + jnp.where(lane == 0, column, 0.0)
        totals.append(own + jnp.where(top, up_ref[c : c + 1], 0.0))
    count = jnp.maximum(totals[3], 1.0)
    rims = []
    for c in range(3):
        mean = totals[c] / count
        for ex in range(CX):
            flow_ref[c, ex] = mean[ex * PY : ex * PY + CY]
        low = pltpu.roll(column_as_row(mean), 64, 1)
        rim = jnp.where(iota((1, 128), 1) < 64, mean[PLANES:ROWS], low)
        rims.append(jnp.broadcast_to(rim, (8, 128)))

    def copy(i):
        part = pl.ds(i * SENDERS, SENDERS)
        return pltpu.make_async_copy(
            out_ref.at[:, :, part, :], out_hbm.at[:, :, part, :], sems.at[i]
        )

    for i in range(devices // SENDERS):
        for rank in range(MOST):
            for k in range(SENDERS // 8):
                source = i * SENDERS + 8 * k
                place = (source * MOST + rank) * 4
                label = slots_ref[pl.ds(place + 3, 8, stride=12), :].astype(i32)
                q = label >> 7
                l = label & 127
                above = q == PLANES
                below = (l == 0) & (q < PLANES)
                rim_lane = jnp.where(above, l, (q + 64) & 127)
                n = [normal_ref[rank, c, pl.ds(source, 8), :] for c in range(3)]
                u = [
                    jnp.where(
                        above | below,
                        jnp.take_along_axis(rims[c], rim_lane, axis=1),
                        found[pl.ds(place + c, 8, stride=12), :],
                    )
                    for c in range(3)
                ]
                w = [slots_ref[pl.ds(place + c, 8, stride=12), :] - u[c] for c in range(3)]
                inner = n[0] * w[0] + n[1] * w[1] + n[2] * w[2]
                crossed = [
                    n[1] * w[2] - n[2] * w[1],
                    n[2] * w[0] - n[0] * w[2],
                    n[0] * w[1] - n[1] * w[0],
                ]
                for c in range(3):
                    out_ref[rank, c, pl.ds(source, 8), :] = (
                        u[c]
                        + w[c] * angle_cosine
                        + crossed[c] * angle_sine
                        + n[c] * inner * (1.0 - angle_cosine)
                    )
        copy(i).start()
    for i in range(devices // SENDERS):
        copy(i).wait()


def both_ways(head, tail, axis):
    count = lax.axis_size(axis)
    up = lax.ppermute(head, axis, [((i + 1) % count, i) for i in range(count)])
    down = lax.ppermute(tail, axis, [(i, (i + 1) % count) for i in range(count)])
    return up, down


def shards(velocity, cell_index, block_target, rotation_axis, grid_shift):
    devices = 128
    shape = jax.ShapeDtypeStruct
    vmem = pl.BlockSpec(memory_space=pltpu.VMEM)
    smem = pl.BlockSpec(memory_space=pltpu.SMEM)
    hbm = pl.BlockSpec(memory_space=pltpu.HBM)
    blocks = velocity.shape[0]
    send = call(
        pack_body,
        shape((devices * MOST * 4, 128), f32),
        in_specs=[hbm, hbm, hbm],
        scratch_shapes=[
            pltpu.VMEM((1, blocks), i32),
            pltpu.VMEM((3, blocks, 128), f32),
            pltpu.VMEM((blocks, 128), i32),
            pltpu.SemaphoreType.DMA((3,)),
        ],
        name="pack",
    )(
        *(
            pltpu.with_memory_space_constraint(x, pltpu.HBM)
            for x in (block_target.reshape(1, -1), jnp.transpose(velocity, (1, 0, 2)), cell_index)
        )
    )
    axes, units = call(
        axes_body,
        [shape((PADROWS, 128), f32), shape((3, 8, 128), f32)],
        in_specs=[smem, vmem],
        scratch_shapes=[pltpu.VMEM((PADROWS, 128), i32)],
        name="axes",
    )(grid_shift, rotation_axis)
    slots = lax.all_to_all(
        send.reshape(devices, MOST, 4, 128), ("gx", "gy", "gz"), split_axis=0, concat_axis=0, tiled=True
    ).reshape(devices * MOST * 4, 128)
    total_shape = shape((4, PADROWS, 128), f32)
    x_face = shape((4, 16, 128), f32)
    y_face = shape((4, 8, 128), f32)
    z_face = shape((8, 128), f32)
    by_slot = pltpu.VMEM((devices * MOST, 128), f32)
    head, tail = call(
        deposit_faces_body,
        [y_face, y_face],
        scratch_shapes=[pltpu.VMEM((16 * (PX + 1), 128), f32), by_slot, by_slot],
        name="deposit_faces",
    )(slots)
    slots, head, tail = lax.optimization_barrier((slots, head, tail))
    up, down = both_ways(head, tail, "gy")
    total = call(
        deposit_body,
        total_shape,
        scratch_shapes=[pltpu.VMEM((2, 192, 128), f32), by_slot, by_slot],
        name="deposit",
    )(slots)
    total, head, tail = call(fold_y_body, [total_shape, x_face, x_face], name="fold_y")(
        total, up, down
    )
    up, down = both_ways(head, tail, "gx")
    found_shape = shape((devices * MOST * 4, 128), f32)

    def look_scratch(listed):
        return [
            pltpu.VMEM((PADROWS, 128), f32),
            pltpu.VMEM((2, (len(listed) + 1) // 2 * 8, 128), f32),
            pltpu.VMEM((devices * MOST, 128), i32),
            by_slot,
        ]

    found = call(
        look_inner_body, found_shape, scratch_shapes=look_scratch(INNER), name="look_inner"
    )(total, axes, slots)
    up, down, found, axes, units = lax.optimization_barrier((up, down, found, axes, units))
    total, head, tail = call(fold_x_body, [total_shape, z_face, z_face], name="fold_x")(
        total, up, down
    )
    up, down = both_ways(head, tail, "gz")
    found, normal = call(
        look_outer_body,
        [found_shape, shape((MOST, 3, devices, 128), f32)],
        scratch_shapes=look_scratch(OUTER),
        name="look_outer",
    )(total, axes, units, slots, found)
    updated, cell_flow = call(
        turn_body,
        [shape((MOST, 3, devices, 128), f32), shape((3, CX, CY, CZ), f32)],
        out_specs=[hbm, vmem],
        scratch_shapes=[
            pltpu.VMEM((MOST, 3, devices, 128), f32),
            pltpu.SemaphoreType.DMA((devices // SENDERS,)),
        ],
        name="turn",
    )(total, up, down, normal, slots, found)
    return jnp.transpose(updated, (2, 0, 1, 3))[None], cell_flow


def solution(mesh):
    return jax.shard_map(
        shards,
        mesh=mesh,
        in_specs=(
            P(("gx", "gy", "gz"), None, None),
            P(("gx", "gy", "gz"), None),
            P(("gx", "gy", "gz"), None),
            P(),
            P(),
        ),
        out_specs=(P(("gx", "gy", "gz"), None, None, None, None), P(None, "gx", "gy", "gz")),
        check_vma=False,
    )
```

```python
import functools

import jax
import jax.numpy as jnp
from jax import lax
from jax.experimental import pallas as pl
from jax.experimental.pallas import tpu as pltpu
from jax.sharding import PartitionSpec as P

CX = 4
CY = 8
CZ = 128
NAX = 64
APER = 32
MOST = 3
PX = CX + 1
PY = CY + 1
PLANES = PX * PY
ROWS = PLANES + 1
PADROWS = 48
EMPTY = 6400.0

angle_cosine = -0.6427876096865393
angle_sine = 0.766044443118978

f32 = jnp.float32
bf16 = jnp.bfloat16
i32 = jnp.int32


def iota(shape, dim):
    return lax.broadcasted_iota(i32, shape, dim)


def axis_table(shape):
    counter = iota(shape, 1).astype(f32) + 0.5
    height = 1.0 - 2.0 * counter / NAX
    radius = jnp.sqrt(jnp.maximum(1.0 - height * height, 0.0))
    turning = counter * 2.399963229728653
    return radius * jnp.cos(turning), radius * jnp.sin(turning), height


def split3(value):
    high = value.astype(bf16)
    rest = value - high.astype(f32)
    middle = rest.astype(bf16)
    return high, middle, (rest - middle.astype(f32)).astype(bf16)


def call(body, out_shape, **kw):
    return pl.pallas_call(
        body,
        out_shape=out_shape,
        compiler_params=pltpu.CompilerParams(vmem_limit_bytes=48 * 1024 * 1024),
        **kw,
    )


def pack_body(target_hbm, velocity_hbm, index_hbm, out_ref, target_ref, velocity_ref, index_ref, sems):
    sources = (target_hbm, index_hbm, velocity_hbm)
    sinks = (target_ref, index_ref, velocity_ref)
    copies = [
        pltpu.make_async_copy(source, sink, sems.at[k])
        for k, (source, sink) in enumerate(zip(sources, sinks))
    ]
    for copy in copies:
        copy.start()
    bricks = 128
    blocks = target_ref.shape[1]
    copies[0].wait()
    target = jnp.broadcast_to(target_ref[...], (bricks, blocks))
    onehot = target == iota((bricks, blocks), 0)
    onehot_bf = jnp.where(onehot, 1.0, 0.0).astype(bf16)
    earlier = jnp.where(iota((blocks, blocks), 0) < iota((blocks, blocks), 1), 1.0, 0.0)
    before = jnp.dot(onehot_bf, earlier.astype(bf16), preferred_element_type=f32)
    places = [
        jnp.where(onehot & (before == float(rank)), 1.0, 0.0).astype(bf16) for rank in range(MOST)
    ]
    copies[1].wait()
    index = index_ref[...]
    plane = (index * 8129) >> 20
    depth = index - plane * (CZ + 1)
    top = depth == CZ
    label = jnp.where(top, PLANES * 128 + plane, plane * 128 + depth)
    label = label.astype(f32) - EMPTY
    copies[2].wait()
    splits = split3(jnp.concatenate([velocity_ref[c] for c in range(3)] + [label], axis=1))
    for rank in range(MOST):
        moved = sum(jnp.dot(places[rank], s, preferred_element_type=f32) for s in reversed(splits))
        for c in range(4):
            value = moved[:, c * 128 : (c + 1) * 128]
            if c == 3:
                value = value + EMPTY
            out_ref[pl.ds(rank * 4 + c, bricks, stride=4 * MOST), :] = value


def axes_body(shift_ref, rotation_ref, out_ref, units_ref, rows):
    base_x = lax.axis_index("gx") * CX + shift_ref[0]
    base_y = lax.axis_index("gy") * CY + shift_ref[1]
    rows[...] = jnp.zeros(rows.shape, i32)
    for ex in range(PX):
        for ey in range(PY):
            a = (base_x + ex) & (APER - 1)
            b = (base_y + ey) & (APER - 1)
            rows[pl.ds(ex * PY + ey, 1), :APER] = rotation_ref[a, pl.ds(b, 1), :]
    value = rows[...].astype(f32)
    value = value + pltpu.roll(value, 32, 1)
    value = value + pltpu.roll(value, 64, 1)
    value = pltpu.roll(value, (128 - shift_ref[2]) & 127, 1)
    first = column_as_row(value)
    out_ref[...] = jnp.where(iota(value.shape, 0) == PLANES, first, value)
    for c, line in enumerate(axis_table((8, 128))):
        units_ref[c] = line


def column_as_row(value):
    column = jnp.broadcast_to(value[:, 0:1], value.shape)
    same = iota(value.shape, 0) == iota(value.shape, 1)
    return jnp.sum(jnp.where(same, column, 0.0), axis=0, keepdims=True)


DEPOSIT_STEP = 128
Q2 = ROWS // 2


def slot_places(slots_ref, rows_q, rows_l):
    slots = slots_ref.shape[0] // 4
    label = slots_ref[pl.ds(3, slots, stride=4), :].astype(i32)
    rows_q[...] = (label >> 8).astype(rows_q.dtype)
    rows_l[...] = jnp.where(label >= PADROWS * 128, 512, label & 255).astype(f32)


def lane_onehot(rows_l, slot, tiles=16):
    step = iota((16, 128), 0).astype(f32).astype(bf16)
    lane = jnp.broadcast_to(rows_l[pl.ds(slot, 1), :], (16, 128)).astype(bf16) - step
    one = jnp.ones((16, 128), bf16)
    zero = jnp.zeros((16, 128), bf16)
    return jnp.concatenate(
        [jnp.where(lane == float(16 * j), one, zero) for j in range(tiles)], axis=0
    )


def sum_rows(slots_ref, rows_q, rows_l, firsts, apart, tiles, store):
    slots = slots_ref.shape[0] // 4
    sub8 = iota((8, 128), 0)
    half = jnp.where(iota((16, 128), 0) >= 8, float(apart), 0.0).astype(bf16)
    zero = jnp.zeros((16, 128), bf16)

    def step(i, carry):
        weighted, depths = [], []
        for k in range(DEPOSIT_STEP):
            slot = i * DEPOSIT_STEP + k
            own = slots_ref[pl.ds(pl.multiple_of(i * DEPOSIT_STEP * 4, 8) + 4 * k, 4), :]
            own = jnp.concatenate([own, own], axis=0)
            high = own.astype(bf16).astype(f32)
            value = jnp.where(sub8 < 4, high, own - high)
            value = jnp.where(sub8 == 3, 1.0, jnp.where(sub8 == 7, 0.0, value))
            value = jnp.concatenate([value, value], axis=0).astype(bf16)
            q = jnp.broadcast_to(rows_q[pl.ds(slot, 1), :], (16, 128)).astype(bf16) - half
            weighted.append(
                jnp.concatenate([jnp.where(q == float(j), value, zero) for j in firsts], axis=0)
            )
            depths.append(lane_onehot(rows_l, slot, tiles).astype(jnp.float8_e4m3fn))
        store(
            lax.dot_general(
                jnp.concatenate(weighted, axis=1),
                jnp.concatenate(depths, axis=1),
                (((1,), (1,)), ((), ())),
                preferred_element_type=f32,
            )
        )
        return carry

    lax.fori_loop(0, slots // DEPOSIT_STEP, step, 0)


def deposit_faces_body(slots_ref, head_ref, tail_ref, acc, rows_q, rows_l):
    slots = slots_ref.shape[0] // 4
    label = slots_ref[pl.ds(3, slots, stride=4), :].astype(i32)
    rows_q[...] = (label >> 7).astype(f32)
    rows_l[...] = (label & 127).astype(f32)
    acc[...] = jnp.zeros(acc.shape, f32)

    def store(got):
        acc[...] += got

    firsts = [ex * PY for ex in range(PX)] + [PLANES]
    sum_rows(slots_ref, rows_q, rows_l, firsts, CY, 8, store)
    for c in range(4):
        for ref, first in ((head_ref, 0), (tail_ref, 8)):
            total = acc[pl.ds(first + c, PX, stride=16), :]
            above = acc[pl.ds(16 * PX + c, 1), :]
            if c < 3:
                total = total + acc[pl.ds(first + c + 4, PX, stride=16), :]
                above = above + acc[pl.ds(16 * PX + c + 4, 1), :]
            ref[c, 0:PX] = total
            ref[c, PX : PX + 1] = above


def deposit_body(slots_ref, total_ref, acc, rows_q, rows_l):
    slot_places(slots_ref, rows_q, rows_l)
    acc[...] = jnp.zeros(acc.shape, f32)

    def store(got):
        acc[0] += got[:, :128]
        acc[1] += got[:, 128:]

    sum_rows(slots_ref, rows_q, rows_l, [2 * j for j in range(12)], 1, 16, store)
    for c in range(4):
        for odd in range(2):
            total = acc[odd, pl.ds(c, Q2, stride=8), :]
            if c < 3:
                total = total + acc[odd, pl.ds(c + 4, Q2, stride=8), :]
            total_ref[c, pl.ds(odd, Q2, stride=2)] = total
        total_ref[c, ROWS:PADROWS] = jnp.zeros((PADROWS - ROWS, 128), f32)


def moved_lanes(row, first, count, shift):
    lane = iota(row.shape, 1)
    rolled = pltpu.roll(row, shift % 128, 1)
    return jnp.where((lane >= first) & (lane < first + count), rolled, 0.0)


def fold_y_body(total_ref, up_ref, down_ref, out_ref, head_ref, tail_ref):
    lane = iota((1, 128), 1)
    edge = lane % PY
    for c in range(4):
        out_ref[c] = total_ref[c]
        out_ref[c, pl.ds(CY, PX, stride=PY)] = (
            total_ref[c, pl.ds(CY, PX, stride=PY)] + up_ref[c, 0:PX]
        )
        out_ref[c, pl.ds(0, PX, stride=PY)] = (
            total_ref[c, pl.ds(0, PX, stride=PY)] + down_ref[c, 0:PX]
        )
        up = pltpu.roll(up_ref[c, PX : PX + 1], CY, 1)
        down = pltpu.roll(down_ref[c, PX : PX + 1], 128 - CY, 1)
        above = (
            total_ref[c, PLANES:ROWS]
            + jnp.where((edge == CY) & (lane < PLANES), up, 0.0)
            + jnp.where((edge == 0) & (lane < PLANES), down, 0.0)
        )
        out_ref[c, PLANES:ROWS] = above
        head_ref[c, 0:PY] = out_ref[c, 0:PY]
        head_ref[c, PY : PY + 1] = above
        tail_ref[c, 0:PY] = out_ref[c, PLANES - PY : PLANES]
        tail_ref[c, PY : PY + 1] = above


def fold_x_body(total_ref, up_ref, down_ref, out_ref, head_ref, tail_ref):
    last = PLANES - PY
    for c in range(4):
        out_ref[c] = total_ref[c]
        out_ref[c, 0:PY] = total_ref[c, 0:PY] + down_ref[c, 0:PY]
        out_ref[c, last:PLANES] = total_ref[c, last:PLANES] + up_ref[c, 0:PY]
        out_ref[c, PLANES:ROWS] = (
            total_ref[c, PLANES:ROWS]
            + moved_lanes(up_ref[c, PY : PY + 1], last, PY, last)
            + moved_lanes(down_ref[c, PY : PY + 1], 0, PY, -last)
        )
        total = out_ref[c]
        head_ref[c : c + 1] = column_as_row(total)
        tail_ref[c : c + 1] = total[PLANES:ROWS]
        head_ref[4 + c : 5 + c] = jnp.zeros((1, 128), f32)
        tail_ref[4 + c : 5 + c] = jnp.zeros((1, 128), f32)


def select_row(rows, bits):
    for bit in bits:
        rows = [
            jnp.where(bit, rows[j + 1], rows[j]) if j + 1 < len(rows) else rows[j]
            for j in range(0, len(rows), 2)
        ]
    return rows[0]


def look_body(
    total_ref, axes_ref, units_ref, slots_ref, found, normal_ref, cells, wide, rows_q, rows_l
):
    slots = slots_ref.shape[0] // 4
    count = jnp.maximum(total_ref[3], 1.0)
    wide[...] = jnp.zeros(wide.shape, f32)

    def tabulate(value, line):
        cells[...] = value
        for odd in range(2):
            wide[odd, pl.ds(line, Q2, stride=8), :] = cells[pl.ds(odd, Q2, stride=2)]

    for c in range(3):
        mean = total_ref[c] / count
        high = mean.astype(bf16).astype(f32)
        tabulate(high, c)
        tabulate(mean - high, c + 4)
    tabulate(axes_ref[...], 3)
    table = jnp.concatenate([wide[0], wide[1]], axis=1).astype(bf16)
    slot_places(slots_ref, rows_q, rows_l)
    sub8 = iota((8, 128), 0)
    for k in range(slots // 2):
        pair = [2 * k, 2 * k + 1]
        hot = jnp.concatenate([lane_onehot(rows_l, slot) for slot in pair], axis=1)
        read = jnp.dot(table, hot, preferred_element_type=f32)
        got = []
        for h in range(2):
            q = jnp.broadcast_to(rows_q[pl.ds(pair[h], 1), :], (8, 128))
            bits = [(q & (1 << b)) != 0 for b in range(5)]
            lines = [read[8 * j : 8 * j + 8, 128 * h : 128 * h + 128] for j in range(Q2)]
            value = select_row(lines, bits)
            got.append(value + pltpu.roll(value, 4, 0))
        found[pl.ds(8 * k, 8), :] = jnp.where(sub8 < 4, got[0], got[1])
        if (k + 1) % (4 * MOST) == 0:
            g = k // (4 * MOST)
            for rank in range(MOST):
                which = found[pl.ds((g * 8 * MOST + rank) * 4 + 3, 8, stride=4 * MOST), :]
                for c in range(3):
                    normal_ref[rank, c, pl.ds(8 * g, 8), :] = jnp.take_along_axis(
                        units_ref[c], which.astype(i32), axis=1
                    )


SENDERS = 32


def turn_body(
    total_ref, up_ref, down_ref, normal_ref, slots_ref, found, out_hbm, flow_hbm,
    out_ref, flow_ref, sems
):
    devices = out_ref.shape[2]
    shape = (PADROWS, 128)
    row = iota(shape, 0)
    lane = iota(shape, 1)
    top = (row == PLANES) & (lane < PLANES)
    totals = []
    for c in range(4):
        own = total_ref[c]
        column = jnp.sum(
            jnp.where((row == lane) & (row < PLANES), down_ref[c : c + 1], 0.0),
            axis=1,
            keepdims=True,
        )
        own = own + jnp.where(lane == 0, column, 0.0)
        totals.append(own + jnp.where(top, up_ref[c : c + 1], 0.0))
    count = jnp.maximum(totals[3], 1.0)
    rims = []
    for c in range(3):
        mean = totals[c] / count
        for ex in range(CX):
            flow_ref[c, ex] = mean[ex * PY : ex * PY + CY]
        low = pltpu.roll(column_as_row(mean), 64, 1)
        rim = jnp.where(iota((1, 128), 1) < 64, mean[PLANES:ROWS], low)
        rims.append(jnp.broadcast_to(rim, (8, 128)))
    parts = devices // SENDERS
    flow_copy = pltpu.make_async_copy(flow_ref, flow_hbm, sems.at[parts])
    flow_copy.start()

    def copy(i):
        part = pl.ds(i * SENDERS, SENDERS)
        return pltpu.make_async_copy(
            out_ref.at[:, :, part, :], out_hbm.at[:, :, part, :], sems.at[i]
        )

    for i in range(parts):
        for rank in range(MOST):
            for k in range(SENDERS // 8):
                source = i * SENDERS + 8 * k
                place = (source * MOST + rank) * 4
                label = slots_ref[pl.ds(place + 3, 8, stride=12), :].astype(i32)
                q = label >> 7
                l = label & 127
                above = q == PLANES
                below = (l == 0) & (q < PLANES)
                rim_lane = jnp.where(above, l, (q + 64) & 127)
                n = [normal_ref[rank, c, pl.ds(source, 8), :] for c in range(3)]
                u = [
                    jnp.where(
                        above | below,
                        jnp.take_along_axis(rims[c], rim_lane, axis=1),
                        found[pl.ds(place + c, 8, stride=12), :],
                    )
                    for c in range(3)
                ]
                w = [slots_ref[pl.ds(place + c, 8, stride=12), :] - u[c] for c in range(3)]
                inner = n[0] * w[0] + n[1] * w[1] + n[2] * w[2]
                crossed = [
                    n[1] * w[2] - n[2] * w[1],
                    n[2] * w[0] - n[0] * w[2],
                    n[0] * w[1] - n[1] * w[0],
                ]
                for c in range(3):
                    out_ref[rank, c, pl.ds(source, 8), :] = (
                        u[c]
                        + w[c] * angle_cosine
                        + crossed[c] * angle_sine
                        + n[c] * inner * (1.0 - angle_cosine)
                    )
        copy(i).start()
    for i in range(parts):
        copy(i).wait()
    flow_copy.wait()


def both_ways(head, tail, axis):
    count = lax.axis_size(axis)
    up = lax.ppermute(head, axis, [((i + 1) % count, i) for i in range(count)])
    down = lax.ppermute(tail, axis, [(i, (i + 1) % count) for i in range(count)])
    return up, down


def shards(velocity, cell_index, block_target, rotation_axis, grid_shift):
    devices = 128
    shape = jax.ShapeDtypeStruct
    vmem = pl.BlockSpec(memory_space=pltpu.VMEM)
    smem = pl.BlockSpec(memory_space=pltpu.SMEM)
    hbm = pl.BlockSpec(memory_space=pltpu.HBM)
    blocks = velocity.shape[0]
    send = call(
        pack_body,
        shape((devices * MOST * 4, 128), f32),
        in_specs=[hbm, hbm, hbm],
        scratch_shapes=[
            pltpu.VMEM((1, blocks), i32),
            pltpu.VMEM((3, blocks, 128), f32),
            pltpu.VMEM((blocks, 128), i32),
            pltpu.SemaphoreType.DMA((3,)),
        ],
        name="pack",
    )(
        *(
            pltpu.with_memory_space_constraint(x, pltpu.HBM)
            for x in (block_target.reshape(1, -1), jnp.transpose(velocity, (1, 0, 2)), cell_index)
        )
    )
    axes, units = call(
        axes_body,
        [shape((PADROWS, 128), f32), shape((3, 8, 128), f32)],
        in_specs=[smem, vmem],
        scratch_shapes=[pltpu.VMEM((PADROWS, 128), i32)],
        name="axes",
    )(grid_shift, rotation_axis)
    slots = lax.all_to_all(
        send.reshape(devices, MOST, 4, 128), ("gx", "gy", "gz"), split_axis=0, concat_axis=0, tiled=True
    ).reshape(devices * MOST * 4, 128)
    total_shape = shape((4, PADROWS, 128), f32)
    x_face = shape((4, 16, 128), f32)
    y_face = shape((4, 8, 128), f32)
    z_face = shape((8, 128), f32)
    by_slot = pltpu.VMEM((devices * MOST, 128), f32)
    head, tail = call(
        deposit_faces_body,
        [y_face, y_face],
        scratch_shapes=[pltpu.VMEM((16 * (PX + 1), 128), f32), by_slot, by_slot],
        name="deposit_faces",
    )(slots)
    slots, head, tail = lax.optimization_barrier((slots, head, tail))
    up, down = both_ways(head, tail, "gy")
    total = call(
        deposit_body,
        total_shape,
        scratch_shapes=[pltpu.VMEM((2, 192, 128), f32), by_slot, by_slot],
        name="deposit",
    )(slots)
    total, head, tail = call(fold_y_body, [total_shape, x_face, x_face], name="fold_y")(
        total, up, down
    )
    up, down = both_ways(head, tail, "gx")
    up, down, axes, units = lax.optimization_barrier((up, down, axes, units))
    total, head, tail = call(fold_x_body, [total_shape, z_face, z_face], name="fold_x")(
        total, up, down
    )
    up, down = both_ways(head, tail, "gz")
    found, normal = call(
        look_body,
        [shape((devices * MOST * 4, 128), f32), shape((MOST, 3, devices, 128), f32)],
        scratch_shapes=[
            pltpu.VMEM((PADROWS, 128), f32),
            pltpu.VMEM((2, Q2 * 8, 128), f32),
            pltpu.VMEM((devices * MOST, 128), i32),
            pltpu.VMEM((devices * MOST, 128), f32),
        ],
        name="look",
    )(total, axes, units, slots)
    updated, cell_flow = call(
        turn_body,
        [shape((MOST, 3, devices, 128), f32), shape((3, CX, CY, CZ), f32)],
        out_specs=[hbm, hbm],
        scratch_shapes=[
            pltpu.VMEM((MOST, 3, devices, 128), f32),
            pltpu.VMEM((3, CX, CY, CZ), f32),
            pltpu.SemaphoreType.DMA((devices // SENDERS + 1,)),
        ],
        name="turn",
    )(total, up, down, normal, slots, found)
    return jnp.transpose(updated, (2, 0, 1, 3))[None], cell_flow


def solution(mesh):
    return jax.shard_map(
        shards,
        mesh=mesh,
        in_specs=(
            P(("gx", "gy", "gz"), None, None),
            P(("gx", "gy", "gz"), None),
            P(("gx", "gy", "gz"), None),
            P(),
            P(),
        ),
        out_specs=(P(("gx", "gy", "gz"), None, None, None, None), P(None, "gx", "gy", "gz")),
        check_vma=False,
    )
```

```python
import functools

import jax
import jax.numpy as jnp
from jax import lax
from jax.experimental import pallas as pl
from jax.experimental.pallas import tpu as pltpu
from jax.sharding import PartitionSpec as P

CX = 4
CY = 8
CZ = 128
NAX = 64
APER = 32
MOST = 3
PX = CX + 1
PY = CY + 1
PLANES = PX * PY
ROWS = PLANES + 1
PADROWS = 48
EMPTY = 6400.0

angle_cosine = -0.6427876096865393
angle_sine = 0.766044443118978

f32 = jnp.float32
bf16 = jnp.bfloat16
i32 = jnp.int32


def iota(shape, dim):
    return lax.broadcasted_iota(i32, shape, dim)


def axis_table(shape):
    counter = iota(shape, 1).astype(f32) + 0.5
    height = 1.0 - 2.0 * counter / NAX
    radius = jnp.sqrt(jnp.maximum(1.0 - height * height, 0.0))
    turning = counter * 2.399963229728653
    return radius * jnp.cos(turning), radius * jnp.sin(turning), height


def split3(value):
    high = value.astype(bf16)
    rest = value - high.astype(f32)
    middle = rest.astype(bf16)
    return high, middle, (rest - middle.astype(f32)).astype(bf16)


def call(body, out_shape, **kw):
    return pl.pallas_call(
        body,
        out_shape=out_shape,
        compiler_params=pltpu.CompilerParams(vmem_limit_bytes=48 * 1024 * 1024),
        **kw,
    )


def pack_body(target_hbm, velocity_hbm, index_hbm, out_ref, target_ref, velocity_ref, index_ref, sems):
    sources = (target_hbm, index_hbm, velocity_hbm)
    sinks = (target_ref, index_ref, velocity_ref)
    copies = [
        pltpu.make_async_copy(source, sink, sems.at[k])
        for k, (source, sink) in enumerate(zip(sources, sinks))
    ]
    for copy in copies:
        copy.start()
    bricks = 128
    blocks = target_ref.shape[1]
    copies[0].wait()
    target = jnp.broadcast_to(target_ref[...], (bricks, blocks))
    onehot = target == iota((bricks, blocks), 0)
    onehot_bf = jnp.where(onehot, 1.0, 0.0).astype(bf16)
    earlier = jnp.where(iota((blocks, blocks), 0) < iota((blocks, blocks), 1), 1.0, 0.0)
    before = jnp.dot(onehot_bf, earlier.astype(bf16), preferred_element_type=f32)
    places = [
        jnp.where(onehot & (before == float(rank)), 1.0, 0.0).astype(bf16) for rank in range(MOST)
    ]
    copies[1].wait()
    index = index_ref[...]
    plane = (index * 8129) >> 20
    depth = index - plane * (CZ + 1)
    top = depth == CZ
    label = jnp.where(top, PLANES * 128 + plane, plane * 128 + depth)
    label = label.astype(f32) - EMPTY
    copies[2].wait()
    splits = split3(jnp.concatenate([velocity_ref[c] for c in range(3)] + [label], axis=1))
    for rank in range(MOST):
        moved = sum(jnp.dot(places[rank], s, preferred_element_type=f32) for s in reversed(splits))
        for c in range(4):
            value = moved[:, c * 128 : (c + 1) * 128]
            if c == 3:
                value = value + EMPTY
            out_ref[pl.ds(rank * 4 + c, bricks, stride=4 * MOST), :] = value


def axes_body(shift_ref, rotation_ref, out_ref, units_ref, rows):
    base_x = lax.axis_index("gx") * CX + shift_ref[0]
    base_y = lax.axis_index("gy") * CY + shift_ref[1]
    rows[...] = jnp.zeros(rows.shape, i32)
    for ex in range(PX):
        for ey in range(PY):
            a = (base_x + ex) & (APER - 1)
            b = (base_y + ey) & (APER - 1)
            rows[pl.ds(ex * PY + ey, 1), :APER] = rotation_ref[a, pl.ds(b, 1), :]
    value = rows[...].astype(f32)
    value = value + pltpu.roll(value, 32, 1)
    value = value + pltpu.roll(value, 64, 1)
    value = pltpu.roll(value, (128 - shift_ref[2]) & 127, 1)
    first = column_as_row(value)
    out_ref[...] = jnp.where(iota(value.shape, 0) == PLANES, first, value)
    for c, line in enumerate(axis_table((8, 128))):
        units_ref[c] = line


def column_as_row(value):
    column = jnp.broadcast_to(value[:, 0:1], value.shape)
    same = iota(value.shape, 0) == iota(value.shape, 1)
    return jnp.sum(jnp.where(same, column, 0.0), axis=0, keepdims=True)


DEPOSIT_STEP = 128
Q2 = ROWS // 2


def slot_places(slots_ref, rows_q, rows_l):
    slots = slots_ref.shape[0] // 4
    label = slots_ref[pl.ds(3, slots, stride=4), :].astype(i32)
    rows_q[...] = (label >> 8).astype(rows_q.dtype)
    rows_l[...] = jnp.where(label >= PADROWS * 128, 512, label & 255).astype(f32)


def lane_onehot(rows_l, slot, tiles=16):
    step = iota((16, 128), 0).astype(f32).astype(bf16)
    lane = jnp.broadcast_to(rows_l[pl.ds(slot, 1), :], (16, 128)).astype(bf16) - step
    one = jnp.ones((16, 128), bf16)
    zero = jnp.zeros((16, 128), bf16)
    return jnp.concatenate(
        [jnp.where(lane == float(16 * j), one, zero) for j in range(tiles)], axis=0
    )


def sum_rows(slots_ref, rows_q, rows_l, firsts, apart, tiles, store):
    slots = slots_ref.shape[0] // 4
    sub8 = iota((8, 128), 0)
    half = jnp.where(iota((16, 128), 0) >= 8, float(apart), 0.0).astype(bf16)
    zero = jnp.zeros((16, 128), bf16)

    def step(i, carry):
        weighted, depths = [], []
        for k in range(DEPOSIT_STEP):
            slot = i * DEPOSIT_STEP + k
            own = slots_ref[pl.ds(pl.multiple_of(i * DEPOSIT_STEP * 4, 8) + 4 * k, 4), :]
            own = jnp.concatenate([own, own], axis=0)
            high = own.astype(bf16).astype(f32)
            value = jnp.where(sub8 < 4, high, own - high)
            value = jnp.where(sub8 == 3, 1.0, jnp.where(sub8 == 7, 0.0, value))
            value = jnp.concatenate([value, value], axis=0).astype(bf16)
            q = jnp.broadcast_to(rows_q[pl.ds(slot, 1), :], (16, 128)).astype(bf16) - half
            weighted.append(
                jnp.concatenate([jnp.where(q == float(j), value, zero) for j in firsts], axis=0)
            )
            depths.append(lane_onehot(rows_l, slot, tiles).astype(jnp.float8_e4m3fn))
        store(
            lax.dot_general(
                jnp.concatenate(weighted, axis=1),
                jnp.concatenate(depths, axis=1),
                (((1,), (1,)), ((), ())),
                preferred_element_type=f32,
            )
        )
        return carry

    lax.fori_loop(0, slots // DEPOSIT_STEP, step, 0)


def deposit_faces_body(slots_ref, head_ref, tail_ref, acc, rows_q, rows_l):
    slots = slots_ref.shape[0] // 4
    label = slots_ref[pl.ds(3, slots, stride=4), :].astype(i32)
    rows_q[...] = (label >> 7).astype(f32)
    rows_l[...] = (label & 127).astype(f32)
    acc[...] = jnp.zeros(acc.shape, f32)

    def store(got):
        acc[...] += got

    firsts = [ex * PY for ex in range(PX)] + [PLANES]
    sum_rows(slots_ref, rows_q, rows_l, firsts, CY, 8, store)
    for c in range(4):
        for ref, first in ((head_ref, 0), (tail_ref, 8)):
            total = acc[pl.ds(first + c, PX, stride=16), :]
            above = acc[pl.ds(16 * PX + c, 1), :]
            if c < 3:
                total = total + acc[pl.ds(first + c + 4, PX, stride=16), :]
                above = above + acc[pl.ds(16 * PX + c + 4, 1), :]
            ref[c, 0:PX] = total
            ref[c, PX : PX + 1] = above


def deposit_sides_body(slots_ref, out_ref, acc, rows_q, rows_l):
    slots = slots_ref.shape[0] // 4
    label = slots_ref[pl.ds(3, slots, stride=4), :].astype(i32)
    rows_q[...] = (label >> 7).astype(f32)
    rows_l[...] = (label & 127).astype(f32)
    acc[...] = jnp.zeros(acc.shape, f32)

    def store(got):
        acc[...] += got

    sum_rows(slots_ref, rows_q, rows_l, list(range(1, CY)), CX * PY, 8, store)
    for c in range(4):
        for first in (0, 8):
            total = acc[pl.ds(first + c, CY - 1, stride=16), :]
            if c < 3:
                total = total + acc[pl.ds(first + c + 4, CY - 1, stride=16), :]
            out_ref[c, first : first + CY - 1] = total


IN_X = CX - 1
IN_Y = CY - 1
IN_HALF = (IN_X * IN_Y + 1) // 2


def deposit_inner_body(slots_ref, out_ref, acc, rows_q, rows_l):
    slots = slots_ref.shape[0] // 4
    label = slots_ref[pl.ds(3, slots, stride=4), :].astype(i32)
    row = label >> 7
    ex = (row * 57) >> 9
    ey = row - ex * PY
    here = (ex >= 1) & (ex < CX) & (ey >= 1) & (ey < CY)
    place = (ex - 1) * IN_Y + ey - 1
    rows_q[...] = (place >> 1).astype(f32)
    rows_l[...] = jnp.where(here, (place & 1) * 128 + (label & 127), 512).astype(f32)
    acc[...] = jnp.zeros(acc.shape, f32)

    def store(got):
        acc[0] += got[:, :128]
        acc[1] += got[:, 128:]

    sum_rows(slots_ref, rows_q, rows_l, list(range(0, IN_HALF, 2)), 1, 16, store)
    for c in range(4):
        for odd in range(2):
            total = acc[odd, pl.ds(c, IN_HALF, stride=8), :]
            if c < 3:
                total = total + acc[odd, pl.ds(c + 4, IN_HALF, stride=8), :]
            out_ref[c, pl.ds(odd, IN_HALF, stride=2)] = total


def moved_lanes(row, first, count, shift):
    lane = iota(row.shape, 1)
    rolled = pltpu.roll(row, shift % 128, 1)
    return jnp.where((lane >= first) & (lane < first + count), rolled, 0.0)


def fold_y_body(
    own_low, own_high, sides_ref, up_ref, down_ref, low_ref, high_ref, head_ref, tail_ref
):
    lane = iota((1, 128), 1)
    edge = lane % PY
    for c in range(4):
        low_ref[c, 0:PX] = own_low[c, 0:PX] + down_ref[c, 0:PX]
        high_ref[c, 0:PX] = own_high[c, 0:PX] + up_ref[c, 0:PX]
        up = pltpu.roll(up_ref[c, PX : PX + 1], CY, 1)
        down = pltpu.roll(down_ref[c, PX : PX + 1], 128 - CY, 1)
        above = (
            own_low[c, PX : PX + 1]
            + jnp.where((edge == CY) & (lane < PLANES), up, 0.0)
            + jnp.where((edge == 0) & (lane < PLANES), down, 0.0)
        )
        low_ref[c, PX : PX + 1] = above
        for ref, ex, first in ((head_ref, 0, 0), (tail_ref, CX, 8)):
            ref[c, 0:1] = low_ref[c, ex : ex + 1]
            ref[c, 1:CY] = sides_ref[c, first : first + CY - 1]
            ref[c, CY:PY] = high_ref[c, ex : ex + 1]
            ref[c, PY : PY + 1] = above


def fold_x_body(
    inner_ref, low_ref, high_ref, own_head, own_tail, up_ref, down_ref, out_ref, head_ref, tail_ref
):
    last = PLANES - PY
    for c in range(4):
        out_ref[c, 0:PY] = own_head[c, 0:PY] + down_ref[c, 0:PY]
        for ex in range(1, CX):
            row = ex * PY
            out_ref[c, row : row + 1] = low_ref[c, ex : ex + 1]
            out_ref[c, row + 1 : row + CY] = inner_ref[c, (ex - 1) * IN_Y : ex * IN_Y]
            out_ref[c, row + CY : row + PY] = high_ref[c, ex : ex + 1]
        out_ref[c, last:PLANES] = own_tail[c, 0:PY] + up_ref[c, 0:PY]
        out_ref[c, PLANES:ROWS] = (
            low_ref[c, PX : PX + 1]
            + moved_lanes(up_ref[c, PY : PY + 1], last, PY, last)
            + moved_lanes(down_ref[c, PY : PY + 1], 0, PY, -last)
        )
        out_ref[c, ROWS:PADROWS] = jnp.zeros((PADROWS - ROWS, 128), f32)
        total = out_ref[c]
        head_ref[c : c + 1] = column_as_row(total)
        tail_ref[c : c + 1] = total[PLANES:ROWS]
        head_ref[4 + c : 5 + c] = jnp.zeros((1, 128), f32)
        tail_ref[4 + c : 5 + c] = jnp.zeros((1, 128), f32)


def select_row(rows, bits):
    for bit in bits:
        rows = [
            jnp.where(bit, rows[j + 1], rows[j]) if j + 1 < len(rows) else rows[j]
            for j in range(0, len(rows), 2)
        ]
    return rows[0]


def look_body(
    total_ref, axes_ref, units_ref, slots_ref, found, normal_ref, cells, wide, rows_q, rows_l
):
    slots = slots_ref.shape[0] // 4
    count = jnp.maximum(total_ref[3], 1.0)
    wide[...] = jnp.zeros(wide.shape, f32)

    def tabulate(value, line):
        cells[...] = value
        for odd in range(2):
            wide[odd, pl.ds(line, Q2, stride=8), :] = cells[pl.ds(odd, Q2, stride=2)]

    for c in range(3):
        mean = total_ref[c] / count
        high = mean.astype(bf16).astype(f32)
        tabulate(high, c)
        tabulate(mean - high, c + 4)
    tabulate(axes_ref[...], 3)
    table = jnp.concatenate([wide[0], wide[1]], axis=1).astype(bf16)
    slot_places(slots_ref, rows_q, rows_l)
    sub8 = iota((8, 128), 0)
    for k in range(slots // 2):
        pair = [2 * k, 2 * k + 1]
        hot = jnp.concatenate([lane_onehot(rows_l, slot) for slot in pair], axis=1)
        read = jnp.dot(table, hot, preferred_element_type=f32)
        got = []
        for h in range(2):
            q = jnp.broadcast_to(rows_q[pl.ds(pair[h], 1), :], (8, 128))
            bits = [(q & (1 << b)) != 0 for b in range(5)]
            lines = [read[8 * j : 8 * j + 8, 128 * h : 128 * h + 128] for j in range(Q2)]
            value = select_row(lines, bits)
            got.append(value + pltpu.roll(value, 4, 0))
        found[pl.ds(8 * k, 8), :] = jnp.where(sub8 < 4, got[0], got[1])
        if (k + 1) % (4 * MOST) == 0:
            g = k // (4 * MOST)
            for rank in range(MOST):
                which = found[pl.ds((g * 8 * MOST + rank) * 4 + 3, 8, stride=4 * MOST), :]
                for c in range(3):
                    normal_ref[rank, c, pl.ds(8 * g, 8), :] = jnp.take_along_axis(
                        units_ref[c], which.astype(i32), axis=1
                    )


SENDERS = 32


def turn_body(
    total_ref, up_ref, down_ref, normal_ref, slots_ref, found, out_hbm, flow_hbm,
    out_ref, flow_ref, sems
):
    devices = out_ref.shape[2]
    shape = (PADROWS, 128)
    row = iota(shape, 0)
    lane = iota(shape, 1)
    top = (row == PLANES) & (lane < PLANES)
    totals = []
    for c in range(4):
        own = total_ref[c]
        column = jnp.sum(
            jnp.where((row == lane) & (row < PLANES), down_ref[c : c + 1], 0.0),
            axis=1,
            keepdims=True,
        )
        own = own + jnp.where(lane == 0, column, 0.0)
        totals.append(own + jnp.where(top, up_ref[c : c + 1], 0.0))
    count = jnp.maximum(totals[3], 1.0)
    rims = []
    for c in range(3):
        mean = totals[c] / count
        for ex in range(CX):
            flow_ref[c, ex] = mean[ex * PY : ex * PY + CY]
        low = pltpu.roll(column_as_row(mean), 64, 1)
        rim = jnp.where(iota((1, 128), 1) < 64, mean[PLANES:ROWS], low)
        rims.append(jnp.broadcast_to(rim, (8, 128)))
    parts = devices // SENDERS
    flow_copy = pltpu.make_async_copy(flow_ref, flow_hbm, sems.at[parts])
    flow_copy.start()

    def copy(i):
        part = pl.ds(i * SENDERS, SENDERS)
        return pltpu.make_async_copy(
            out_ref.at[:, :, part, :], out_hbm.at[:, :, part, :], sems.at[i]
        )

    for i in range(parts):
        for rank in range(MOST):
            for k in range(SENDERS // 8):
                source = i * SENDERS + 8 * k
                place = (source * MOST + rank) * 4
                label = slots_ref[pl.ds(place + 3, 8, stride=12), :].astype(i32)
                q = label >> 7
                l = label & 127
                above = q == PLANES
                below = (l == 0) & (q < PLANES)
                rim_lane = jnp.where(above, l, (q + 64) & 127)
                n = [normal_ref[rank, c, pl.ds(source, 8), :] for c in range(3)]
                u = [
                    jnp.where(
                        above | below,
                        jnp.take_along_axis(rims[c], rim_lane, axis=1),
                        found[pl.ds(place + c, 8, stride=12), :],
                    )
                    for c in range(3)
                ]
                w = [slots_ref[pl.ds(place + c, 8, stride=12), :] - u[c] for c in range(3)]
                inner = n[0] * w[0] + n[1] * w[1] + n[2] * w[2]
                crossed = [
                    n[1] * w[2] - n[2] * w[1],
                    n[2] * w[0] - n[0] * w[2],
                    n[0] * w[1] - n[1] * w[0],
                ]
                for c in range(3):
                    out_ref[rank, c, pl.ds(source, 8), :] = (
                        u[c]
                        + w[c] * angle_cosine
                        + crossed[c] * angle_sine
                        + n[c] * inner * (1.0 - angle_cosine)
                    )
        copy(i).start()
    for i in range(parts):
        copy(i).wait()
    flow_copy.wait()


def both_ways(head, tail, axis):
    count = lax.axis_size(axis)
    up = lax.ppermute(head, axis, [((i + 1) % count, i) for i in range(count)])
    down = lax.ppermute(tail, axis, [(i, (i + 1) % count) for i in range(count)])
    return up, down


def shards(velocity, cell_index, block_target, rotation_axis, grid_shift):
    devices = 128
    shape = jax.ShapeDtypeStruct
    vmem = pl.BlockSpec(memory_space=pltpu.VMEM)
    smem = pl.BlockSpec(memory_space=pltpu.SMEM)
    hbm = pl.BlockSpec(memory_space=pltpu.HBM)
    blocks = velocity.shape[0]
    send = call(
        pack_body,
        shape((devices * MOST * 4, 128), f32),
        in_specs=[hbm, hbm, hbm],
        scratch_shapes=[
            pltpu.VMEM((1, blocks), i32),
            pltpu.VMEM((3, blocks, 128), f32),
            pltpu.VMEM((blocks, 128), i32),
            pltpu.SemaphoreType.DMA((3,)),
        ],
        name="pack",
    )(
        *(
            pltpu.with_memory_space_constraint(x, pltpu.HBM)
            for x in (block_target.reshape(1, -1), jnp.transpose(velocity, (1, 0, 2)), cell_index)
        )
    )
    axes, units = call(
        axes_body,
        [shape((PADROWS, 128), f32), shape((3, 8, 128), f32)],
        in_specs=[smem, vmem],
        scratch_shapes=[pltpu.VMEM((PADROWS, 128), i32)],
        name="axes",
    )(grid_shift, rotation_axis)
    slots = lax.all_to_all(
        send.reshape(devices, MOST, 4, 128), ("gx", "gy", "gz"), split_axis=0, concat_axis=0, tiled=True
    ).reshape(devices * MOST * 4, 128)
    total_shape = shape((4, PADROWS, 128), f32)
    x_face = shape((4, 16, 128), f32)
    y_face = shape((4, 8, 128), f32)
    z_face = shape((8, 128), f32)
    by_slot = pltpu.VMEM((devices * MOST, 128), f32)
    head, tail = call(
        deposit_faces_body,
        [y_face, y_face],
        scratch_shapes=[pltpu.VMEM((16 * (PX + 1), 128), f32), by_slot, by_slot],
        name="deposit_faces",
    )(slots)
    slots, low, high = lax.optimization_barrier((slots, head, tail))
    up, down = both_ways(low, high, "gy")
    sides = call(
        deposit_sides_body,
        x_face,
        scratch_shapes=[pltpu.VMEM((16 * (CY - 1), 128), f32), by_slot, by_slot],
        name="deposit_sides",
    )(slots)
    low, high, head, tail = call(
        fold_y_body, [y_face, y_face, x_face, x_face], name="fold_y"
    )(low, high, sides, up, down)
    slots, head, tail = lax.optimization_barrier((slots, head, tail))
    up, down = both_ways(head, tail, "gx")
    inner = call(
        deposit_inner_body,
        shape((4, 24, 128), f32),
        scratch_shapes=[pltpu.VMEM((2, 96, 128), f32), by_slot, by_slot],
        name="deposit_inner",
    )(slots)
    up, down, axes, units, inner = lax.optimization_barrier((up, down, axes, units, inner))
    total, head, tail = call(fold_x_body, [total_shape, z_face, z_face], name="fold_x")(
        inner, low, high, head, tail, up, down
    )
    up, down = both_ways(head, tail, "gz")
    found, normal = call(
        look_body,
        [shape((devices * MOST * 4, 128), f32), shape((MOST, 3, devices, 128), f32)],
        scratch_shapes=[
            pltpu.VMEM((PADROWS, 128), f32),
            pltpu.VMEM((2, Q2 * 8, 128), f32),
            pltpu.VMEM((devices * MOST, 128), i32),
            pltpu.VMEM((devices * MOST, 128), f32),
        ],
        name="look",
    )(total, axes, units, slots)
    updated, cell_flow = call(
        turn_body,
        [shape((MOST, 3, devices, 128), f32), shape((3, CX, CY, CZ), f32)],
        out_specs=[hbm, hbm],
        scratch_shapes=[
            pltpu.VMEM((MOST, 3, devices, 128), f32),
            pltpu.VMEM((3, CX, CY, CZ), f32),
            pltpu.SemaphoreType.DMA((devices // SENDERS + 1,)),
        ],
        name="turn",
    )(total, up, down, normal, slots, found)
    return jnp.transpose(updated, (2, 0, 1, 3))[None], cell_flow


def solution(mesh):
    return jax.shard_map(
        shards,
        mesh=mesh,
        in_specs=(
            P(("gx", "gy", "gz"), None, None),
            P(("gx", "gy", "gz"), None),
            P(("gx", "gy", "gz"), None),
            P(),
            P(),
        ),
        out_specs=(P(("gx", "gy", "gz"), None, None, None, None), P(None, "gx", "gy", "gz")),
        check_vma=False,
    )
```

```python
import functools

import jax
import jax.numpy as jnp
from jax import lax
from jax.experimental import pallas as pl
from jax.experimental.pallas import tpu as pltpu
from jax.sharding import PartitionSpec as P

CX = 4
CY = 8
CZ = 128
NAX = 64
APER = 32
MOST = 3
PX = CX + 1
PY = CY + 1
PLANES = PX * PY
ROWS = PLANES + 1
PADROWS = 48
EMPTY = 6400.0

angle_cosine = -0.6427876096865393
angle_sine = 0.766044443118978

f32 = jnp.float32
bf16 = jnp.bfloat16
i32 = jnp.int32


def iota(shape, dim):
    return lax.broadcasted_iota(i32, shape, dim)


def axis_table(shape):
    counter = iota(shape, 1).astype(f32) + 0.5
    height = 1.0 - 2.0 * counter / NAX
    radius = jnp.sqrt(jnp.maximum(1.0 - height * height, 0.0))
    turning = counter * 2.399963229728653
    return radius * jnp.cos(turning), radius * jnp.sin(turning), height


def split3(value):
    high = value.astype(bf16)
    rest = value - high.astype(f32)
    middle = rest.astype(bf16)
    return high, middle, (rest - middle.astype(f32)).astype(bf16)


def call(body, out_shape, **kw):
    return pl.pallas_call(
        body,
        out_shape=out_shape,
        compiler_params=pltpu.CompilerParams(vmem_limit_bytes=48 * 1024 * 1024),
        **kw,
    )


def pack_body(
    target_hbm, velocity_hbm, index_hbm, out_ref, units_ref, target_ref, velocity_ref, index_ref, sems
):
    sources = (target_hbm, index_hbm, velocity_hbm)
    sinks = (target_ref, index_ref, velocity_ref)
    copies = [
        pltpu.make_async_copy(source, sink, sems.at[k])
        for k, (source, sink) in enumerate(zip(sources, sinks))
    ]
    for copy in copies:
        copy.start()
    for c, line in enumerate(axis_table((8, 128))):
        units_ref[c] = line
    bricks = 128
    blocks = target_ref.shape[1]
    copies[0].wait()
    target = jnp.broadcast_to(target_ref[...], (bricks, blocks))
    onehot = target == iota((bricks, blocks), 0)
    onehot_bf = jnp.where(onehot, 1.0, 0.0).astype(bf16)
    earlier = jnp.where(iota((blocks, blocks), 0) < iota((blocks, blocks), 1), 1.0, 0.0)
    before = jnp.dot(onehot_bf, earlier.astype(bf16), preferred_element_type=f32)
    places = [
        jnp.where(onehot & (before == float(rank)), 1.0, 0.0).astype(bf16) for rank in range(MOST)
    ]
    copies[1].wait()
    index = index_ref[...]
    plane = (index * 8129) >> 20
    depth = index - plane * (CZ + 1)
    top = depth == CZ
    label = jnp.where(top, PLANES * 128 + plane, plane * 128 + depth)
    label = label.astype(f32) - EMPTY
    copies[2].wait()
    splits = split3(jnp.concatenate([velocity_ref[c] for c in range(3)] + [label], axis=1))
    for rank in range(MOST):
        moved = sum(jnp.dot(places[rank], s, preferred_element_type=f32) for s in reversed(splits))
        for c in range(4):
            value = moved[:, c * 128 : (c + 1) * 128]
            if c == 3:
                value = value + EMPTY
            out_ref[pl.ds(rank * 4 + c, bricks, stride=4 * MOST), :] = value


def axes_body(shift_ref, rotation_ref, out_ref, rows):
    base_x = lax.axis_index("gx") * CX + shift_ref[0]
    base_y = lax.axis_index("gy") * CY + shift_ref[1]
    rows[...] = jnp.zeros(rows.shape, i32)
    for ex in range(PX):
        for ey in range(PY):
            a = (base_x + ex) & (APER - 1)
            b = (base_y + ey) & (APER - 1)
            rows[pl.ds(ex * PY + ey, 1), :APER] = rotation_ref[a, pl.ds(b, 1), :]
    value = rows[...].astype(f32)
    value = value + pltpu.roll(value, 32, 1)
    value = value + pltpu.roll(value, 64, 1)
    value = pltpu.roll(value, (128 - shift_ref[2]) & 127, 1)
    first = column_as_row(value)
    out_ref[...] = jnp.where(iota(value.shape, 0) == PLANES, first, value)


def column_as_row(value):
    column = jnp.broadcast_to(value[:, 0:1], value.shape)
    same = iota(value.shape, 0) == iota(value.shape, 1)
    return jnp.sum(jnp.where(same, column, 0.0), axis=0, keepdims=True)


DEPOSIT_STEP = 128
Q2 = ROWS // 2


def slot_places(slots_ref, rows_q, rows_l):
    slots = slots_ref.shape[0] // 4
    label = slots_ref[pl.ds(3, slots, stride=4), :].astype(i32)
    rows_q[...] = (label >> 8).astype(rows_q.dtype)
    rows_l[...] = jnp.where(label >= PADROWS * 128, 512, label & 255).astype(f32)


def lane_onehot(rows_l, slot, tiles=16):
    step = iota((16, 128), 0).astype(f32).astype(bf16)
    lane = jnp.broadcast_to(rows_l[pl.ds(slot, 1), :], (16, 128)).astype(bf16) - step
    one = jnp.ones((16, 128), bf16)
    zero = jnp.zeros((16, 128), bf16)
    return jnp.concatenate(
        [jnp.where(lane == float(16 * j), one, zero) for j in range(tiles)], axis=0
    )


def sum_rows(slots_ref, rows_q, rows_l, firsts, apart, tiles, store):
    slots = slots_ref.shape[0] // 4
    sub8 = iota((8, 128), 0)
    half = jnp.where(iota((16, 128), 0) >= 8, float(apart), 0.0).astype(bf16)
    zero = jnp.zeros((16, 128), bf16)

    def step(i, carry):
        weighted, depths, values = [], [], []
        for k in range(DEPOSIT_STEP // 2):
            own = slots_ref[pl.ds(pl.multiple_of(i * DEPOSIT_STEP * 4, 8) + 8 * k, 8), :]
            high = own.astype(bf16).astype(f32)
            low = own - high
            first = jnp.where(sub8 < 4, high, pltpu.roll(low, 4, 0))
            second = jnp.where(sub8 < 4, pltpu.roll(high, 4, 0), low)
            for value in (first, second):
                value = jnp.where(sub8 == 3, 1.0, value).astype(bf16)
                values.append(jnp.concatenate([value, value], axis=0))
        for k in range(DEPOSIT_STEP):
            slot = i * DEPOSIT_STEP + k
            value = values[k]
            q = jnp.broadcast_to(rows_q[pl.ds(slot, 1), :], (16, 128)).astype(bf16) - half
            weighted.append(
                jnp.concatenate([jnp.where(q == float(j), value, zero) for j in firsts], axis=0)
            )
            depths.append(lane_onehot(rows_l, slot, tiles).astype(jnp.float8_e4m3fn))
        store(
            lax.dot_general(
                jnp.concatenate(weighted, axis=1),
                jnp.concatenate(depths, axis=1),
                (((1,), (1,)), ((), ())),
                preferred_element_type=f32,
            )
        )
        return carry

    lax.fori_loop(0, slots // DEPOSIT_STEP, step, 0)


def deposit_faces_body(slots_ref, head_ref, tail_ref, acc, rows_q, rows_l):
    slots = slots_ref.shape[0] // 4
    label = slots_ref[pl.ds(3, slots, stride=4), :].astype(i32)
    rows_q[...] = (label >> 7).astype(f32)
    rows_l[...] = (label & 127).astype(f32)
    acc[...] = jnp.zeros(acc.shape, f32)

    def store(got):
        acc[...] += got

    firsts = [ex * PY for ex in range(PX)] + [PLANES]
    sum_rows(slots_ref, rows_q, rows_l, firsts, CY, 8, store)
    for c in range(4):
        for ref, first in ((head_ref, 0), (tail_ref, 8)):
            total = acc[pl.ds(first + c, PX, stride=16), :]
            above = acc[pl.ds(16 * PX + c, 1), :]
            if c < 3:
                total = total + acc[pl.ds(first + c + 4, PX, stride=16), :]
                above = above + acc[pl.ds(16 * PX + c + 4, 1), :]
            ref[c, 0:PX] = total
            ref[c, PX : PX + 1] = above


def deposit_body(slots_ref, total_ref, acc, rows_q, rows_l):
    slot_places(slots_ref, rows_q, rows_l)
    acc[...] = jnp.zeros(acc.shape, f32)

    def store(got):
        acc[0] += got[:, :128]
        acc[1] += got[:, 128:]

    sum_rows(slots_ref, rows_q, rows_l, [2 * j for j in range(12)], 1, 16, store)
    for c in range(4):
        for odd in range(2):
            total = acc[odd, pl.ds(c, Q2, stride=8), :]
            if c < 3:
                total = total + acc[odd, pl.ds(c + 4, Q2, stride=8), :]
            total_ref[c, pl.ds(odd, Q2, stride=2)] = total
        total_ref[c, ROWS:PADROWS] = jnp.zeros((PADROWS - ROWS, 128), f32)


def moved_lanes(row, first, count, shift):
    lane = iota(row.shape, 1)
    rolled = pltpu.roll(row, shift % 128, 1)
    return jnp.where((lane >= first) & (lane < first + count), rolled, 0.0)


def fold_y_body(total_ref, up_ref, down_ref, out_ref, head_ref, tail_ref):
    lane = iota((1, 128), 1)
    edge = lane % PY
    for c in range(4):
        out_ref[c] = total_ref[c]
        out_ref[c, pl.ds(CY, PX, stride=PY)] = (
            total_ref[c, pl.ds(CY, PX, stride=PY)] + up_ref[c, 0:PX]
        )
        out_ref[c, pl.ds(0, PX, stride=PY)] = (
            total_ref[c, pl.ds(0, PX, stride=PY)] + down_ref[c, 0:PX]
        )
        up = pltpu.roll(up_ref[c, PX : PX + 1], CY, 1)
        down = pltpu.roll(down_ref[c, PX : PX + 1], 128 - CY, 1)
        above = (
            total_ref[c, PLANES:ROWS]
            + jnp.where((edge == CY) & (lane < PLANES), up, 0.0)
            + jnp.where((edge == 0) & (lane < PLANES), down, 0.0)
        )
        out_ref[c, PLANES:ROWS] = above
        head_ref[c, 0:PY] = out_ref[c, 0:PY]
        head_ref[c, PY : PY + 1] = above
        tail_ref[c, 0:PY] = out_ref[c, PLANES - PY : PLANES]
        tail_ref[c, PY : PY + 1] = above


def fold_x_body(total_ref, up_ref, down_ref, out_ref, head_ref, tail_ref):
    last = PLANES - PY
    for c in range(4):
        out_ref[c] = total_ref[c]
        out_ref[c, 0:PY] = total_ref[c, 0:PY] + down_ref[c, 0:PY]
        out_ref[c, last:PLANES] = total_ref[c, last:PLANES] + up_ref[c, 0:PY]
        out_ref[c, PLANES:ROWS] = (
            total_ref[c, PLANES:ROWS]
            + moved_lanes(up_ref[c, PY : PY + 1], last, PY, last)
            + moved_lanes(down_ref[c, PY : PY + 1], 0, PY, -last)
        )
        total = out_ref[c]
        head_ref[c : c + 1] = column_as_row(total)
        tail_ref[c : c + 1] = total[PLANES:ROWS]
        head_ref[4 + c : 5 + c] = jnp.zeros((1, 128), f32)
        tail_ref[4 + c : 5 + c] = jnp.zeros((1, 128), f32)


def select_row(rows, bits):
    for bit in bits:
        rows = [
            jnp.where(bit, rows[j + 1], rows[j]) if j + 1 < len(rows) else rows[j]
            for j in range(0, len(rows), 2)
        ]
    return rows[0]


def look_body(
    total_ref, axes_ref, units_ref, slots_ref, found, normal_ref, cells, wide, rows_q, rows_l
):
    slots = slots_ref.shape[0] // 4
    count = jnp.maximum(total_ref[3], 1.0)
    wide[...] = jnp.zeros(wide.shape, f32)

    def tabulate(value, line):
        cells[...] = value
        for odd in range(2):
            wide[odd, pl.ds(line, Q2, stride=8), :] = cells[pl.ds(odd, Q2, stride=2)]

    for c in range(3):
        mean = total_ref[c] / count
        high = mean.astype(bf16).astype(f32)
        tabulate(high, c)
        tabulate(mean - high, c + 4)
    tabulate(axes_ref[...], 3)
    table = jnp.concatenate([wide[0], wide[1]], axis=1).astype(bf16)
    slot_places(slots_ref, rows_q, rows_l)
    sub8 = iota((8, 128), 0)
    for k in range(slots // 2):
        pair = [2 * k, 2 * k + 1]
        hot = jnp.concatenate([lane_onehot(rows_l, slot) for slot in pair], axis=1)
        read = jnp.dot(table, hot, preferred_element_type=f32)
        got = []
        for h in range(2):
            q = jnp.broadcast_to(rows_q[pl.ds(pair[h], 1), :], (8, 128))
            bits = [(q & (1 << b)) != 0 for b in range(5)]
            lines = [read[8 * j : 8 * j + 8, 128 * h : 128 * h + 128] for j in range(Q2)]
            value = select_row(lines, bits)
            got.append(value + pltpu.roll(value, 4, 0))
        found[pl.ds(8 * k, 8), :] = jnp.where(sub8 < 4, got[0], got[1])
        if (k + 1) % (4 * MOST) == 0:
            g = k // (4 * MOST)
            for rank in range(MOST):
                which = found[pl.ds((g * 8 * MOST + rank) * 4 + 3, 8, stride=4 * MOST), :]
                for c in range(3):
                    normal_ref[rank, c, pl.ds(8 * g, 8), :] = jnp.take_along_axis(
                        units_ref[c], which.astype(i32), axis=1
                    )


SENDERS = 32


def turn_body(
    total_ref, up_ref, down_ref, normal_ref, slots_ref, found, out_hbm, flow_hbm,
    out_ref, flow_ref, sems
):
    devices = out_ref.shape[2]
    shape = (PADROWS, 128)
    row = iota(shape, 0)
    lane = iota(shape, 1)
    top = (row == PLANES) & (lane < PLANES)
    totals = []
    for c in range(4):
        own = total_ref[c]
        column = jnp.sum(
            jnp.where((row == lane) & (row < PLANES), down_ref[c : c + 1], 0.0),
            axis=1,
            keepdims=True,
        )
        own = own + jnp.where(lane == 0, column, 0.0)
        totals.append(own + jnp.where(top, up_ref[c : c + 1], 0.0))
    count = jnp.maximum(totals[3], 1.0)
    rims = []
    for c in range(3):
        mean = totals[c] / count
        for ex in range(CX):
            flow_ref[c, ex] = mean[ex * PY : ex * PY + CY]
        low = pltpu.roll(column_as_row(mean), 64, 1)
        rim = jnp.where(iota((1, 128), 1) < 64, mean[PLANES:ROWS], low)
        rims.append(jnp.broadcast_to(rim, (8, 128)))
    parts = devices // SENDERS
    flow_copy = pltpu.make_async_copy(flow_ref, flow_hbm, sems.at[parts])
    flow_copy.start()

    def copy(i):
        part = pl.ds(i * SENDERS, SENDERS)
        return pltpu.make_async_copy(
            out_ref.at[:, :, part, :], out_hbm.at[:, :, part, :], sems.at[i]
        )

    for i in range(parts):
        for rank in range(MOST):
            for k in range(SENDERS // 8):
                source = i * SENDERS + 8 * k
                place = (source * MOST + rank) * 4
                label = slots_ref[pl.ds(place + 3, 8, stride=12), :].astype(i32)
                q = label >> 7
                l = label & 127
                above = q == PLANES
                below = (l == 0) & (q < PLANES)
                rim_lane = jnp.where(above, l, (q + 64) & 127)
                n = [normal_ref[rank, c, pl.ds(source, 8), :] for c in range(3)]
                u = [
                    jnp.where(
                        above | below,
                        jnp.take_along_axis(rims[c], rim_lane, axis=1),
                        found[pl.ds(place + c, 8, stride=12), :],
                    )
                    for c in range(3)
                ]
                w = [slots_ref[pl.ds(place + c, 8, stride=12), :] - u[c] for c in range(3)]
                inner = n[0] * w[0] + n[1] * w[1] + n[2] * w[2]
                crossed = [
                    n[1] * w[2] - n[2] * w[1],
                    n[2] * w[0] - n[0] * w[2],
                    n[0] * w[1] - n[1] * w[0],
                ]
                for c in range(3):
                    out_ref[rank, c, pl.ds(source, 8), :] = (
                        u[c]
                        + w[c] * angle_cosine
                        + crossed[c] * angle_sine
                        + n[c] * inner * (1.0 - angle_cosine)
                    )
        copy(i).start()
    for i in range(parts):
        copy(i).wait()
    flow_copy.wait()


def both_ways(head, tail, axis):
    count = lax.axis_size(axis)
    up = lax.ppermute(head, axis, [((i + 1) % count, i) for i in range(count)])
    down = lax.ppermute(tail, axis, [(i, (i + 1) % count) for i in range(count)])
    return up, down


def shards(velocity, cell_index, block_target, rotation_axis, grid_shift):
    devices = 128
    shape = jax.ShapeDtypeStruct
    vmem = pl.BlockSpec(memory_space=pltpu.VMEM)
    smem = pl.BlockSpec(memory_space=pltpu.SMEM)
    hbm = pl.BlockSpec(memory_space=pltpu.HBM)
    blocks = velocity.shape[0]
    send, units = call(
        pack_body,
        [shape((devices * MOST * 4, 128), f32), shape((3, 8, 128), f32)],
        in_specs=[hbm, hbm, hbm],
        scratch_shapes=[
            pltpu.VMEM((1, blocks), i32),
            pltpu.VMEM((3, blocks, 128), f32),
            pltpu.VMEM((blocks, 128), i32),
            pltpu.SemaphoreType.DMA((3,)),
        ],
        name="pack",
    )(
        *(
            pltpu.with_memory_space_constraint(x, pltpu.HBM)
            for x in (block_target.reshape(1, -1), jnp.transpose(velocity, (1, 0, 2)), cell_index)
        )
    )
    axes = call(
        axes_body,
        shape((PADROWS, 128), f32),
        in_specs=[smem, vmem],
        scratch_shapes=[pltpu.VMEM((PADROWS, 128), i32)],
        name="axes",
    )(grid_shift, rotation_axis)
    slots = lax.all_to_all(
        send.reshape(devices, MOST, 4, 128), ("gx", "gy", "gz"), split_axis=0, concat_axis=0, tiled=True
    ).reshape(devices * MOST * 4, 128)
    total_shape = shape((4, PADROWS, 128), f32)
    x_face = shape((4, 16, 128), f32)
    y_face = shape((4, 8, 128), f32)
    z_face = shape((8, 128), f32)
    by_slot = pltpu.VMEM((devices * MOST, 128), f32)
    head, tail = call(
        deposit_faces_body,
        [y_face, y_face],
        scratch_shapes=[pltpu.VMEM((16 * (PX + 1), 128), f32), by_slot, by_slot],
        name="deposit_faces",
    )(slots)
    slots, head, tail = lax.optimization_barrier((slots, head, tail))
    up, down = both_ways(head, tail, "gy")
    total = call(
        deposit_body,
        total_shape,
        scratch_shapes=[pltpu.VMEM((2, 192, 128), f32), by_slot, by_slot],
        name="deposit",
    )(slots)
    total, head, tail = call(fold_y_body, [total_shape, x_face, x_face], name="fold_y")(
        total, up, down
    )
    up, down = both_ways(head, tail, "gx")
    up, down, axes = lax.optimization_barrier((up, down, axes))
    total, head, tail = call(fold_x_body, [total_shape, z_face, z_face], name="fold_x")(
        total, up, down
    )
    up, down = both_ways(head, tail, "gz")
    found, normal = call(
        look_body,
        [shape((devices * MOST * 4, 128), f32), shape((MOST, 3, devices, 128), f32)],
        scratch_shapes=[
            pltpu.VMEM((PADROWS, 128), f32),
            pltpu.VMEM((2, Q2 * 8, 128), f32),
            pltpu.VMEM((devices * MOST, 128), i32),
            pltpu.VMEM((devices * MOST, 128), f32),
        ],
        name="look",
    )(total, axes, units, slots)
    updated, cell_flow = call(
        turn_body,
        [shape((MOST, 3, devices, 128), f32), shape((3, CX, CY, CZ), f32)],
        out_specs=[hbm, hbm],
        scratch_shapes=[
            pltpu.VMEM((MOST, 3, devices, 128), f32),
            pltpu.VMEM((3, CX, CY, CZ), f32),
            pltpu.SemaphoreType.DMA((devices // SENDERS + 1,)),
        ],
        name="turn",
    )(total, up, down, normal, slots, found)
    return jnp.transpose(updated, (2, 0, 1, 3))[None], cell_flow


def solution(mesh):
    return jax.shard_map(
        shards,
        mesh=mesh,
        in_specs=(
            P(("gx", "gy", "gz"), None, None),
            P(("gx", "gy", "gz"), None),
            P(("gx", "gy", "gz"), None),
            P(),
            P(),
        ),
        out_specs=(P(("gx", "gy", "gz"), None, None, None, None), P(None, "gx", "gy", "gz")),
        check_vma=False,
    )
```

```python
import functools

import jax
import jax.numpy as jnp
from jax import lax
from jax.experimental import pallas as pl
from jax.experimental.pallas import tpu as pltpu
from jax.sharding import PartitionSpec as P

CX = 4
CY = 8
CZ = 128
NAX = 64
APER = 32
MOST = 3
PX = CX + 1
PY = CY + 1
PLANES = PX * PY
ROWS = PLANES + 1
PADROWS = 48
EMPTY = 6400.0

angle_cosine = -0.6427876096865393
angle_sine = 0.766044443118978

f32 = jnp.float32
bf16 = jnp.bfloat16
i32 = jnp.int32


def iota(shape, dim):
    return lax.broadcasted_iota(i32, shape, dim)


def axis_table(shape):
    counter = iota(shape, 1).astype(f32) + 0.5
    height = 1.0 - 2.0 * counter / NAX
    radius = jnp.sqrt(jnp.maximum(1.0 - height * height, 0.0))
    turning = counter * 2.399963229728653
    return radius * jnp.cos(turning), radius * jnp.sin(turning), height


def split3(value):
    high = value.astype(bf16)
    rest = value - high.astype(f32)
    middle = rest.astype(bf16)
    return high, middle, (rest - middle.astype(f32)).astype(bf16)


def call(body, out_shape, **kw):
    return pl.pallas_call(
        body,
        out_shape=out_shape,
        compiler_params=pltpu.CompilerParams(vmem_limit_bytes=48 * 1024 * 1024),
        **kw,
    )


def pack_body(
    target_hbm, velocity_hbm, index_hbm, out_ref, units_ref, target_ref, velocity_ref, index_ref, sems
):
    sources = (target_hbm, index_hbm, velocity_hbm)
    sinks = (target_ref, index_ref, velocity_ref)
    copies = [
        pltpu.make_async_copy(source, sink, sems.at[k])
        for k, (source, sink) in enumerate(zip(sources, sinks))
    ]
    for copy in copies:
        copy.start()
    for c, line in enumerate(axis_table((8, 128))):
        units_ref[c] = line
    bricks = 128
    blocks = target_ref.shape[1]
    copies[0].wait()
    target = jnp.broadcast_to(target_ref[...], (bricks, blocks))
    onehot = target == iota((bricks, blocks), 0)
    onehot_bf = jnp.where(onehot, 1.0, 0.0).astype(bf16)
    earlier = jnp.where(iota((blocks, blocks), 0) < iota((blocks, blocks), 1), 1.0, 0.0)
    before = jnp.dot(onehot_bf, earlier.astype(bf16), preferred_element_type=f32)
    places = [
        jnp.where(onehot & (before == float(rank)), 1.0, 0.0).astype(bf16) for rank in range(MOST)
    ]
    copies[1].wait()
    index = index_ref[...]
    plane = (index * 8129) >> 20
    depth = index - plane * (CZ + 1)
    top = depth == CZ
    label = jnp.where(top, PLANES * 128 + plane, plane * 128 + depth)
    label = label.astype(f32) - EMPTY
    copies[2].wait()
    splits = split3(jnp.concatenate([velocity_ref[c] for c in range(3)] + [label], axis=1))
    for rank in range(MOST):
        moved = sum(jnp.dot(places[rank], s, preferred_element_type=f32) for s in reversed(splits))
        for c in range(4):
            value = moved[:, c * 128 : (c + 1) * 128]
            if c == 3:
                value = value + EMPTY
            out_ref[pl.ds(rank * 4 + c, bricks, stride=4 * MOST), :] = value


def axes_body(shift_ref, rotation_ref, out_ref, rows):
    base_x = lax.axis_index("gx") * CX + shift_ref[0]
    base_y = lax.axis_index("gy") * CY + shift_ref[1]
    rows[...] = jnp.zeros(rows.shape, i32)
    for ex in range(PX):
        for ey in range(PY):
            a = (base_x + ex) & (APER - 1)
            b = (base_y + ey) & (APER - 1)
            rows[pl.ds(ex * PY + ey, 1), :APER] = rotation_ref[a, pl.ds(b, 1), :]
    value = rows[...].astype(f32)
    value = value + pltpu.roll(value, 32, 1)
    value = value + pltpu.roll(value, 64, 1)
    value = pltpu.roll(value, (128 - shift_ref[2]) & 127, 1)
    first = column_as_row(value)
    out_ref[...] = jnp.where(iota(value.shape, 0) == PLANES, first, value)


def column_as_row(value):
    column = jnp.broadcast_to(value[:, 0:1], value.shape)
    same = iota(value.shape, 0) == iota(value.shape, 1)
    return jnp.sum(jnp.where(same, column, 0.0), axis=0, keepdims=True)


DEPOSIT_STEP = 384
Q2 = ROWS // 2


def slot_places(slots_ref, rows_q, rows_l):
    slots = slots_ref.shape[0] // 4
    label = slots_ref[pl.ds(3, slots, stride=4), :].astype(i32)
    rows_q[...] = (label >> 8).astype(rows_q.dtype)
    rows_l[...] = jnp.where(label >= PADROWS * 128, 512, label & 255).astype(f32)


def lane_onehot(rows_l, slot, tiles=16):
    step = iota((16, 128), 0).astype(f32).astype(bf16)
    lane = jnp.broadcast_to(rows_l[pl.ds(slot, 1), :], (16, 128)).astype(bf16) - step
    one = jnp.ones((16, 128), bf16)
    zero = jnp.zeros((16, 128), bf16)
    return jnp.concatenate(
        [jnp.where(lane == float(16 * j), one, zero) for j in range(tiles)], axis=0
    )


def sum_rows(slots_ref, rows_q, rows_l, firsts, apart, tiles, store):
    slots = slots_ref.shape[0] // 4
    sub8 = iota((8, 128), 0)
    half = jnp.where(iota((16, 128), 0) >= 8, float(apart), 0.0).astype(bf16)
    zero = jnp.zeros((16, 128), bf16)

    def step(i, carry):
        weighted, depths, values = [], [], []
        for k in range(DEPOSIT_STEP // 2):
            own = slots_ref[pl.ds(pl.multiple_of(i * DEPOSIT_STEP * 4, 8) + 8 * k, 8), :]
            high = own.astype(bf16).astype(f32)
            low = own - high
            first = jnp.where(sub8 < 4, high, pltpu.roll(low, 4, 0))
            second = jnp.where(sub8 < 4, pltpu.roll(high, 4, 0), low)
            for value in (first, second):
                value = jnp.where(sub8 == 3, 1.0, value).astype(bf16)
                values.append(jnp.concatenate([value, value], axis=0))
        for k in range(DEPOSIT_STEP):
            slot = i * DEPOSIT_STEP + k
            value = values[k]
            q = jnp.broadcast_to(rows_q[pl.ds(slot, 1), :], (16, 128)).astype(bf16) - half
            weighted.append(
                jnp.concatenate([jnp.where(q == float(j), value, zero) for j in firsts], axis=0)
            )
            depths.append(lane_onehot(rows_l, slot, tiles).astype(jnp.float8_e4m3fn))
        store(
            lax.dot_general(
                jnp.concatenate(weighted, axis=1),
                jnp.concatenate(depths, axis=1),
                (((1,), (1,)), ((), ())),
                preferred_element_type=f32,
            )
        )
        return carry

    lax.fori_loop(0, slots // DEPOSIT_STEP, step, 0)


def deposit_faces_body(slots_ref, head_ref, tail_ref, acc, rows_q, rows_l):
    slots = slots_ref.shape[0] // 4
    label = slots_ref[pl.ds(3, slots, stride=4), :].astype(i32)
    rows_q[...] = (label >> 7).astype(f32)
    rows_l[...] = (label & 127).astype(f32)
    acc[...] = jnp.zeros(acc.shape, f32)

    def store(got):
        acc[...] += got

    firsts = [ex * PY for ex in range(PX)] + [PLANES]
    sum_rows(slots_ref, rows_q, rows_l, firsts, CY, 8, store)
    for c in range(4):
        for ref, first in ((head_ref, 0), (tail_ref, 8)):
            total = acc[pl.ds(first + c, PX, stride=16), :]
            above = acc[pl.ds(16 * PX + c, 1), :]
            if c < 3:
                total = total + acc[pl.ds(first + c + 4, PX, stride=16), :]
                above = above + acc[pl.ds(16 * PX + c + 4, 1), :]
            ref[c, 0:PX] = total
            ref[c, PX : PX + 1] = above


def deposit_body(slots_ref, total_ref, acc, rows_q, rows_l):
    slot_places(slots_ref, rows_q, rows_l)
    acc[...] = jnp.zeros(acc.shape, f32)

    def store(got):
        acc[0] += got[:, :128]
        acc[1] += got[:, 128:]

    sum_rows(slots_ref, rows_q, rows_l, [2 * j for j in range(12)], 1, 16, store)
    for c in range(4):
        for odd in range(2):
            total = acc[odd, pl.ds(c, Q2, stride=8), :]
            if c < 3:
                total = total + acc[odd, pl.ds(c + 4, Q2, stride=8), :]
            total_ref[c, pl.ds(odd, Q2, stride=2)] = total
        total_ref[c, ROWS:PADROWS] = jnp.zeros((PADROWS - ROWS, 128), f32)


def moved_lanes(row, first, count, shift):
    lane = iota(row.shape, 1)
    rolled = pltpu.roll(row, shift % 128, 1)
    return jnp.where((lane >= first) & (lane < first + count), rolled, 0.0)


def fold_y_body(total_ref, up_ref, down_ref, out_ref, head_ref, tail_ref):
    lane = iota((1, 128), 1)
    edge = lane % PY
    for c in range(4):
        out_ref[c] = total_ref[c]
        out_ref[c, pl.ds(CY, PX, stride=PY)] = (
            total_ref[c, pl.ds(CY, PX, stride=PY)] + up_ref[c, 0:PX]
        )
        out_ref[c, pl.ds(0, PX, stride=PY)] = (
            total_ref[c, pl.ds(0, PX, stride=PY)] + down_ref[c, 0:PX]
        )
        up = pltpu.roll(up_ref[c, PX : PX + 1], CY, 1)
        down = pltpu.roll(down_ref[c, PX : PX + 1], 128 - CY, 1)
        above = (
            total_ref[c, PLANES:ROWS]
            + jnp.where((edge == CY) & (lane < PLANES), up, 0.0)
            + jnp.where((edge == 0) & (lane < PLANES), down, 0.0)
        )
        out_ref[c, PLANES:ROWS] = above
        head_ref[c, 0:PY] = out_ref[c, 0:PY]
        head_ref[c, PY : PY + 1] = above
        tail_ref[c, 0:PY] = out_ref[c, PLANES - PY : PLANES]
        tail_ref[c, PY : PY + 1] = above


def fold_x_body(total_ref, up_ref, down_ref, out_ref, head_ref, tail_ref):
    last = PLANES - PY
    for c in range(4):
        out_ref[c] = total_ref[c]
        out_ref[c, 0:PY] = total_ref[c, 0:PY] + down_ref[c, 0:PY]
        out_ref[c, last:PLANES] = total_ref[c, last:PLANES] + up_ref[c, 0:PY]
        out_ref[c, PLANES:ROWS] = (
            total_ref[c, PLANES:ROWS]
            + moved_lanes(up_ref[c, PY : PY + 1], last, PY, last)
            + moved_lanes(down_ref[c, PY : PY + 1], 0, PY, -last)
        )
        total = out_ref[c]
        head_ref[c : c + 1] = column_as_row(total)
        tail_ref[c : c + 1] = total[PLANES:ROWS]
        head_ref[4 + c : 5 + c] = jnp.zeros((1, 128), f32)
        tail_ref[4 + c : 5 + c] = jnp.zeros((1, 128), f32)


def select_row(rows, bits):
    for bit in bits:
        rows = [
            jnp.where(bit, rows[j + 1], rows[j]) if j + 1 < len(rows) else rows[j]
            for j in range(0, len(rows), 2)
        ]
    return rows[0]


def look_body(
    total_ref, axes_ref, units_ref, slots_ref, found, normal_ref, cells, wide, rows_q, rows_l
):
    slots = slots_ref.shape[0] // 4
    count = jnp.maximum(total_ref[3], 1.0)
    wide[...] = jnp.zeros(wide.shape, f32)

    def tabulate(value, line):
        cells[...] = value
        for odd in range(2):
            wide[odd, pl.ds(line, Q2, stride=8), :] = cells[pl.ds(odd, Q2, stride=2)]

    for c in range(3):
        mean = total_ref[c] / count
        high = mean.astype(bf16).astype(f32)
        tabulate(high, c)
        tabulate(mean - high, c + 4)
    tabulate(axes_ref[...], 3)
    table = jnp.concatenate([wide[0], wide[1]], axis=1).astype(bf16)
    slot_places(slots_ref, rows_q, rows_l)
    sub8 = iota((8, 128), 0)
    for k in range(slots // 2):
        pair = [2 * k, 2 * k + 1]
        hot = jnp.concatenate([lane_onehot(rows_l, slot) for slot in pair], axis=1)
        read = jnp.dot(table, hot, preferred_element_type=f32)
        got = []
        for h in range(2):
            q = jnp.broadcast_to(rows_q[pl.ds(pair[h], 1), :], (8, 128))
            bits = [(q & (1 << b)) != 0 for b in range(5)]
            lines = [read[8 * j : 8 * j + 8, 128 * h : 128 * h + 128] for j in range(Q2)]
            value = select_row(lines, bits)
            got.append(value + pltpu.roll(value, 4, 0))
        found[pl.ds(8 * k, 8), :] = jnp.where(sub8 < 4, got[0], got[1])
        if (k + 1) % (4 * MOST) == 0:
            g = k // (4 * MOST)
            for rank in range(MOST):
                which = found[pl.ds((g * 8 * MOST + rank) * 4 + 3, 8, stride=4 * MOST), :]
                for c in range(3):
                    normal_ref[rank, c, pl.ds(8 * g, 8), :] = jnp.take_along_axis(
                        units_ref[c], which.astype(i32), axis=1
                    )


SENDERS = 32


def turn_body(
    total_ref, up_ref, down_ref, normal_ref, slots_ref, found, out_hbm, flow_hbm,
    out_ref, flow_ref, sems
):
    devices = out_ref.shape[2]
    shape = (PADROWS, 128)
    row = iota(shape, 0)
    lane = iota(shape, 1)
    top = (row == PLANES) & (lane < PLANES)
    totals = []
    for c in range(4):
        own = total_ref[c]
        column = jnp.sum(
            jnp.where((row == lane) & (row < PLANES), down_ref[c : c + 1], 0.0),
            axis=1,
            keepdims=True,
        )
        own = own + jnp.where(lane == 0, column, 0.0)
        totals.append(own + jnp.where(top, up_ref[c : c + 1], 0.0))
    count = jnp.maximum(totals[3], 1.0)
    rims = []
    for c in range(3):
        mean = totals[c] / count
        for ex in range(CX):
            flow_ref[c, ex] = mean[ex * PY : ex * PY + CY]
        low = pltpu.roll(column_as_row(mean), 64, 1)
        rim = jnp.where(iota((1, 128), 1) < 64, mean[PLANES:ROWS], low)
        rims.append(jnp.broadcast_to(rim, (8, 128)))
    parts = devices // SENDERS
    flow_copy = pltpu.make_async_copy(flow_ref, flow_hbm, sems.at[parts])
    flow_copy.start()

    def copy(i):
        part = pl.ds(i * SENDERS, SENDERS)
        return pltpu.make_async_copy(
            out_ref.at[:, :, part, :], out_hbm.at[:, :, part, :], sems.at[i]
        )

    for i in range(parts):
        for rank in range(MOST):
            for k in range(SENDERS // 8):
                source = i * SENDERS + 8 * k
                place = (source * MOST + rank) * 4
                label = slots_ref[pl.ds(place + 3, 8, stride=12), :].astype(i32)
                q = label >> 7
                l = label & 127
                above = q == PLANES
                below = (l == 0) & (q < PLANES)
                rim_lane = jnp.where(above, l, (q + 64) & 127)
                n = [normal_ref[rank, c, pl.ds(source, 8), :] for c in range(3)]
                u = [
                    jnp.where(
                        above | below,
                        jnp.take_along_axis(rims[c], rim_lane, axis=1),
                        found[pl.ds(place + c, 8, stride=12), :],
                    )
                    for c in range(3)
                ]
                w = [slots_ref[pl.ds(place + c, 8, stride=12), :] - u[c] for c in range(3)]
                inner = n[0] * w[0] + n[1] * w[1] + n[2] * w[2]
                crossed = [
                    n[1] * w[2] - n[2] * w[1],
                    n[2] * w[0] - n[0] * w[2],
                    n[0] * w[1] - n[1] * w[0],
                ]
                for c in range(3):
                    out_ref[rank, c, pl.ds(source, 8), :] = (
                        u[c]
                        + w[c] * angle_cosine
                        + crossed[c] * angle_sine
                        + n[c] * inner * (1.0 - angle_cosine)
                    )
        copy(i).start()
    for i in range(parts):
        copy(i).wait()
    flow_copy.wait()


def both_ways(head, tail, axis):
    count = lax.axis_size(axis)
    up = lax.ppermute(head, axis, [((i + 1) % count, i) for i in range(count)])
    down = lax.ppermute(tail, axis, [(i, (i + 1) % count) for i in range(count)])
    return up, down


def shards(velocity, cell_index, block_target, rotation_axis, grid_shift):
    devices = 128
    shape = jax.ShapeDtypeStruct
    vmem = pl.BlockSpec(memory_space=pltpu.VMEM)
    smem = pl.BlockSpec(memory_space=pltpu.SMEM)
    hbm = pl.BlockSpec(memory_space=pltpu.HBM)
    blocks = velocity.shape[0]
    send, units = call(
        pack_body,
        [shape((devices * MOST * 4, 128), f32), shape((3, 8, 128), f32)],
        in_specs=[hbm, hbm, hbm],
        scratch_shapes=[
            pltpu.VMEM((1, blocks), i32),
            pltpu.VMEM((3, blocks, 128), f32),
            pltpu.VMEM((blocks, 128), i32),
            pltpu.SemaphoreType.DMA((3,)),
        ],
        name="pack",
    )(
        *(
            pltpu.with_memory_space_constraint(x, pltpu.HBM)
            for x in (block_target.reshape(1, -1), jnp.transpose(velocity, (1, 0, 2)), cell_index)
        )
    )
    axes = call(
        axes_body,
        shape((PADROWS, 128), f32),
        in_specs=[smem, vmem],
        scratch_shapes=[pltpu.VMEM((PADROWS, 128), i32)],
        name="axes",
    )(grid_shift, rotation_axis)
    slots = lax.all_to_all(
        send.reshape(devices, MOST, 4, 128), ("gx", "gy", "gz"), split_axis=0, concat_axis=0, tiled=True
    ).reshape(devices * MOST * 4, 128)
    total_shape = shape((4, PADROWS, 128), f32)
    x_face = shape((4, 16, 128), f32)
    y_face = shape((4, 8, 128), f32)
    z_face = shape((8, 128), f32)
    by_slot = pltpu.VMEM((devices * MOST, 128), f32)
    head, tail = call(
        deposit_faces_body,
        [y_face, y_face],
        scratch_shapes=[pltpu.VMEM((16 * (PX + 1), 128), f32), by_slot, by_slot],
        name="deposit_faces",
    )(slots)
    slots, head, tail = lax.optimization_barrier((slots, head, tail))
    up, down = both_ways(head, tail, "gy")
    total = call(
        deposit_body,
        total_shape,
        scratch_shapes=[pltpu.VMEM((2, 192, 128), f32), by_slot, by_slot],
        name="deposit",
    )(slots)
    total, head, tail = call(fold_y_body, [total_shape, x_face, x_face], name="fold_y")(
        total, up, down
    )
    up, down = both_ways(head, tail, "gx")
    up, down, axes = lax.optimization_barrier((up, down, axes))
    total, head, tail = call(fold_x_body, [total_shape, z_face, z_face], name="fold_x")(
        total, up, down
    )
    up, down = both_ways(head, tail, "gz")
    found, normal = call(
        look_body,
        [shape((devices * MOST * 4, 128), f32), shape((MOST, 3, devices, 128), f32)],
        scratch_shapes=[
            pltpu.VMEM((PADROWS, 128), f32),
            pltpu.VMEM((2, Q2 * 8, 128), f32),
            pltpu.VMEM((devices * MOST, 128), i32),
            pltpu.VMEM((devices * MOST, 128), f32),
        ],
        name="look",
    )(total, axes, units, slots)
    updated, cell_flow = call(
        turn_body,
        [shape((MOST, 3, devices, 128), f32), shape((3, CX, CY, CZ), f32)],
        out_specs=[hbm, hbm],
        scratch_shapes=[
            pltpu.VMEM((MOST, 3, devices, 128), f32),
            pltpu.VMEM((3, CX, CY, CZ), f32),
            pltpu.SemaphoreType.DMA((devices // SENDERS + 1,)),
        ],
        name="turn",
    )(total, up, down, normal, slots, found)
    return jnp.transpose(updated, (2, 0, 1, 3))[None], cell_flow


def solution(mesh):
    return jax.shard_map(
        shards,
        mesh=mesh,
        in_specs=(
            P(("gx", "gy", "gz"), None, None),
            P(("gx", "gy", "gz"), None),
            P(("gx", "gy", "gz"), None),
            P(),
            P(),
        ),
        out_specs=(P(("gx", "gy", "gz"), None, None, None, None), P(None, "gx", "gy", "gz")),
        check_vma=False,
    )
```
